512 devices in a mesh: grp: 32 (over z, y_lo, core), dom: 16 (over y_hi, x).
Axes of the slice: x: 4, y: 8 (y_hi: 4, y_lo: 2; y = y_hi * 2 + y_lo), z: 8, core: 2. Of those that a mesh axis runs over, the one named last changes fastest.
Arguments:
- connect: int32 [20, 65536], P(None, ('grp', 'dom')), may hold values from 0 to 511, as said below
- interface_nodes: int32 [512, 4, 32], P(('grp', 'dom')), may hold values from 0 to 511, as said below
- neighbours: int32 [512, 4], P(('grp', 'dom')), may hold values from 0 to 1, as said below
- point_rank: int32 [512, 2048], P(('grp', 'dom')), may hold values from 0 to 2047, each once within a row
- shape_grad: float32 [48, 20], replicated, may hold values from -1.25 to 1.25
- inverse_jacobian: float32 [9, 65536], P(None, ('grp', 'dom')), may hold values from -0.45 to 2.5
- lame_moduli: float32 [2, 65536], P(None, ('grp', 'dom')), may hold values from 0.5 to 2
- point_weights: float32 [16, 65536], P(None, ('grp', 'dom')), may hold values from 0.003 to 0.02
- mass_elem: float32 [20, 65536], P(None, ('grp', 'dom')), may hold values from 0.5 to 2
- source_pattern: float32 [3, 262144], P(None, ('grp', 'dom')), may hold values from -6 to 6
- wavelet: float32 [16], replicated, may hold values from -6 to 6
Outputs:
- strain_db: bfloat16 [16, 6, 1048576], P(None, None, ('grp', 'dom'))
The draws below stay inside these ranges and needn't reach their ends.
Inputs may be any that keep to these rules, and one draw needn't show every extreme that they name: `connect`: every one of a partition's 512 nodes is named by some element of that partition. `interface_nodes`: entry i of list k of a partition and entry i of the opposite list of the partition beside it in direction k are copies of one node; no node stands twice among a partition's four lists. `neighbours`: the entry of a partition in direction k equals that of the partition beside it in the opposite direction; it is 0 where no partition lies in direction k.
All inputs are finite; a program needn't handle non-finite values.
Results may differ from the reference program's by a relative error of at most 0.001.
Values may be sent and summed in bfloat16 or wider, within the bound.
No kernel may reach another device: no remote copies, remote signals or barrier semaphores. Data moves between devices by JAX's collectives and lax.ppermute only.
A program may use at most 64 MiB of HBM per device.

```python
import math
import jax
import jax.numpy as jnp
from jax import lax

ELEM_DEV = 128
EL_NODES = 20
POINTS = 16
STRAIN = 6
STEPS = 16
NODE_DEV = 512
FACE_NODES = 32
PT_DEV = 2048
GROUPS = 32
WRITERS = 16
PARTS_SIZE = 512
ELEMS = 65536
NODES = 262144


def draw_connect(key, part):
    streams = jax.random.split(key, PARTS_SIZE)

    def one_partition(stream):
        first_key, second_key = jax.random.split(stream)
        shuffled = jax.random.permutation(first_key, EL_NODES * ELEM_DEV)
        filler = jax.random.randint(second_key, (EL_NODES * ELEM_DEV,), 0, NODE_DEV)
        node_ids = jnp.where(shuffled < NODE_DEV, shuffled, filler)
        return node_ids.reshape(EL_NODES, ELEM_DEV).astype(jnp.int32)
    blocks = jax.vmap(one_partition)(streams)
    return blocks.transpose(1, 0, 2).reshape(EL_NODES, PARTS_SIZE * ELEM_DEV)


def draw_interface_nodes(key, part):
    streams = jax.random.split(jax.random.fold_in(key, 11), PARTS_SIZE)

    def pick_lists(stream):
        shuffled = jax.random.permutation(stream, NODE_DEV)
        return shuffled[:4 * FACE_NODES].reshape(4, FACE_NODES).astype(jnp.int32)
    return jax.vmap(pick_lists)(streams)


def draw_neighbours(key, part):
    first_key, second_key = jax.random.split(jax.random.fold_in(key, 23))
    vertical = (jax.random.randint(first_key, (GROUPS, WRITERS), 0, 4) < 3).astype(jnp.int32)
    vertical = vertical * (jnp.arange(GROUPS) < GROUPS - 1).astype(jnp.int32)[:, None]
    lateral = (jax.random.randint(second_key, (GROUPS, WRITERS), 0, 4) < 3).astype(jnp.int32)
    lateral = lateral * (jnp.arange(WRITERS) < WRITERS - 1).astype(jnp.int32)[None, :]
    toward_lower = jnp.concatenate([jnp.zeros((1, WRITERS), jnp.int32), vertical[:-1]], axis=0)
    toward_left = jnp.concatenate([jnp.zeros((GROUPS, 1), jnp.int32), lateral[:, :-1]], axis=1)
    table = jnp.stack([toward_lower, vertical, toward_left, lateral], axis=2)
    return table.reshape(PARTS_SIZE, 4).astype(jnp.int32)


def draw_inverse_jacobian(key, part):
    first_key, second_key = jax.random.split(jax.random.fold_in(key, 37))
    count = PARTS_SIZE * ELEM_DEV
    diagonal = jnp.exp(jax.random.uniform(first_key, (3, count), jnp.float32, -0.5, 0.5))
    shearing = jnp.clip(0.25 * jax.random.normal(second_key, (3, 3, count), jnp.float32), -0.45, 0.45)
    identity = jnp.eye(3, dtype=jnp.float32)
    matrix = shearing * (1.0 - identity)[:, :, None] + identity[:, :, None] * diagonal[:, None, :]
    return matrix.reshape(9, count).astype(jnp.float32)


def level_of(stream_key, extent, shards, smallest, top_value):
    def one(position, shards_of):
        steps = jax.random.uniform(jax.random.fold_in(jax.random.fold_in(stream_key, 6), position), (shards_of,), jnp.float32, smallest / len(shards), top_value / len(shards))
        return jnp.repeat(jnp.exp(steps), extent[position] // shards_of).reshape((-1,) + (1,) * (len(extent) - position - 1))

    gain = one(*shards[0])
    for cut in shards[1:]:
        gain = gain * one(*cut)
    return gain


def gaussian(rng, dims, spread, bound, pieces=(), kind=jnp.bfloat16):
    loudness = level_of(rng, dims, pieces, -0.22, 0.18) if pieces else 1.0
    values = jax.random.normal(rng, dims, jnp.float32) * spread * loudness
    return jnp.minimum(jnp.maximum(values, -bound), bound).astype(kind)


def setup_inputs(seed: int = 0) -> dict:
    arg_keys = jax.random.split(jax.random.key(seed), 12)
    return {
        "connect": draw_connect(jax.random.fold_in(arg_keys[11], 71), 0),
        "interface_nodes": draw_interface_nodes(jax.random.fold_in(arg_keys[11], 71), 0),
        "neighbours": draw_neighbours(jax.random.fold_in(arg_keys[11], 71), 0),
        "point_rank": jax.vmap(lambda own: jax.random.permutation(own, PT_DEV))(jax.random.split(arg_keys[3], PARTS_SIZE)).reshape((PARTS_SIZE, PT_DEV)).astype(jnp.int32),
        "shape_grad": gaussian(arg_keys[4], (3 * POINTS, EL_NODES), EL_NODES ** -0.5, 1.25, (), jnp.float32),
        "inverse_jacobian": draw_inverse_jacobian(jax.random.fold_in(arg_keys[11], 71), 0),
        "lame_moduli": jnp.clip(jnp.exp(math.log(2.0) - 1.3862944 * jax.random.uniform(arg_keys[6], (2, ELEMS), jnp.float32) ** level_of(arg_keys[6], (2, ELEMS), ((1, 512),), -0.2, 0.2)), 0.5, 2.0),
        "point_weights": jnp.clip(jnp.exp(math.log(0.02) - 1.89712 * jax.random.uniform(arg_keys[7], (POINTS, ELEMS), jnp.float32) ** level_of(arg_keys[7], (POINTS, ELEMS), ((1, 512),), -0.2, 0.2)), 0.003, 0.02),
        "mass_elem": jnp.clip(jnp.exp(math.log(2.0) - 1.3862944 * jax.random.uniform(arg_keys[8], (EL_NODES, ELEMS), jnp.float32) ** level_of(arg_keys[8], (EL_NODES, ELEMS), ((1, 512),), -0.2, 0.2)), 0.5, 2.0),
        "source_pattern": gaussian(arg_keys[9], (3, NODES), 1.0, 6.0, ((1, 512),), jnp.float32),
        "wavelet": gaussian(arg_keys[10], (STEPS,), 1.0, 6.0, (), jnp.float32),
    }


time_step = 0.5


def gradient_at(displace, connect, shape_grad, inverse_jacobian):
    elements = connect.shape[1]
    node_values = jnp.take(displace, connect, axis=1)
    along_ref = jnp.einsum('mn,cne->cme', shape_grad, node_values, precision=lax.Precision.HIGHEST)
    along_ref = along_ref.reshape(3, 3, POINTS, elements)
    jacobian = inverse_jacobian.reshape(3, 3, elements)
    result = along_ref[:, 0, None] * jacobian[0][None, :, None, :]
    result = result + along_ref[:, 1, None] * jacobian[1][None, :, None, :]
    result = result + along_ref[:, 2, None] * jacobian[2][None, :, None, :]
    return result


def strain_of(tensor):
    return jnp.stack([tensor[0, 0], tensor[1, 1], tensor[2, 2],
                      0.5 * (tensor[1, 2] + tensor[2, 1]),
                      0.5 * (tensor[0, 2] + tensor[2, 0]),
                      0.5 * (tensor[0, 1] + tensor[1, 0])], axis=0)


def element_forces(tensor, lame_moduli, point_weights, inverse_jacobian, shape_grad, connect, node_count):
    elements = connect.shape[1]
    jacobian = inverse_jacobian.reshape(3, 3, elements)
    volume_change = tensor[0, 0] + tensor[1, 1] + tensor[2, 2]
    identity = jnp.eye(3, dtype=jnp.float32)
    stress = lame_moduli[1][None, None, None, :] * (tensor + tensor.transpose(1, 0, 2, 3))
    stress = stress + identity[:, :, None, None] * (lame_moduli[0][None, :] * volume_change)[None, None]
    mapped = stress[:, 0][:, None] * jacobian[:, 0][None, :, None, :]
    mapped = mapped + stress[:, 1][:, None] * jacobian[:, 1][None, :, None, :]
    mapped = mapped + stress[:, 2][:, None] * jacobian[:, 2][None, :, None, :]
    mapped = mapped * point_weights[None, None]
    node_values = jnp.einsum('mn,cme->cne', shape_grad, mapped.reshape(3, 3 * POINTS, elements),
                             precision=lax.Precision.HIGHEST)
    return jnp.zeros((3, node_count), jnp.float32).at[:, connect].add(node_values)


def split_parts(array, width):
    return array.reshape(array.shape[0], PARTS_SIZE, width).transpose(1, 0, 2)


def assemble_parts(node_field, interface_nodes, neighbours):
    channels = node_field.shape[1]
    picked = jax.vmap(lambda values, shared: jnp.take(values, shared, axis=1))(node_field, interface_nodes)
    picked = picked.reshape(GROUPS, WRITERS, channels, 4, FACE_NODES)
    zero_row = jnp.zeros((1, WRITERS, channels, FACE_NODES), jnp.float32)
    zero_column = jnp.zeros((GROUPS, 1, channels, FACE_NODES), jnp.float32)
    from_below = jnp.concatenate([zero_row, picked[:-1, :, :, 1]], axis=0)
    from_above = jnp.concatenate([picked[1:, :, :, 0], zero_row], axis=0)
    from_left = jnp.concatenate([zero_column, picked[:, :-1, :, 3]], axis=1)
    from_right = jnp.concatenate([picked[:, 1:, :, 2], zero_column], axis=1)
    received = jnp.stack([from_below, from_above, from_left, from_right], axis=3)
    received = received.reshape(PARTS_SIZE, channels, 4, FACE_NODES)
    received = received * neighbours.astype(jnp.float32)[:, None, :, None]
    return jax.vmap(lambda values, shared, incoming: values.at[:, shared].add(incoming))(
        node_field, interface_nodes, received)


def reference(connect, interface_nodes, neighbours, point_rank, shape_grad, inverse_jacobian,
              lame_moduli, point_weights, mass_elem, source_pattern, wavelet):
    connect_parts = split_parts(connect, ELEM_DEV)
    jacobian_parts = split_parts(inverse_jacobian, ELEM_DEV)
    moduli_parts = split_parts(lame_moduli, ELEM_DEV)
    weight_parts = split_parts(point_weights, ELEM_DEV)
    mass_parts = split_parts(mass_elem, ELEM_DEV)
    pattern_parts = split_parts(source_pattern, NODE_DEV)
    node_mass = jax.vmap(lambda connect_part, mass_part: jnp.zeros((1, NODE_DEV), jnp.float32).at[0, connect_part].add(mass_part))(connect_parts, mass_parts)
    inverse_mass = 1.0 / assemble_parts(node_mass, interface_nodes, neighbours)
    gradient_all = jax.vmap(gradient_at, in_axes=(0, 0, None, 0))
    forces_all = jax.vmap(lambda tensor, moduli, weight_part, jacobian_part, connect_part: element_forces(
        tensor, moduli, weight_part, jacobian_part, shape_grad, connect_part, NODE_DEV))

    def advance(loop_state, wave):
        displace, velocity = loop_state
        tensor = gradient_all(displace, connect_parts, shape_grad, jacobian_parts)
        force = wave * pattern_parts - forces_all(tensor, moduli_parts, weight_parts, jacobian_parts, connect_parts)
        force = assemble_parts(force, interface_nodes, neighbours)
        velocity = velocity + time_step * inverse_mass * force
        displace = displace + time_step * velocity
        snapshot = jax.vmap(strain_of)(gradient_all(displace, connect_parts, shape_grad, jacobian_parts))
        snapshot = snapshot.reshape(PARTS_SIZE, STRAIN, PT_DEV).astype(jnp.bfloat16)
        return (displace, velocity), snapshot

    start = jnp.zeros((PARTS_SIZE, 3, NODE_DEV), jnp.float32)
    unused, snapshots = lax.scan(advance, (start, start), wavelet)
    inverse_rank = jax.vmap(lambda ranking: jnp.zeros((PT_DEV,), jnp.int32).at[ranking].set(
        jnp.arange(PT_DEV, dtype=jnp.int32)))(point_rank)
    ordered = jax.vmap(lambda values, positions: jnp.take(values, positions, axis=2),
                       in_axes=(1, 0), out_axes=1)(snapshots, inverse_rank)
    per_writer = PT_DEV // WRITERS
    ordered = ordered.reshape(STEPS, GROUPS, WRITERS, STRAIN, WRITERS, per_writer).transpose(0, 3, 1, 4, 2, 5)
    return ordered.reshape(STEPS, STRAIN, PARTS_SIZE * PT_DEV)
```

```python
import functools

import jax
import jax.numpy as jnp
from jax import lax
from jax.experimental import pallas as pl
from jax.experimental.pallas import tpu as pltpu
from jax.sharding import PartitionSpec as P


EL_NODES = 20
NODE_ROWS = 24
POINTS = 16
STRAIN = 6
STEPS = 16
LANES = 128
FACES = 4

time_step = 0.5

EXCHANGES = ("dom1", "grp1", "dom0", "grp0")

VMEM = pl.BlockSpec(memory_space=pltpu.VMEM)
SMEM = pl.BlockSpec(memory_space=pltpu.SMEM)


def kernel_call(body, outs, n_in, smem=(), scratch=()):
    return pl.pallas_call(
        body,
        out_shape=outs,
        in_specs=[SMEM if i in smem else VMEM for i in range(n_in)],
        out_specs=[VMEM] * len(outs),
        scratch_shapes=list(scratch),
        compiler_params=pltpu.CompilerParams(vmem_limit_bytes=24 * 1024 * 1024),
    )


def parts_of(x):
    high = x.astype(jnp.bfloat16).astype(jnp.float32)
    rest = x - high
    middle = rest.astype(jnp.bfloat16).astype(jnp.float32)
    low = (rest - middle).astype(jnp.bfloat16).astype(jnp.float32)
    return high, middle, low


def matmul(left, right):
    return jnp.dot(left, right, preferred_element_type=jnp.float32)


def lane_gather(row, index):
    return jnp.take_along_axis(row, index, axis=1)


def pick_lanes(field, index):
    low = jnp.bitwise_and(index, LANES - 1)
    chunk = jnp.right_shift(index, 7)
    out = lane_gather(field[:, 0:LANES], low)
    for j in range(1, field.shape[1] // LANES):
        out = jnp.where(
            chunk == j, lane_gather(field[:, j * LANES : (j + 1) * LANES], low), out
        )
    return out


def spread(received, inverse):
    out = []
    for j in range(inverse.shape[1] // LANES):
        index = inverse[:, j * LANES : (j + 1) * LANES]
        taken = lane_gather(received, jnp.maximum(index, 0))
        out.append(jnp.where(index >= 0, taken, 0.0))
    return jnp.concatenate(out, axis=1)


def merge_received(source, dom1, grp1, dom0, grp0):
    out = jnp.where(source == 0, grp0, grp1)
    out = jnp.where(source == 2, dom0, out)
    return jnp.where(source == 3, dom1, out)


def scatter_nodes(rows, incidence):
    left = jnp.concatenate(parts_of(rows), axis=0).astype(jnp.bfloat16)
    sums = matmul(left, incidence)
    return (sums[16:24] + sums[8:16]) + sums[0:8]


def prepare_kernel(
    connect,
    lists,
    swapped,
    active,
    mass_elem,
    source_pattern,
    incidence,
    field,
    send,
    pick_index,
    inverse_index,
):
    nodes = source_pattern.shape[1]
    lane = lax.broadcasted_iota(jnp.int32, (LANES, nodes), 1)
    for n in range(EL_NODES):
        column = jnp.broadcast_to(connect[n : n + 1, :], (LANES, LANES)).T
        wide = jnp.concatenate([column] * (nodes // LANES), axis=1)
        incidence[n * LANES : (n + 1) * LANES, :] = jnp.where(wide == lane, 1.0, 0.0).astype(
            jnp.bfloat16
        )
    listed = jnp.where(active[...] != 0, lists[...], -1)
    column = jnp.broadcast_to(listed, (LANES, LANES)).T
    wide = jnp.concatenate([column] * (nodes // LANES), axis=1)
    slot = lax.broadcasted_iota(jnp.int32, (LANES, nodes), 0) + 1
    found = jnp.sum(jnp.where(wide == lane, slot, 0), axis=0, keepdims=True)
    inverse_index[...] = jnp.broadcast_to(found - 1, (8, nodes))
    index = jnp.broadcast_to(swapped[...], (8, LANES))
    pick_index[...] = index
    rows = jnp.concatenate(
        [jnp.broadcast_to(mass_elem[n : n + 1, :], (8, LANES)) for n in range(EL_NODES)], axis=1
    )
    field[...] = scatter_nodes(rows, incidence[...])
    field[0:3, :] = source_pattern[...]
    send[...] = pick_lanes(field[...], index)


def strain_and_force(
    displace,
    strain,
    connect,
    left_gradient,
    left_force,
    inverse_jacobian,
    lame_moduli,
    point_weights,
    incidence,
    need_force,
):
    index = connect[...]
    low = jnp.bitwise_and(index, LANES - 1)
    chunk = jnp.right_shift(index, 7)
    is_chunk = [chunk == j for j in range(1, displace.shape[1] // LANES)]
    columns = []
    for c in range(3):
        pieces = []
        for b in range(NODE_ROWS // 8):
            rows = slice(8 * b, 8 * b + 8)
            out = None
            for j in range(displace.shape[1] // LANES):
                row = jnp.broadcast_to(displace[c : c + 1, j * LANES : (j + 1) * LANES], (8, LANES))
                taken = lane_gather(row, low[rows])
                out = taken if j == 0 else jnp.where(is_chunk[j - 1][rows], taken, out)
            pieces.append(out)
        columns.append(jnp.concatenate(pieces, axis=0))
    node_values = jnp.concatenate(columns, axis=1)
    right = jnp.concatenate(parts_of(node_values), axis=0).astype(jnp.bfloat16)
    sums = matmul(left_gradient[...], right)
    height = 3 * POINTS
    along = (sums[2 * height :] + sums[height : 2 * height]) + sums[0:height]
    jac = [inverse_jacobian[i : i + 1, :] for i in range(9)]

    def ref_derivative(c, r):
        return along[r * POINTS : (r + 1) * POINTS, c * LANES : (c + 1) * LANES]

    grad = [
        [
            (ref_derivative(c, 0) * jac[d] + ref_derivative(c, 1) * jac[3 + d])
            + ref_derivative(c, 2) * jac[6 + d]
            for d in range(3)
        ]
        for c in range(3)
    ]
    shear = {(c, d): grad[c][d] + grad[d][c] for c, d in ((1, 2), (0, 2), (0, 1))}
    rows = [grad[0][0], grad[1][1], grad[2][2]] + [0.5 * shear[k] for k in ((1, 2), (0, 2), (0, 1))]
    for s in range(STRAIN):
        strain[s * POINTS : (s + 1) * POINTS, :] = rows[s]
    if not need_force:
        return None
    volume = (grad[0][0] + grad[1][1]) + grad[2][2]
    weights = point_weights[...]
    shear_scale = lame_moduli[1:2, :] * weights
    pressure = (lame_moduli[0:1, :] * weights) * volume
    stress = [[None] * 3 for _ in range(3)]
    for c in range(3):
        for d in range(3):
            if c == d:
                stress[c][d] = shear_scale * (grad[c][c] + grad[c][c]) + pressure
            else:
                stress[c][d] = shear_scale * shear[(min(c, d), max(c, d))]
    columns = []
    for c in range(3):
        mapped = [
            (stress[c][0] * jac[3 * r] + stress[c][1] * jac[3 * r + 1])
            + stress[c][2] * jac[3 * r + 2]
            for r in range(3)
        ]
        columns.append(jnp.concatenate(mapped, axis=0))
    mapped = jnp.concatenate(columns, axis=1)
    right = jnp.concatenate(parts_of(mapped), axis=0).astype(jnp.bfloat16)
    sums = matmul(left_force[...], right)
    node_forces = (sums[2 * NODE_ROWS :] + sums[NODE_ROWS : 2 * NODE_ROWS]) + sums[0:NODE_ROWS]
    row_id = lax.broadcasted_iota(jnp.int32, (8, LANES), 0)
    pieces = []
    for n in range(EL_NODES):
        first, second, third = (
            jnp.broadcast_to(node_forces[n : n + 1, c * LANES : (c + 1) * LANES], (8, LANES))
            for c in range(3)
        )
        pieces.append(jnp.where(row_id == 0, first, jnp.where(row_id == 1, second, third)))
    return scatter_nodes(jnp.concatenate(pieces, axis=1), incidence[...])


def first_kernel(
    wavelet,
    dom1,
    grp1,
    dom0,
    grp0,
    source,
    inverse_index,
    pick_index,
    field,
    connect,
    left_gradient,
    left_force,
    inverse_jacobian,
    lame_moduli,
    point_weights,
    incidence,
    strain,
    displace,
    velocity,
    pattern,
    half_inverse_mass,
    force,
    send,
):
    received = merge_received(source[...], dom1[...], grp1[...], dom0[...], grp0[...])
    total = field[...] + spread(received, inverse_index[...])
    scale = jnp.broadcast_to(time_step * (1.0 / total[3:4, :]), total.shape)
    pattern[...] = total
    half_inverse_mass[...] = scale
    new_velocity = scale * (wavelet[0] * total)
    velocity[...] = new_velocity
    new_displace = time_step * new_velocity
    displace[...] = new_displace
    new_force = strain_and_force(
        new_displace,
        strain,
        connect,
        left_gradient,
        left_force,
        inverse_jacobian,
        lame_moduli,
        point_weights,
        incidence,
        True,
    )
    force[...] = new_force
    send[...] = pick_lanes(new_force, pick_index[...])


def step_kernel(
    step,
    wavelet,
    dom1,
    grp1,
    dom0,
    grp0,
    source,
    inverse_index,
    pick_index,
    connect,
    left_gradient,
    left_force,
    inverse_jacobian,
    lame_moduli,
    point_weights,
    incidence,
    pattern,
    half_inverse_mass,
    old_displace,
    old_velocity,
    old_force,
    strain,
    *rest,
):
    received = merge_received(source[...], dom1[...], grp1[...], dom0[...], grp0[...])
    stiff = old_force[...] + spread(received, inverse_index[...])
    total = wavelet[step] * pattern[...] - stiff
    new_velocity = old_velocity[...] + half_inverse_mass[...] * total
    new_displace = old_displace[...] + time_step * new_velocity
    new_force = strain_and_force(
        new_displace,
        strain,
        connect,
        left_gradient,
        left_force,
        inverse_jacobian,
        lame_moduli,
        point_weights,
        incidence,
        bool(rest),
    )
    if rest:
        displace, velocity, force, send = rest
        displace[...] = new_displace
        velocity[...] = new_velocity
        force[...] = new_force
        send[...] = pick_lanes(new_force, pick_index[...])


def order_kernel(rank, *refs):
    strains, out, store = refs[:STEPS], refs[STEPS], refs[STEPS + 1]
    per_step = STRAIN * POINTS
    for t in range(STEPS):
        store[t * per_step : (t + 1) * per_step, :] = strains[t][...]
    count = rank.shape[0] * LANES
    lane = lax.broadcasted_iota(jnp.int32, (LANES, count), 1)
    total = None
    for q in range(POINTS):
        values = store[pl.ds(q, STEPS * STRAIN, stride=POINTS), :].astype(jnp.bfloat16)
        column = jnp.broadcast_to(rank[q : q + 1, :], (LANES, LANES)).T
        wide = jnp.concatenate([column] * (count // LANES), axis=1)
        chosen = jnp.where(wide == lane, 1.0, 0.0).astype(jnp.bfloat16)
        part = matmul(values, chosen)
        total = part if total is None else total + part
    for w in range(count // LANES):
        out[w] = total[:, w * LANES : (w + 1) * LANES].astype(jnp.bfloat16)


def place_kernel(pieces, out, store):
    writers = pieces.shape[0]
    for w in range(writers):
        store[:, w * LANES : (w + 1) * LANES] = pieces[w].astype(jnp.float32)
    for t in range(STEPS):
        out[t] = store[t * STRAIN : (t + 1) * STRAIN, :].astype(jnp.bfloat16)


def rounded(x):
    return lax.reduce_precision(x, 8, 7)


def left_operand(matrix, rows, columns):
    padded = jnp.pad(matrix, ((0, rows - matrix.shape[0]), (0, columns - matrix.shape[1])))
    high = rounded(padded)
    middle = rounded(padded - high)
    low = rounded(padded - high - middle)
    zero = jnp.zeros_like(padded)
    blocks = [[high, high, high], [middle, middle, zero], [low, zero, zero]]
    return jnp.block(blocks).astype(jnp.bfloat16)


def shards(
    connect,
    interface_nodes,
    neighbours,
    point_rank,
    shape_grad,
    inverse_jacobian,
    lame_moduli,
    point_weights,
    mass_elem,
    source_pattern,
    wavelet,
):
    nodes = source_pattern.shape[1]
    f32 = jnp.float32
    field_t = jax.ShapeDtypeStruct((8, nodes), f32)
    lanes_t = jax.ShapeDtypeStruct((8, LANES), f32)
    index_t = jax.ShapeDtypeStruct((8, LANES), jnp.int32)
    strain_t = jax.ShapeDtypeStruct((STRAIN * POINTS, LANES), f32)

    lists = interface_nodes.reshape(1, LANES)
    swapped = interface_nodes.reshape(2, 2, LANES // 4)[:, ::-1].reshape(1, LANES)
    active = jnp.repeat(neighbours, LANES // FACES, axis=1)
    face = lax.broadcasted_iota(jnp.int32, (8, LANES), 1) // (LANES // FACES)
    parity = jnp.where(face < 2, lax.axis_index("grp") % 2, lax.axis_index("dom") % 2)
    source = 2 * (face // 2) + jnp.bitwise_xor(parity, 1 - face % 2)
    left_gradient = left_operand(shape_grad, 3 * POINTS, NODE_ROWS)
    left_force = left_operand(shape_grad.T, NODE_ROWS, 3 * POINTS)
    padded_connect = jnp.pad(connect, ((0, NODE_ROWS - EL_NODES), (0, 0)))

    def exchange(send):
        received = []
        for name in EXCHANGES:
            axis, offset = name[:3], int(name[3])
            count = lax.axis_size(axis)
            pairs = []
            for i in range(offset, count - 1, 2):
                pairs += [(i, i + 1), (i + 1, i)]
            received.append(lax.ppermute(send, axis, pairs))
        return received

    incidence, field, send, pick_index, inverse_index = kernel_call(
        prepare_kernel,
        [
            jax.ShapeDtypeStruct((EL_NODES * LANES, nodes), jnp.bfloat16),
            field_t,
            lanes_t,
            index_t,
            jax.ShapeDtypeStruct((8, nodes), jnp.int32),
        ],
        6,
    )(connect, lists, swapped, active, mass_elem, source_pattern)
    element_data = (
        padded_connect,
        left_gradient,
        left_force,
        inverse_jacobian,
        lame_moduli,
        point_weights,
        incidence,
    )
    received = exchange(send)
    strain, displace, velocity, pattern, half_inverse_mass, force, send = kernel_call(
        first_kernel,
        [strain_t, field_t, field_t, field_t, field_t, field_t, lanes_t],
        16,
        smem=(0,),
    )(wavelet, *received, source, inverse_index, pick_index, field, *element_data)
    strains = [strain]
    for step in range(1, STEPS):
        received = exchange(send)
        last = step == STEPS - 1
        outs = kernel_call(
            functools.partial(step_kernel, step),
            [strain_t] + ([] if last else [field_t, field_t, field_t, lanes_t]),
            20,
            smem=(0,),
        )(
            wavelet,
            *received,
            source,
            inverse_index,
            pick_index,
            *element_data,
            pattern,
            half_inverse_mass,
            displace,
            velocity,
            force,
        )
        strains.append(outs[0])
        if not last:
            displace, velocity, force, send = outs[1:]
    writers = lax.axis_size("dom")
    (ordered,) = kernel_call(
        order_kernel,
        [jax.ShapeDtypeStruct((writers, STEPS * STRAIN, LANES), jnp.bfloat16)],
        1 + STEPS,
        scratch=[pltpu.VMEM((STEPS * STRAIN * POINTS, LANES), f32)],
    )(point_rank.reshape(POINTS, LANES), *strains)
    pieces = lax.all_to_all(ordered, "dom", split_axis=0, concat_axis=0, tiled=True)
    (placed,) = kernel_call(
        place_kernel,
        [jax.ShapeDtypeStruct((STEPS, STRAIN, writers * LANES), jnp.bfloat16)],
        1,
        scratch=[pltpu.VMEM((STEPS * STRAIN, writers * LANES), f32)],
    )(pieces)
    return placed


def solution(mesh):
    placed = (
        P(None, ("grp", "dom")),
        P(("grp", "dom"), None, None),
        P(("grp", "dom"), None),
        P(("grp", "dom"), None),
        P(),
        P(None, ("grp", "dom")),
        P(None, ("grp", "dom")),
        P(None, ("grp", "dom")),
        P(None, ("grp", "dom")),
        P(None, ("grp", "dom")),
        P(),
    )
    return jax.shard_map(
        shards, mesh=mesh, in_specs=placed, out_specs=P(None, None, ("grp", "dom")), check_vma=False
    )
```

```python
import functools

import jax
import jax.numpy as jnp
from jax import lax
from jax.experimental import pallas as pl
from jax.experimental.pallas import tpu as pltpu
from jax.sharding import PartitionSpec as P


EL_NODES = 20
NODE_ROWS = 24
POINTS = 16
STRAIN = 6
STEPS = 16
LANES = 128
FACES = 4
GRADIENT_BLOCK = 32
FORCE_BLOCK = 64

time_step = 0.5

EXCHANGES = ("dom1", "grp1", "dom0", "grp0")

VMEM = pl.BlockSpec(memory_space=pltpu.VMEM)
HBM = pl.BlockSpec(memory_space=pltpu.MemorySpace.HBM)


def kernel_call(body, outs, specs, scratch=()):
    return pl.pallas_call(
        body,
        out_shape=outs,
        in_specs=specs,
        out_specs=[VMEM] * len(outs),
        scratch_shapes=list(scratch),
        compiler_params=pltpu.CompilerParams(vmem_limit_bytes=24 * 1024 * 1024),
    )


def parts_of(x):
    high = x.astype(jnp.bfloat16).astype(jnp.float32)
    rest = x - high
    middle = rest.astype(jnp.bfloat16).astype(jnp.float32)
    low = (rest - middle).astype(jnp.bfloat16).astype(jnp.float32)
    return high, middle, low


def matmul(left, right):
    return jnp.dot(left, right, preferred_element_type=jnp.float32)


def lane_gather(row, index):
    return jnp.take_along_axis(row, index, axis=1)


def pick_lanes(field, index):
    low = jnp.bitwise_and(index, LANES - 1)
    chunk = jnp.right_shift(index, 7)
    out = lane_gather(field[:, 0:LANES], low)
    for j in range(1, field.shape[1] // LANES):
        out = jnp.where(
            chunk == j, lane_gather(field[:, j * LANES : (j + 1) * LANES], low), out
        )
    return out


def spread(received, inverse):
    out = []
    for j in range(inverse.shape[1] // LANES):
        index = inverse[:, j * LANES : (j + 1) * LANES]
        taken = lane_gather(received, jnp.maximum(index, 0))
        out.append(jnp.where(index >= 0, taken, 0.0))
    return jnp.concatenate(out, axis=1)


def merge_received(source, dom1, grp1, dom0, grp0):
    out = jnp.where(source == 0, grp0, grp1)
    out = jnp.where(source == 2, dom0, out)
    return jnp.where(source == 3, dom1, out)


def scatter_nodes(rows, incidence):
    left = jnp.concatenate(parts_of(rows), axis=0).astype(jnp.bfloat16)
    sums = matmul(left, incidence)
    return (sums[16:24] + sums[8:16]) + sums[0:8]


def prepare_kernel(
    wavelet_in,
    neighbours_in,
    connect_in,
    lists_in,
    mass_in,
    source_in,
    shape_in,
    jacobian_in,
    lame_in,
    weights_in,
    rank_in,
    incidence,
    field,
    send,
    pick_index,
    inverse_index,
    connect,
    left_gradient,
    left_force,
    wave,
    inverse_jacobian,
    lame_moduli,
    point_weights,
    rank,
    element_nodes,
    wavelet,
    neighbours,
    lists,
    mass_elem,
    source_pattern,
    shape_t,
    sems,
):
    moves = [
        (connect_in, element_nodes),
        (wavelet_in, wavelet),
        (neighbours_in, neighbours),
        (lists_in, lists),
        (mass_in, mass_elem),
        (source_in, source_pattern),
        (shape_in, shape_t),
        (jacobian_in, inverse_jacobian),
        (lame_in, lame_moduli),
        (weights_in, point_weights),
        (rank_in, rank),
    ]
    copies = [pltpu.make_async_copy(a, b, sems.at[i]) for i, (a, b) in enumerate(moves)]
    for copy in copies:
        copy.start()
    copies[0].wait()
    nodes = field.shape[1]
    connect[...] = jnp.zeros(connect.shape, jnp.int32)
    connect[0:EL_NODES, :] = element_nodes[...]
    lane = lax.broadcasted_iota(jnp.int32, (LANES, nodes), 1)
    for n in range(EL_NODES):
        column = jnp.broadcast_to(element_nodes[n : n + 1, :], (LANES, LANES)).T
        wide = jnp.concatenate([column] * (nodes // LANES), axis=1)
        incidence[n * LANES : (n + 1) * LANES, :] = jnp.where(wide == lane, 1.0, 0.0).astype(
            jnp.bfloat16
        )
    for copy in copies[1:]:
        copy.wait()
    wave[...] = jnp.concatenate(
        [jnp.full((1, LANES), wavelet[t], jnp.float32) for t in range(STEPS)], axis=0
    )
    face = [lists[0, k : k + 1, :] for k in range(FACES)]
    listed = jnp.concatenate(face, axis=1)
    swapped = jnp.concatenate([face[1], face[0], face[3], face[2]], axis=1)
    side = lax.broadcasted_iota(jnp.int32, (1, LANES), 1) // (LANES // FACES)
    open_side = jnp.where(
        side < 2,
        jnp.where(side == 0, neighbours[0, 0], neighbours[0, 1]),
        jnp.where(side == 2, neighbours[0, 2], neighbours[0, 3]),
    )
    listed = jnp.where(open_side != 0, listed, -1)
    column = jnp.broadcast_to(listed, (LANES, LANES)).T
    wide = jnp.concatenate([column] * (nodes // LANES), axis=1)
    slot = lax.broadcasted_iota(jnp.int32, (LANES, nodes), 0) + 1
    found = jnp.sum(jnp.where(wide == lane, slot, 0), axis=0, keepdims=True)
    inverse_index[...] = jnp.broadcast_to(found - 1, (8, nodes))
    index = jnp.broadcast_to(swapped, (8, LANES))
    pick_index[...] = index
    rows = jnp.concatenate(
        [jnp.broadcast_to(mass_elem[n : n + 1, :], (8, LANES)) for n in range(EL_NODES)], axis=1
    )
    field[...] = scatter_nodes(rows, incidence[...])
    field[0:3, :] = source_pattern[...]
    send[...] = pick_lanes(field[...], index)

    reference_rows = 3 * POINTS
    shape_rows = jnp.concatenate(
        [shape_t[...], jnp.zeros((EL_NODES, LANES - reference_rows), jnp.float32)], axis=1
    )
    shape_rows = jnp.concatenate(
        [shape_rows, jnp.zeros((LANES - EL_NODES, LANES), jnp.float32)], axis=0
    )
    forward = parts_of(shape_rows.T[0:reference_rows, :])
    for j in range(3):
        block = forward[j]
        for i in range(1, 3 - j):
            block = block + pltpu.roll(forward[j], i * GRADIENT_BLOCK, 1)
        left_gradient[j * reference_rows : (j + 1) * reference_rows, :] = block[
            :, 0 : 3 * GRADIENT_BLOCK
        ].astype(jnp.bfloat16)
    backward = parts_of(shape_rows[0:NODE_ROWS, :])
    firsts, seconds = [], []
    for j in range(3):
        block = backward[j]
        firsts.append(block if j == 2 else block + pltpu.roll(block, FORCE_BLOCK, 1))
        seconds.append(block if j == 0 else jnp.zeros_like(block))
    left_force[:, 0:LANES] = jnp.concatenate(firsts, axis=0).astype(jnp.bfloat16)
    left_force[:, LANES:] = jnp.concatenate(seconds, axis=0)[:, 0:FORCE_BLOCK].astype(jnp.bfloat16)


def stacked_parts(x, height):
    gap = height - x.shape[0]
    pieces = []
    for part in parts_of(x):
        pieces += [part, jnp.zeros((gap, x.shape[1]), jnp.float32)]
    return jnp.concatenate(pieces, axis=0).astype(jnp.bfloat16)


def wave_row(wave, step, width):
    return jnp.concatenate([wave[step : step + 1, :]] * (width // LANES), axis=1)


def strain_and_force(
    displace,
    strain,
    connect,
    left_gradient,
    left_force,
    inverse_jacobian,
    lame_moduli,
    point_weights,
    incidence,
    need_force,
):
    index = connect[...]
    low = jnp.bitwise_and(index, LANES - 1)
    chunk = jnp.right_shift(index, 7)
    is_chunk = [chunk == j for j in range(1, displace.shape[1] // LANES)]
    columns = []
    for c in range(3):
        pieces = []
        for b in range(NODE_ROWS // 8):
            rows = slice(8 * b, 8 * b + 8)
            out = None
            for j in range(displace.shape[1] // LANES):
                row = jnp.broadcast_to(displace[c : c + 1, j * LANES : (j + 1) * LANES], (8, LANES))
                taken = lane_gather(row, low[rows])
                out = taken if j == 0 else jnp.where(is_chunk[j - 1][rows], taken, out)
            pieces.append(out)
        columns.append(jnp.concatenate(pieces, axis=0))
    node_values = jnp.concatenate(columns, axis=1)
    right = stacked_parts(node_values, GRADIENT_BLOCK)
    sums = matmul(left_gradient[...], right)
    height = 3 * POINTS
    along = (sums[2 * height :] + sums[height : 2 * height]) + sums[0:height]
    jac = [inverse_jacobian[i : i + 1, :] for i in range(9)]

    def ref_derivative(c, r):
        return along[r * POINTS : (r + 1) * POINTS, c * LANES : (c + 1) * LANES]

    grad = [
        [
            (ref_derivative(c, 0) * jac[d] + ref_derivative(c, 1) * jac[3 + d])
            + ref_derivative(c, 2) * jac[6 + d]
            for d in range(3)
        ]
        for c in range(3)
    ]
    shear = {(c, d): grad[c][d] + grad[d][c] for c, d in ((1, 2), (0, 2), (0, 1))}
    rows = [grad[0][0], grad[1][1], grad[2][2]] + [0.5 * shear[k] for k in ((1, 2), (0, 2), (0, 1))]
    for s in range(STRAIN):
        strain[s * POINTS : (s + 1) * POINTS, :] = rows[s]
    if not need_force:
        return None
    volume = (grad[0][0] + grad[1][1]) + grad[2][2]
    weights = point_weights[...]
    shear_scale = lame_moduli[1:2, :] * weights
    pressure = (lame_moduli[0:1, :] * weights) * volume
    stress = [[None] * 3 for _ in range(3)]
    for c in range(3):
        for d in range(3):
            if c == d:
                stress[c][d] = shear_scale * (grad[c][c] + grad[c][c]) + pressure
            else:
                stress[c][d] = shear_scale * shear[(min(c, d), max(c, d))]
    columns = []
    for c in range(3):
        mapped = [
            (stress[c][0] * jac[3 * r] + stress[c][1] * jac[3 * r + 1])
            + stress[c][2] * jac[3 * r + 2]
            for r in range(3)
        ]
        columns.append(jnp.concatenate(mapped, axis=0))
    mapped = jnp.concatenate(columns, axis=1)
    right = stacked_parts(mapped, FORCE_BLOCK)
    sums = matmul(left_force[...], right)
    node_forces = (sums[2 * NODE_ROWS :] + sums[NODE_ROWS : 2 * NODE_ROWS]) + sums[0:NODE_ROWS]
    row_id = lax.broadcasted_iota(jnp.int32, (8, LANES), 0)
    pieces = []
    for n in range(EL_NODES):
        first, second, third = (
            jnp.broadcast_to(node_forces[n : n + 1, c * LANES : (c + 1) * LANES], (8, LANES))
            for c in range(3)
        )
        pieces.append(jnp.where(row_id == 0, first, jnp.where(row_id == 1, second, third)))
    return scatter_nodes(jnp.concatenate(pieces, axis=1), incidence[...])


def first_kernel(
    wave,
    dom1,
    grp1,
    dom0,
    grp0,
    source,
    inverse_index,
    pick_index,
    field,
    connect,
    left_gradient,
    left_force,
    inverse_jacobian,
    lame_moduli,
    point_weights,
    incidence,
    strain,
    displace,
    velocity,
    pattern,
    half_inverse_mass,
    force,
    send,
):
    received = merge_received(source[...], dom1[...], grp1[...], dom0[...], grp0[...])
    total = field[...] + spread(received, inverse_index[...])
    scale = jnp.broadcast_to(time_step * (1.0 / total[3:4, :]), total.shape)
    pattern[...] = total
    half_inverse_mass[...] = scale
    new_velocity = scale * (wave_row(wave, 0, total.shape[1]) * total)
    velocity[...] = new_velocity
    new_displace = time_step * new_velocity
    displace[...] = new_displace
    new_force = strain_and_force(
        new_displace,
        strain,
        connect,
        left_gradient,
        left_force,
        inverse_jacobian,
        lame_moduli,
        point_weights,
        incidence,
        True,
    )
    force[...] = new_force
    send[...] = pick_lanes(new_force, pick_index[...])


def step_kernel(
    step,
    wave,
    dom1,
    grp1,
    dom0,
    grp0,
    source,
    inverse_index,
    pick_index,
    connect,
    left_gradient,
    left_force,
    inverse_jacobian,
    lame_moduli,
    point_weights,
    incidence,
    pattern,
    half_inverse_mass,
    old_displace,
    old_velocity,
    old_force,
    strain,
    *rest,
):
    received = merge_received(source[...], dom1[...], grp1[...], dom0[...], grp0[...])
    stiff = old_force[...] + spread(received, inverse_index[...])
    total = wave_row(wave, step, stiff.shape[1]) * pattern[...] - stiff
    new_velocity = old_velocity[...] + half_inverse_mass[...] * total
    new_displace = old_displace[...] + time_step * new_velocity
    new_force = strain_and_force(
        new_displace,
        strain,
        connect,
        left_gradient,
        left_force,
        inverse_jacobian,
        lame_moduli,
        point_weights,
        incidence,
        bool(rest),
    )
    if rest:
        displace, velocity, force, send = rest
        displace[...] = new_displace
        velocity[...] = new_velocity
        force[...] = new_force
        send[...] = pick_lanes(new_force, pick_index[...])


def order_kernel(rank, *refs):
    strains, out, store = refs[:STEPS], refs[STEPS], refs[STEPS + 1]
    for t in range(STEPS):
        for c in range(STRAIN):
            row = (c * STEPS + t) * POINTS
            store[row : row + POINTS, :] = strains[t][c * POINTS : (c + 1) * POINTS, :]
    count = rank.shape[0] * LANES
    lane = lax.broadcasted_iota(jnp.int32, (LANES, count), 1)
    total = None
    for q in range(POINTS):
        values = store[pl.ds(q, STEPS * STRAIN, stride=POINTS), :].astype(jnp.bfloat16)
        column = jnp.broadcast_to(rank[q : q + 1, :], (LANES, LANES)).T
        wide = jnp.concatenate([column] * (count // LANES), axis=1)
        chosen = jnp.where(wide == lane, 1.0, 0.0).astype(jnp.bfloat16)
        part = matmul(values, chosen)
        total = part if total is None else total + part
    for w in range(count // LANES):
        out[w] = total[:, w * LANES : (w + 1) * LANES].astype(jnp.bfloat16)


def place_kernel(pieces, out):
    for w in range(pieces.shape[0]):
        for c in range(STRAIN):
            out[c, :, w * LANES : (w + 1) * LANES] = pieces[w, c * STEPS : (c + 1) * STEPS, :]


def shards(
    connect,
    interface_nodes,
    neighbours,
    point_rank,
    shape_grad,
    inverse_jacobian,
    lame_moduli,
    point_weights,
    mass_elem,
    source_pattern,
    wavelet,
):
    nodes = source_pattern.shape[1]
    f32 = jnp.float32
    field_t = jax.ShapeDtypeStruct((8, nodes), f32)
    lanes_t = jax.ShapeDtypeStruct((8, LANES), f32)
    index_t = jax.ShapeDtypeStruct((8, LANES), jnp.int32)
    strain_t = jax.ShapeDtypeStruct((STRAIN * POINTS, LANES), f32)

    face = lax.broadcasted_iota(jnp.int32, (8, LANES), 1) // (LANES // FACES)
    parity = jnp.where(face < 2, lax.axis_index("grp") % 2, lax.axis_index("dom") % 2)
    source = 2 * (face // 2) + jnp.bitwise_xor(parity, 1 - face % 2)

    def exchange(send):
        received = []
        for name in EXCHANGES:
            axis, offset = name[:3], int(name[3])
            count = lax.axis_size(axis)
            pairs = []
            for i in range(offset, count - 1, 2):
                pairs += [(i, i + 1), (i + 1, i)]
            received.append(lax.ppermute(send, axis, pairs))
        return received

    i32, bf16 = jnp.int32, jnp.bfloat16
    rank_rows = point_rank.reshape(POINTS, LANES)
    outs = kernel_call(
        prepare_kernel,
        [
            jax.ShapeDtypeStruct((EL_NODES * LANES, nodes), bf16),
            field_t,
            lanes_t,
            index_t,
            jax.ShapeDtypeStruct((8, nodes), i32),
            jax.ShapeDtypeStruct((NODE_ROWS, LANES), i32),
            jax.ShapeDtypeStruct((9 * POINTS, 3 * GRADIENT_BLOCK), bf16),
            jax.ShapeDtypeStruct((3 * NODE_ROWS, 3 * FORCE_BLOCK), bf16),
            jax.ShapeDtypeStruct((STEPS, LANES), f32),
            jax.ShapeDtypeStruct(inverse_jacobian.shape, f32),
            jax.ShapeDtypeStruct(lame_moduli.shape, f32),
            jax.ShapeDtypeStruct(point_weights.shape, f32),
            jax.ShapeDtypeStruct(rank_rows.shape, i32),
        ],
        [HBM] * 11,
        scratch=[
            pltpu.VMEM(connect.shape, i32),
            pltpu.SMEM(wavelet.shape, f32),
            pltpu.SMEM(neighbours.shape, i32),
            pltpu.VMEM(interface_nodes.shape, i32),
            pltpu.VMEM(mass_elem.shape, f32),
            pltpu.VMEM(source_pattern.shape, f32),
            pltpu.VMEM(shape_grad.T.shape, f32),
            pltpu.SemaphoreType.DMA((11,)),
        ],
    )(
        *(
            pltpu.with_memory_space_constraint(x, pltpu.MemorySpace.HBM)
            for x in (
                wavelet,
                neighbours,
                connect,
                interface_nodes,
                mass_elem,
                source_pattern,
                shape_grad.T,
                inverse_jacobian,
                lame_moduli,
                point_weights,
                rank_rows,
            )
        ),
    )
    incidence, field, send, pick_index, inverse_index = outs[:5]
    wave, rank = outs[8], outs[12]
    element_data = (*outs[5:8], *outs[9:12], incidence)
    received = exchange(send)
    strain, displace, velocity, pattern, half_inverse_mass, force, send = kernel_call(
        first_kernel, [strain_t, field_t, field_t, field_t, field_t, field_t, lanes_t], [VMEM] * 16
    )(wave, *received, source, inverse_index, pick_index, field, *element_data)
    strains = [strain]
    for step in range(1, STEPS):
        received = exchange(send)
        last = step == STEPS - 1
        outs = kernel_call(
            functools.partial(step_kernel, step),
            [strain_t] + ([] if last else [field_t, field_t, field_t, lanes_t]),
            [VMEM] * 20,
        )(
            wave,
            *received,
            source,
            inverse_index,
            pick_index,
            *element_data,
            pattern,
            half_inverse_mass,
            displace,
            velocity,
            force,
        )
        strains.append(outs[0])
        if not last:
            displace, velocity, force, send = outs[1:]
    writers = lax.axis_size("dom")
    (ordered,) = kernel_call(
        order_kernel,
        [jax.ShapeDtypeStruct((writers, STEPS * STRAIN, LANES), jnp.bfloat16)],
        [VMEM] * (1 + STEPS),
        scratch=[pltpu.VMEM((STEPS * STRAIN * POINTS, LANES), f32)],
    )(rank, *strains)
    pieces = lax.all_to_all(ordered, "dom", split_axis=0, concat_axis=0, tiled=True)
    (placed,) = kernel_call(
        place_kernel, [jax.ShapeDtypeStruct((STRAIN, STEPS, writers * LANES), jnp.bfloat16)], [VMEM]
    )(pieces)
    return placed.transpose(1, 0, 2)


def solution(mesh):
    placed = (
        P(None, ("grp", "dom")),
        P(("grp", "dom"), None, None),
        P(("grp", "dom"), None),
        P(("grp", "dom"), None),
        P(),
        P(None, ("grp", "dom")),
        P(None, ("grp", "dom")),
        P(None, ("grp", "dom")),
        P(None, ("grp", "dom")),
        P(None, ("grp", "dom")),
        P(),
    )
    return jax.shard_map(
        shards, mesh=mesh, in_specs=placed, out_specs=P(None, None, ("grp", "dom")), check_vma=False
    )
```

```python
import functools

import jax
import jax.numpy as jnp
from jax import lax
from jax.experimental import pallas as pl
from jax.experimental.pallas import tpu as pltpu
from jax.sharding import PartitionSpec as P


EL_NODES = 20
NODE_ROWS = 24
POINTS = 16
STRAIN = 6
STEPS = 16
LANES = 128
FACES = 4
GRADIENT_BLOCK = 32
FORCE_BLOCK = 64

time_step = 0.5

DOM_ROW = 4

EXCHANGES = ("dom1", "grp1", "dom0", "grp0")

VMEM = pl.BlockSpec(memory_space=pltpu.VMEM)
HBM = pl.BlockSpec(memory_space=pltpu.MemorySpace.HBM)


def snake(axis, index):
    row, column = index // DOM_ROW, index % DOM_ROW
    return index if axis == "grp" or row % 2 == 0 else row * DOM_ROW + DOM_ROW - 1 - column


def kernel_call(body, outs, specs, scratch=()):
    return pl.pallas_call(
        body,
        out_shape=outs,
        in_specs=specs,
        out_specs=[VMEM] * len(outs),
        scratch_shapes=list(scratch),
        compiler_params=pltpu.CompilerParams(vmem_limit_bytes=24 * 1024 * 1024),
    )


def parts_of(x):
    high = x.astype(jnp.bfloat16).astype(jnp.float32)
    rest = x - high
    middle = rest.astype(jnp.bfloat16).astype(jnp.float32)
    low = (rest - middle).astype(jnp.bfloat16).astype(jnp.float32)
    return high, middle, low


def matmul(left, right):
    return jnp.dot(left, right, preferred_element_type=jnp.float32)


def lane_gather(row, index):
    return jnp.take_along_axis(row, index, axis=1)


def pick_lanes(field, index):
    low = jnp.bitwise_and(index, LANES - 1)
    chunk = jnp.right_shift(index, 7)
    out = lane_gather(field[:, 0:LANES], low)
    for j in range(1, field.shape[1] // LANES):
        out = jnp.where(
            chunk == j, lane_gather(field[:, j * LANES : (j + 1) * LANES], low), out
        )
    return out


def spread(received, inverse):
    out = []
    for j in range(inverse.shape[1] // LANES):
        index = inverse[:, j * LANES : (j + 1) * LANES]
        taken = lane_gather(received, jnp.maximum(index, 0))
        out.append(jnp.where(index >= 0, taken, 0.0))
    return jnp.concatenate(out, axis=1)


def merge_received(source, dom1, grp1, dom0, grp0):
    out = jnp.where(source == 0, grp0, grp1)
    out = jnp.where(source == 2, dom0, out)
    return jnp.where(source == 3, dom1, out)


def scatter_nodes(rows, incidence):
    left = jnp.concatenate(parts_of(rows), axis=0).astype(jnp.bfloat16)
    sums = matmul(left, incidence)
    return (sums[16:24] + sums[8:16]) + sums[0:8]


CONNECT_ROW = 0
MASS_ROW = 24
LAME_ROW = 44
LISTED_ROW = 46
SWAPPED_ROW = 47
JACOBIAN_ROW = 48
WEIGHTS_ROW = 64
SOURCE_ROW = 80
RANK_ROW = 96
PACKED_ROWS = 112


def pack_kernel(
    wavelet_in,
    neighbours_in,
    connect_in,
    lists_in,
    mass_in,
    source_in,
    shape_in,
    jacobian_in,
    lame_in,
    weights_in,
    rank_in,
    packed,
    shape_t,
    wave,
    wavelet,
    neighbours,
    connect,
    lists,
    mass_elem,
    source_pattern,
    jacobian,
    lame,
    weights,
    rank,
    sems,
):
    moves = [
        (wavelet_in, wavelet),
        (neighbours_in, neighbours),
        (connect_in, connect),
        (lists_in, lists),
        (mass_in, mass_elem),
        (source_in, source_pattern),
        (shape_in, shape_t),
        (jacobian_in, jacobian),
        (lame_in, lame),
        (weights_in, weights),
        (rank_in, rank),
    ]
    copies = [pltpu.make_async_copy(a, b, sems.at[i]) for i, (a, b) in enumerate(moves)]
    for copy in copies:
        copy.start()
    packed[...] = jnp.zeros(packed.shape, jnp.float32)
    for copy in copies:
        copy.wait()
    wave[...] = jnp.concatenate(
        [jnp.full((1, LANES), wavelet[t], jnp.float32) for t in range(STEPS)], axis=0
    )
    packed[CONNECT_ROW : CONNECT_ROW + EL_NODES, :] = connect[...].astype(jnp.float32)
    packed[MASS_ROW : MASS_ROW + EL_NODES, :] = mass_elem[...]
    packed[LAME_ROW : LAME_ROW + 2, :] = lame[...]
    packed[JACOBIAN_ROW : JACOBIAN_ROW + 9, :] = jacobian[...]
    packed[WEIGHTS_ROW : WEIGHTS_ROW + POINTS, :] = weights[...]
    packed[RANK_ROW : RANK_ROW + POINTS, :] = rank[...].astype(jnp.float32)
    for j in range(source_pattern.shape[1] // LANES):
        row = SOURCE_ROW + 3 * j
        packed[row : row + 3, :] = source_pattern[:, j * LANES : (j + 1) * LANES]
    face = [lists[0, k : k + 1, :] for k in range(FACES)]
    listed = jnp.concatenate(face, axis=1)
    swapped = jnp.concatenate([face[1], face[0], face[3], face[2]], axis=1)
    side = lax.broadcasted_iota(jnp.int32, (1, LANES), 1) // (LANES // FACES)
    open_side = jnp.where(
        side < 2,
        jnp.where(side == 0, neighbours[0, 0], neighbours[0, 1]),
        jnp.where(side == 2, neighbours[0, 2], neighbours[0, 3]),
    )
    listed = jnp.where(open_side != 0, listed, -1)
    packed[LISTED_ROW : LISTED_ROW + 1, :] = listed.astype(jnp.float32)
    packed[SWAPPED_ROW : SWAPPED_ROW + 1, :] = swapped.astype(jnp.float32)


def prepare_kernel(
    packed,
    shape_t,
    incidence,
    field,
    send,
    pick_index,
    inverse_index,
    connect,
    left_gradient,
    left_force,
    inverse_jacobian,
    lame_moduli,
    point_weights,
    rank,
):
    nodes = field.shape[1]
    element_nodes = packed[CONNECT_ROW : CONNECT_ROW + NODE_ROWS, :].astype(jnp.int32)
    connect[...] = element_nodes
    inverse_jacobian[...] = packed[JACOBIAN_ROW : JACOBIAN_ROW + 9, :]
    lame_moduli[...] = packed[LAME_ROW : LAME_ROW + 2, :]
    point_weights[...] = packed[WEIGHTS_ROW : WEIGHTS_ROW + POINTS, :]
    rank[...] = packed[RANK_ROW : RANK_ROW + POINTS, :].astype(jnp.int32)
    lane = lax.broadcasted_iota(jnp.int32, (LANES, nodes), 1)
    for n in range(EL_NODES):
        column = jnp.broadcast_to(element_nodes[n : n + 1, :], (LANES, LANES)).T
        wide = jnp.concatenate([column] * (nodes // LANES), axis=1)
        incidence[n * LANES : (n + 1) * LANES, :] = jnp.where(wide == lane, 1.0, 0.0).astype(
            jnp.bfloat16
        )
    listed = packed[LISTED_ROW : LISTED_ROW + 1, :].astype(jnp.int32)
    column = jnp.broadcast_to(listed, (LANES, LANES)).T
    wide = jnp.concatenate([column] * (nodes // LANES), axis=1)
    slot = lax.broadcasted_iota(jnp.int32, (LANES, nodes), 0) + 1
    found = jnp.sum(jnp.where(wide == lane, slot, 0), axis=0, keepdims=True)
    inverse_index[...] = jnp.broadcast_to(found - 1, (8, nodes))
    swapped = packed[SWAPPED_ROW : SWAPPED_ROW + 1, :].astype(jnp.int32)
    index = jnp.broadcast_to(swapped, (8, LANES))
    pick_index[...] = index
    rows = jnp.concatenate(
        [
            jnp.broadcast_to(packed[MASS_ROW + n : MASS_ROW + n + 1, :], (8, LANES))
            for n in range(EL_NODES)
        ],
        axis=1,
    )
    field[...] = scatter_nodes(rows, incidence[...])
    for j in range(nodes // LANES):
        row = SOURCE_ROW + 3 * j
        field[0:3, j * LANES : (j + 1) * LANES] = packed[row : row + 3, :]
    send[...] = pick_lanes(field[...], index)

    reference_rows = 3 * POINTS
    shape_rows = jnp.concatenate(
        [shape_t[...], jnp.zeros((EL_NODES, LANES - reference_rows), jnp.float32)], axis=1
    )
    shape_rows = jnp.concatenate(
        [shape_rows, jnp.zeros((LANES - EL_NODES, LANES), jnp.float32)], axis=0
    )
    forward = parts_of(shape_rows.T[0:reference_rows, :])
    for j in range(3):
        block = forward[j]
        for i in range(1, 3 - j):
            block = block + pltpu.roll(forward[j], i * GRADIENT_BLOCK, 1)
        left_gradient[j * reference_rows : (j + 1) * reference_rows, :] = block[
            :, 0 : 3 * GRADIENT_BLOCK
        ].astype(jnp.bfloat16)
    backward = parts_of(shape_rows[0:NODE_ROWS, :])
    firsts, seconds = [], []
    for j in range(3):
        block = backward[j]
        firsts.append(block if j == 2 else block + pltpu.roll(block, FORCE_BLOCK, 1))
        seconds.append(block if j == 0 else jnp.zeros_like(block))
    left_force[:, 0:LANES] = jnp.concatenate(firsts, axis=0).astype(jnp.bfloat16)
    left_force[:, LANES:] = jnp.concatenate(seconds, axis=0)[:, 0:FORCE_BLOCK].astype(jnp.bfloat16)


def stacked_parts(x, height):
    gap = height - x.shape[0]
    pieces = []
    for part in parts_of(x):
        pieces += [part, jnp.zeros((gap, x.shape[1]), jnp.float32)]
    return jnp.concatenate(pieces, axis=0).astype(jnp.bfloat16)


def wave_row(wave, step, width):
    return jnp.concatenate([wave[step : step + 1, :]] * (width // LANES), axis=1)


def strain_and_force(
    displace,
    strain,
    connect,
    left_gradient,
    left_force,
    inverse_jacobian,
    lame_moduli,
    point_weights,
    incidence,
    need_force,
):
    index = connect[...]
    low = jnp.bitwise_and(index, LANES - 1)
    chunk = jnp.right_shift(index, 7)
    is_chunk = [chunk == j for j in range(1, displace.shape[1] // LANES)]
    columns = []
    for c in range(3):
        pieces = []
        for b in range(NODE_ROWS // 8):
            rows = slice(8 * b, 8 * b + 8)
            out = None
            for j in range(displace.shape[1] // LANES):
                row = jnp.broadcast_to(displace[c : c + 1, j * LANES : (j + 1) * LANES], (8, LANES))
                taken = lane_gather(row, low[rows])
                out = taken if j == 0 else jnp.where(is_chunk[j - 1][rows], taken, out)
            pieces.append(out)
        columns.append(jnp.concatenate(pieces, axis=0))
    node_values = jnp.concatenate(columns, axis=1)
    right = stacked_parts(node_values, GRADIENT_BLOCK)
    sums = matmul(left_gradient[...], right)
    height = 3 * POINTS
    along = (sums[2 * height :] + sums[height : 2 * height]) + sums[0:height]
    jac = [inverse_jacobian[i : i + 1, :] for i in range(9)]

    def ref_derivative(c, r):
        return along[r * POINTS : (r + 1) * POINTS, c * LANES : (c + 1) * LANES]

    grad = [
        [
            (ref_derivative(c, 0) * jac[d] + ref_derivative(c, 1) * jac[3 + d])
            + ref_derivative(c, 2) * jac[6 + d]
            for d in range(3)
        ]
        for c in range(3)
    ]
    shear = {(c, d): grad[c][d] + grad[d][c] for c, d in ((1, 2), (0, 2), (0, 1))}
    rows = [grad[0][0], grad[1][1], grad[2][2]] + [0.5 * shear[k] for k in ((1, 2), (0, 2), (0, 1))]
    for s in range(STRAIN):
        strain[s * POINTS : (s + 1) * POINTS, :] = rows[s]
    if not need_force:
        return None
    volume = (grad[0][0] + grad[1][1]) + grad[2][2]
    weights = point_weights[...]
    shear_scale = lame_moduli[1:2, :] * weights
    pressure = (lame_moduli[0:1, :] * weights) * volume
    stress = [[None] * 3 for _ in range(3)]
    for c in range(3):
        for d in range(3):
            if c == d:
                stress[c][d] = shear_scale * (grad[c][c] + grad[c][c]) + pressure
            else:
                stress[c][d] = shear_scale * shear[(min(c, d), max(c, d))]
    columns = []
    for c in range(3):
        mapped = [
            (stress[c][0] * jac[3 * r] + stress[c][1] * jac[3 * r + 1])
            + stress[c][2] * jac[3 * r + 2]
            for r in range(3)
        ]
        columns.append(jnp.concatenate(mapped, axis=0))
    mapped = jnp.concatenate(columns, axis=1)
    right = stacked_parts(mapped, FORCE_BLOCK)
    sums = matmul(left_force[...], right)
    node_forces = (sums[2 * NODE_ROWS :] + sums[NODE_ROWS : 2 * NODE_ROWS]) + sums[0:NODE_ROWS]
    row_id = lax.broadcasted_iota(jnp.int32, (8, LANES), 0)
    pieces = []
    for n in range(EL_NODES):
        first, second, third = (
            jnp.broadcast_to(node_forces[n : n + 1, c * LANES : (c + 1) * LANES], (8, LANES))
            for c in range(3)
        )
        pieces.append(jnp.where(row_id == 0, first, jnp.where(row_id == 1, second, third)))
    return scatter_nodes(jnp.concatenate(pieces, axis=1), incidence[...])


def first_kernel(
    wave,
    dom1,
    grp1,
    dom0,
    grp0,
    source,
    inverse_index,
    pick_index,
    field,
    connect,
    left_gradient,
    left_force,
    inverse_jacobian,
    lame_moduli,
    point_weights,
    incidence,
    strain,
    displace,
    velocity,
    pattern,
    half_inverse_mass,
    force,
    send,
):
    received = merge_received(source[...], dom1[...], grp1[...], dom0[...], grp0[...])
    total = field[...] + spread(received, inverse_index[...])
    scale = jnp.broadcast_to(time_step * (1.0 / total[3:4, :]), total.shape)
    pattern[...] = total
    half_inverse_mass[...] = scale
    new_velocity = scale * (wave_row(wave, 0, total.shape[1]) * total)
    velocity[...] = new_velocity
    new_displace = time_step * new_velocity
    displace[...] = new_displace
    new_force = strain_and_force(
        new_displace,
        strain,
        connect,
        left_gradient,
        left_force,
        inverse_jacobian,
        lame_moduli,
        point_weights,
        incidence,
        True,
    )
    force[...] = new_force
    send[...] = pick_lanes(new_force, pick_index[...])


def step_kernel(
    step,
    wave,
    dom1,
    grp1,
    dom0,
    grp0,
    source,
    inverse_index,
    pick_index,
    connect,
    left_gradient,
    left_force,
    inverse_jacobian,
    lame_moduli,
    point_weights,
    incidence,
    pattern,
    half_inverse_mass,
    old_displace,
    old_velocity,
    old_force,
    strain,
    *rest,
):
    received = merge_received(source[...], dom1[...], grp1[...], dom0[...], grp0[...])
    stiff = old_force[...] + spread(received, inverse_index[...])
    total = wave_row(wave, step, stiff.shape[1]) * pattern[...] - stiff
    new_velocity = old_velocity[...] + half_inverse_mass[...] * total
    new_displace = old_displace[...] + time_step * new_velocity
    new_force = strain_and_force(
        new_displace,
        strain,
        connect,
        left_gradient,
        left_force,
        inverse_jacobian,
        lame_moduli,
        point_weights,
        incidence,
        bool(rest),
    )
    if rest:
        displace, velocity, force, send = rest
        displace[...] = new_displace
        velocity[...] = new_velocity
        force[...] = new_force
        send[...] = pick_lanes(new_force, pick_index[...])


def order_kernel(rank, *refs):
    strains, out, store = refs[:STEPS], refs[STEPS], refs[STEPS + 1]
    for t in range(STEPS):
        for c in range(STRAIN):
            row = (c * STEPS + t) * POINTS
            store[row : row + POINTS, :] = strains[t][c * POINTS : (c + 1) * POINTS, :]
    count = rank.shape[0] * LANES
    lane = lax.broadcasted_iota(jnp.int32, (LANES, count), 1)
    total = None
    for q in range(POINTS):
        values = store[pl.ds(q, STEPS * STRAIN, stride=POINTS), :].astype(jnp.bfloat16)
        column = jnp.broadcast_to(rank[q : q + 1, :], (LANES, LANES)).T
        wide = jnp.concatenate([column] * (count // LANES), axis=1)
        chosen = jnp.where(wide == lane, 1.0, 0.0).astype(jnp.bfloat16)
        part = matmul(values, chosen)
        total = part if total is None else total + part
    for w in range(count // LANES):
        out[w] = total[:, w * LANES : (w + 1) * LANES].astype(jnp.bfloat16)


def place_kernel(pieces, out):
    for w in range(pieces.shape[0]):
        held = snake("dom", w)
        for c in range(STRAIN):
            out[c, :, w * LANES : (w + 1) * LANES] = pieces[held, c * STEPS : (c + 1) * STEPS, :]


def shards(
    connect,
    interface_nodes,
    neighbours,
    point_rank,
    shape_grad,
    inverse_jacobian,
    lame_moduli,
    point_weights,
    mass_elem,
    source_pattern,
    wavelet,
):
    nodes = source_pattern.shape[1]
    f32 = jnp.float32
    field_t = jax.ShapeDtypeStruct((8, nodes), f32)
    lanes_t = jax.ShapeDtypeStruct((8, LANES), f32)
    index_t = jax.ShapeDtypeStruct((8, LANES), jnp.int32)
    strain_t = jax.ShapeDtypeStruct((STRAIN * POINTS, LANES), f32)

    face = lax.broadcasted_iota(jnp.int32, (8, LANES), 1) // (LANES // FACES)
    dom = lax.axis_index("dom")
    parity = jnp.where(face < 2, lax.axis_index("grp") % 2, (dom // DOM_ROW + dom) % 2)
    source = 2 * (face // 2) + jnp.bitwise_xor(parity, 1 - face % 2)

    def exchange(send):
        received = []
        for name in EXCHANGES:
            axis, offset = name[:3], int(name[3])
            count = lax.axis_size(axis)
            pairs = []
            for i in range(offset, count - 1, 2):
                first, second = snake(axis, i), snake(axis, i + 1)
                pairs += [(first, second), (second, first)]
            received.append(lax.ppermute(send, axis, pairs))
        return received

    i32, bf16 = jnp.int32, jnp.bfloat16
    rank_rows = point_rank.reshape(POINTS, LANES)
    arguments = (
        wavelet,
        neighbours,
        connect,
        interface_nodes,
        mass_elem,
        source_pattern,
        shape_grad.T,
        inverse_jacobian,
        lame_moduli,
        point_weights,
        rank_rows,
    )
    buffers = [pltpu.SMEM(x.shape, x.dtype) for x in arguments[:2]]
    buffers += [pltpu.VMEM(x.shape, x.dtype) for x in arguments[2:6] + arguments[7:]]
    packed, shape_t, wave = kernel_call(
        pack_kernel,
        [
            jax.ShapeDtypeStruct((PACKED_ROWS, LANES), f32),
            jax.ShapeDtypeStruct(shape_grad.T.shape, f32),
            jax.ShapeDtypeStruct((STEPS, LANES), f32),
        ],
        [HBM] * len(arguments),
        scratch=buffers + [pltpu.SemaphoreType.DMA((len(arguments),))],
    )(*(pltpu.with_memory_space_constraint(x, pltpu.MemorySpace.HBM) for x in arguments))
    writers = lax.axis_size("dom")
    packed = lax.ppermute(packed, "dom", [(i, snake("dom", i)) for i in range(writers)])
    outs = kernel_call(
        prepare_kernel,
        [
            jax.ShapeDtypeStruct((EL_NODES * LANES, nodes), bf16),
            field_t,
            lanes_t,
            index_t,
            jax.ShapeDtypeStruct((8, nodes), i32),
            jax.ShapeDtypeStruct((NODE_ROWS, LANES), i32),
            jax.ShapeDtypeStruct((9 * POINTS, 3 * GRADIENT_BLOCK), bf16),
            jax.ShapeDtypeStruct((3 * NODE_ROWS, 3 * FORCE_BLOCK), bf16),
            jax.ShapeDtypeStruct(inverse_jacobian.shape, f32),
            jax.ShapeDtypeStruct(lame_moduli.shape, f32),
            jax.ShapeDtypeStruct(point_weights.shape, f32),
            jax.ShapeDtypeStruct(rank_rows.shape, i32),
        ],
        [VMEM, VMEM],
    )(packed, shape_t)
    incidence, field, send, pick_index, inverse_index = outs[:5]
    rank = outs[11]
    element_data = (*outs[5:11], incidence)
    received = exchange(send)
    strain, displace, velocity, pattern, half_inverse_mass, force, send = kernel_call(
        first_kernel, [strain_t, field_t, field_t, field_t, field_t, field_t, lanes_t], [VMEM] * 16
    )(wave, *received, source, inverse_index, pick_index, field, *element_data)
    strains = [strain]
    for step in range(1, STEPS):
        received = exchange(send)
        last = step == STEPS - 1
        outs = kernel_call(
            functools.partial(step_kernel, step),
            [strain_t] + ([] if last else [field_t, field_t, field_t, lanes_t]),
            [VMEM] * 20,
        )(
            wave,
            *received,
            source,
            inverse_index,
            pick_index,
            *element_data,
            pattern,
            half_inverse_mass,
            displace,
            velocity,
            force,
        )
        strains.append(outs[0])
        if not last:
            displace, velocity, force, send = outs[1:]
    (ordered,) = kernel_call(
        order_kernel,
        [jax.ShapeDtypeStruct((writers, STEPS * STRAIN, LANES), jnp.bfloat16)],
        [VMEM] * (1 + STEPS),
        scratch=[pltpu.VMEM((STEPS * STRAIN * POINTS, LANES), f32)],
    )(rank, *strains)
    pieces = lax.all_to_all(ordered, "dom", split_axis=0, concat_axis=0, tiled=True)
    (placed,) = kernel_call(
        place_kernel, [jax.ShapeDtypeStruct((STRAIN, STEPS, writers * LANES), jnp.bfloat16)], [VMEM]
    )(pieces)
    return placed.transpose(1, 0, 2)


def solution(mesh):
    placed = (
        P(None, ("grp", "dom")),
        P(("grp", "dom"), None, None),
        P(("grp", "dom"), None),
        P(("grp", "dom"), None),
        P(),
        P(None, ("grp", "dom")),
        P(None, ("grp", "dom")),
        P(None, ("grp", "dom")),
        P(None, ("grp", "dom")),
        P(None, ("grp", "dom")),
        P(),
    )
    return jax.shard_map(
        shards, mesh=mesh, in_specs=placed, out_specs=P(None, None, ("grp", "dom")), check_vma=False
    )
```

```python
import jax
import jax.numpy as jnp
from jax import lax
from jax.experimental import pallas as pl
from jax.experimental.pallas import tpu as pltpu
from jax.sharding import PartitionSpec as P


EL_NODES = 20
NODE_ROWS = 24
POINTS = 16
STRAIN = 6
STEPS = 16
LANES = 128
FACES = 4
GRADIENT_BLOCK = 32
FORCE_BLOCK = 64

time_step = 0.5

DOM_ROW = 4

EXCHANGES = ("dom1", "grp1", "dom0", "grp0")

VMEM = pl.BlockSpec(memory_space=pltpu.VMEM)
HBM = pl.BlockSpec(memory_space=pltpu.MemorySpace.HBM)


def snake(axis, index):
    row, column = index // DOM_ROW, index % DOM_ROW
    return index if axis == "grp" or row % 2 == 0 else row * DOM_ROW + DOM_ROW - 1 - column


def kernel_call(body, outs, specs, scratch=()):
    return pl.pallas_call(
        body,
        out_shape=outs,
        in_specs=specs,
        out_specs=[VMEM] * len(outs),
        scratch_shapes=list(scratch),
        compiler_params=pltpu.CompilerParams(vmem_limit_bytes=24 * 1024 * 1024),
    )


def parts_of(x):
    high = x.astype(jnp.bfloat16).astype(jnp.float32)
    rest = x - high
    middle = rest.astype(jnp.bfloat16).astype(jnp.float32)
    low = (rest - middle).astype(jnp.bfloat16).astype(jnp.float32)
    return high, middle, low


def matmul(left, right):
    return jnp.dot(left, right, preferred_element_type=jnp.float32)


def lane_gather(row, index):
    return jnp.take_along_axis(row, index, axis=1)


def pick_lanes(field, index):
    low = jnp.bitwise_and(index, LANES - 1)
    chunk = jnp.right_shift(index, 7)
    out = lane_gather(field[:, 0:LANES], low)
    for j in range(1, field.shape[1] // LANES):
        out = jnp.where(
            chunk == j, lane_gather(field[:, j * LANES : (j + 1) * LANES], low), out
        )
    return out


def spread(received, inverse):
    out = []
    for j in range(inverse.shape[1] // LANES):
        index = inverse[:, j * LANES : (j + 1) * LANES]
        taken = lane_gather(received, jnp.maximum(index, 0))
        out.append(jnp.where(index >= 0, taken, 0.0))
    return jnp.concatenate(out, axis=1)


def merge_received(source, dom1, grp1, dom0, grp0):
    out = jnp.where(source == 0, grp0, grp1)
    out = jnp.where(source == 2, dom0, out)
    return jnp.where(source == 3, dom1, out)


def scatter_nodes(pieces, chunks, incidence):
    group = lax.broadcasted_iota(jnp.int32, (8, LANES), 0) // 4
    parts = [[], [], []]
    for piece, chunk in zip(pieces, chunks):
        both = [jnp.where(chunk == group + base, piece, 0.0) for base in (0, 2)]
        for i, part in enumerate(parts_of(jnp.concatenate(both, axis=0))):
            parts[i].append(part.astype(jnp.bfloat16))
    left = jnp.concatenate([jnp.concatenate(p, axis=1) for p in parts], axis=0)
    sums = matmul(left, incidence)
    total = (sums[32:48] + sums[16:32]) + sums[0:16]
    fields = []
    for base in (0, 8):
        rows = total[base : base + 8]
        fields += [rows, pltpu.roll(rows, 4, 0)]
    return jnp.concatenate(fields, axis=1)


CONNECT_ROW = 0
MASS_ROW = 24
LAME_ROW = 44
LISTED_ROW = 46
SWAPPED_ROW = 47
JACOBIAN_ROW = 48
WEIGHTS_ROW = 64
SOURCE_ROW = 80
RANK_ROW = 96
PACKED_ROWS = 112


def pack_kernel(
    wavelet_in,
    neighbours_in,
    connect_in,
    lists_in,
    mass_in,
    source_in,
    shape_in,
    jacobian_in,
    lame_in,
    weights_in,
    rank_in,
    packed,
    shape_t,
    wave,
    wavelet,
    neighbours,
    connect,
    lists,
    mass_elem,
    source_pattern,
    jacobian,
    lame,
    weights,
    rank,
    sems,
):
    moves = [
        (wavelet_in, wavelet),
        (neighbours_in, neighbours),
        (connect_in, connect),
        (lists_in, lists),
        (mass_in, mass_elem),
        (source_in, source_pattern),
        (shape_in, shape_t),
        (jacobian_in, jacobian),
        (lame_in, lame),
        (weights_in, weights),
        (rank_in, rank),
    ]
    copies = [pltpu.make_async_copy(a, b, sems.at[i]) for i, (a, b) in enumerate(moves)]
    for copy in copies:
        copy.start()
    packed[...] = jnp.zeros(packed.shape, jnp.float32)
    for copy in copies:
        copy.wait()
    wave[...] = jnp.concatenate(
        [jnp.full((1, LANES), wavelet[t], jnp.float32) for t in range(STEPS)], axis=0
    )
    packed[CONNECT_ROW : CONNECT_ROW + EL_NODES, :] = connect[...].astype(jnp.float32)
    packed[MASS_ROW : MASS_ROW + EL_NODES, :] = mass_elem[...]
    packed[LAME_ROW : LAME_ROW + 2, :] = lame[...]
    packed[JACOBIAN_ROW : JACOBIAN_ROW + 9, :] = jacobian[...]
    packed[WEIGHTS_ROW : WEIGHTS_ROW + POINTS, :] = weights[...]
    packed[RANK_ROW : RANK_ROW + POINTS, :] = rank[...].astype(jnp.float32)
    for j in range(source_pattern.shape[1] // LANES):
        row = SOURCE_ROW + 3 * j
        packed[row : row + 3, :] = source_pattern[:, j * LANES : (j + 1) * LANES]
    face = [lists[0, k : k + 1, :] for k in range(FACES)]
    listed = jnp.concatenate(face, axis=1)
    swapped = jnp.concatenate([face[1], face[0], face[3], face[2]], axis=1)
    side = lax.broadcasted_iota(jnp.int32, (1, LANES), 1) // (LANES // FACES)
    open_side = jnp.where(
        side < 2,
        jnp.where(side == 0, neighbours[0, 0], neighbours[0, 1]),
        jnp.where(side == 2, neighbours[0, 2], neighbours[0, 3]),
    )
    listed = jnp.where(open_side != 0, listed, -1)
    packed[LISTED_ROW : LISTED_ROW + 1, :] = listed.astype(jnp.float32)
    packed[SWAPPED_ROW : SWAPPED_ROW + 1, :] = swapped.astype(jnp.float32)


def prepare_kernel(
    packed,
    shape_t,
    incidence,
    field,
    send,
    pick_index,
    inverse_index,
    connect,
    left_gradient,
    left_force,
    inverse_jacobian,
    lame_moduli,
    point_weights,
    rank,
):
    nodes = field.shape[1]
    element_nodes = packed[CONNECT_ROW : CONNECT_ROW + NODE_ROWS, :].astype(jnp.int32)
    connect[...] = element_nodes
    inverse_jacobian[...] = packed[JACOBIAN_ROW : JACOBIAN_ROW + 9, :]
    lame_moduli[...] = packed[LAME_ROW : LAME_ROW + 2, :]
    point_weights[...] = packed[WEIGHTS_ROW : WEIGHTS_ROW + POINTS, :]
    rank[...] = packed[RANK_ROW : RANK_ROW + POINTS, :].astype(jnp.int32)
    low = jnp.bitwise_and(element_nodes, LANES - 1)
    chunk = jnp.right_shift(element_nodes, 7)
    own_lane = lax.broadcasted_iota(jnp.int32, (LANES, LANES), 1)
    for n in range(EL_NODES):
        column = jnp.broadcast_to(low[n : n + 1, :], (LANES, LANES)).T
        incidence[n * LANES : (n + 1) * LANES, :] = jnp.where(
            column == own_lane, 1.0, 0.0
        ).astype(jnp.bfloat16)
    lane = lax.broadcasted_iota(jnp.int32, (LANES, nodes), 1)
    listed = packed[LISTED_ROW : LISTED_ROW + 1, :].astype(jnp.int32)
    column = jnp.broadcast_to(listed, (LANES, LANES)).T
    wide = jnp.concatenate([column] * (nodes // LANES), axis=1)
    slot = lax.broadcasted_iota(jnp.int32, (LANES, nodes), 0) + 1
    found = jnp.sum(jnp.where(wide == lane, slot, 0), axis=0, keepdims=True)
    inverse_index[...] = jnp.broadcast_to(found - 1, (8, nodes))
    swapped = packed[SWAPPED_ROW : SWAPPED_ROW + 1, :].astype(jnp.int32)
    index = jnp.broadcast_to(swapped, (8, LANES))
    pick_index[...] = index
    masses = [
        jnp.broadcast_to(packed[MASS_ROW + n : MASS_ROW + n + 1, :], (8, LANES))
        for n in range(EL_NODES)
    ]
    chunks = [chunk[n : n + 1, :] for n in range(EL_NODES)]
    field[...] = scatter_nodes(masses, chunks, incidence[...])
    for j in range(nodes // LANES):
        row = SOURCE_ROW + 3 * j
        field[0:3, j * LANES : (j + 1) * LANES] = packed[row : row + 3, :]
    send[...] = pick_lanes(field[...], index)

    reference_rows = 3 * POINTS
    shape_rows = jnp.concatenate(
        [shape_t[...], jnp.zeros((EL_NODES, LANES - reference_rows), jnp.float32)], axis=1
    )
    shape_rows = jnp.concatenate(
        [shape_rows, jnp.zeros((LANES - EL_NODES, LANES), jnp.float32)], axis=0
    )
    forward = parts_of(shape_rows.T[0:reference_rows, :])
    for j in range(3):
        block = forward[j]
        for i in range(1, 3 - j):
            block = block + pltpu.roll(forward[j], i * GRADIENT_BLOCK, 1)
        left_gradient[j * reference_rows : (j + 1) * reference_rows, :] = block[
            :, 0 : 3 * GRADIENT_BLOCK
        ].astype(jnp.bfloat16)
    backward = parts_of(shape_rows[0:NODE_ROWS, :])
    firsts, seconds = [], []
    for j in range(3):
        block = backward[j]
        firsts.append(block if j == 2 else block + pltpu.roll(block, FORCE_BLOCK, 1))
        seconds.append(block if j == 0 else jnp.zeros_like(block))
    left_force[:, 0:LANES] = jnp.concatenate(firsts, axis=0).astype(jnp.bfloat16)
    left_force[:, LANES:] = jnp.concatenate(seconds, axis=0)[:, 0:FORCE_BLOCK].astype(jnp.bfloat16)


def stacked_parts(x, height):
    gap = height - x.shape[0]
    pieces = []
    for part in parts_of(x):
        pieces += [part, jnp.zeros((gap, x.shape[1]), jnp.float32)]
    return jnp.concatenate(pieces, axis=0).astype(jnp.bfloat16)


def wave_row(wave, width):
    return jnp.concatenate([wave[0:1, :]] * (width // LANES), axis=1)


def moved_up(wave):
    return pltpu.roll(wave[...], STEPS - 1, 0)


def strain_and_force(
    displace,
    strain,
    connect,
    left_gradient,
    left_force,
    inverse_jacobian,
    lame_moduli,
    point_weights,
    incidence,
    need_force,
):
    index = connect[...]
    low = jnp.bitwise_and(index, LANES - 1)
    chunk = jnp.right_shift(index, 7)
    is_chunk = [chunk == j for j in range(1, displace.shape[1] // LANES)]
    columns = []
    for c in range(3):
        pieces = []
        for b in range(NODE_ROWS // 8):
            rows = slice(8 * b, 8 * b + 8)
            out = None
            for j in range(displace.shape[1] // LANES):
                row = jnp.broadcast_to(displace[c : c + 1, j * LANES : (j + 1) * LANES], (8, LANES))
                taken = lane_gather(row, low[rows])
                out = taken if j == 0 else jnp.where(is_chunk[j - 1][rows], taken, out)
            pieces.append(out)
        columns.append(jnp.concatenate(pieces, axis=0))
    node_values = jnp.concatenate(columns, axis=1)
    right = stacked_parts(node_values, GRADIENT_BLOCK)
    sums = matmul(left_gradient[...], right)
    height = 3 * POINTS
    along = (sums[2 * height :] + sums[height : 2 * height]) + sums[0:height]
    jac = [inverse_jacobian[i : i + 1, :] for i in range(9)]

    def ref_derivative(c, r):
        return along[r * POINTS : (r + 1) * POINTS, c * LANES : (c + 1) * LANES]

    grad = [
        [
            (ref_derivative(c, 0) * jac[d] + ref_derivative(c, 1) * jac[3 + d])
            + ref_derivative(c, 2) * jac[6 + d]
            for d in range(3)
        ]
        for c in range(3)
    ]
    shear = {(c, d): grad[c][d] + grad[d][c] for c, d in ((1, 2), (0, 2), (0, 1))}
    rows = [grad[0][0], grad[1][1], grad[2][2]] + [0.5 * shear[k] for k in ((1, 2), (0, 2), (0, 1))]
    for s in range(STRAIN):
        strain[s * POINTS : (s + 1) * POINTS, :] = rows[s]
    if not need_force:
        return None
    volume = (grad[0][0] + grad[1][1]) + grad[2][2]
    weights = point_weights[...]
    shear_scale = lame_moduli[1:2, :] * weights
    pressure = (lame_moduli[0:1, :] * weights) * volume
    stress = [[None] * 3 for _ in range(3)]
    for c in range(3):
        for d in range(3):
            if c == d:
                stress[c][d] = shear_scale * (grad[c][c] + grad[c][c]) + pressure
            else:
                stress[c][d] = shear_scale * shear[(min(c, d), max(c, d))]
    columns = []
    for c in range(3):
        mapped = [
            (stress[c][0] * jac[3 * r] + stress[c][1] * jac[3 * r + 1])
            + stress[c][2] * jac[3 * r + 2]
            for r in range(3)
        ]
        columns.append(jnp.concatenate(mapped, axis=0))
    mapped = jnp.concatenate(columns, axis=1)
    right = stacked_parts(mapped, FORCE_BLOCK)
    sums = matmul(left_force[...], right)
    node_forces = (sums[2 * NODE_ROWS :] + sums[NODE_ROWS : 2 * NODE_ROWS]) + sums[0:NODE_ROWS]
    row_id = lax.broadcasted_iota(jnp.int32, (8, LANES), 0) % 4
    pieces = []
    for n in range(EL_NODES):
        first, second, third = (
            jnp.broadcast_to(node_forces[n : n + 1, c * LANES : (c + 1) * LANES], (8, LANES))
            for c in range(3)
        )
        pieces.append(jnp.where(row_id == 0, first, jnp.where(row_id == 1, second, third)))
    chunks = [chunk[n : n + 1, :] for n in range(EL_NODES)]
    return scatter_nodes(pieces, chunks, incidence[...])


def first_kernel(
    wave,
    dom1,
    grp1,
    dom0,
    grp0,
    source,
    inverse_index,
    pick_index,
    field,
    connect,
    left_gradient,
    left_force,
    inverse_jacobian,
    lame_moduli,
    point_weights,
    incidence,
    strain,
    displace,
    velocity,
    pattern,
    half_inverse_mass,
    force,
    send,
    next_wave,
):
    next_wave[...] = moved_up(wave)
    received = merge_received(source[...], dom1[...], grp1[...], dom0[...], grp0[...])
    total = field[...] + spread(received, inverse_index[...])
    scale = jnp.broadcast_to(time_step * (1.0 / total[3:4, :]), total.shape)
    pattern[...] = total
    half_inverse_mass[...] = scale
    new_velocity = scale * (wave_row(wave, total.shape[1]) * total)
    velocity[...] = new_velocity
    new_displace = time_step * new_velocity
    displace[...] = new_displace
    new_force = strain_and_force(
        new_displace,
        strain,
        connect,
        left_gradient,
        left_force,
        inverse_jacobian,
        lame_moduli,
        point_weights,
        incidence,
        True,
    )
    force[...] = new_force
    send[...] = pick_lanes(new_force, pick_index[...])


def step_kernel(
    wave,
    dom1,
    grp1,
    dom0,
    grp0,
    source,
    inverse_index,
    pick_index,
    connect,
    left_gradient,
    left_force,
    inverse_jacobian,
    lame_moduli,
    point_weights,
    incidence,
    pattern,
    half_inverse_mass,
    old_displace,
    old_velocity,
    old_force,
    strain,
    *rest,
):
    received = merge_received(source[...], dom1[...], grp1[...], dom0[...], grp0[...])
    stiff = old_force[...] + spread(received, inverse_index[...])
    total = wave_row(wave, stiff.shape[1]) * pattern[...] - stiff
    new_velocity = old_velocity[...] + half_inverse_mass[...] * total
    new_displace = old_displace[...] + time_step * new_velocity
    new_force = strain_and_force(
        new_displace,
        strain,
        connect,
        left_gradient,
        left_force,
        inverse_jacobian,
        lame_moduli,
        point_weights,
        incidence,
        bool(rest),
    )
    if rest:
        displace, velocity, force, send, next_wave = rest
        next_wave[...] = moved_up(wave)
        displace[...] = new_displace
        velocity[...] = new_velocity
        force[...] = new_force
        send[...] = pick_lanes(new_force, pick_index[...])


def order_kernel(rank, strains, last, out, store):
    for t in range(STEPS):
        for c in range(STRAIN):
            row = (c * STEPS + t) * POINTS
            rows = slice(c * POINTS, (c + 1) * POINTS)
            store[row : row + POINTS, :] = strains[t, rows, :] if t < STEPS - 1 else last[rows, :]
    count = rank.shape[0] * LANES
    lane = lax.broadcasted_iota(jnp.int32, (LANES, count), 1)
    total = None
    for q in range(POINTS):
        values = store[pl.ds(q, STEPS * STRAIN, stride=POINTS), :].astype(jnp.bfloat16)
        column = jnp.broadcast_to(rank[q : q + 1, :], (LANES, LANES)).T
        wide = jnp.concatenate([column] * (count // LANES), axis=1)
        chosen = jnp.where(wide == lane, 1.0, 0.0).astype(jnp.bfloat16)
        part = matmul(values, chosen)
        total = part if total is None else total + part
    for w in range(count // LANES):
        out[w] = total[:, w * LANES : (w + 1) * LANES].astype(jnp.bfloat16)


def place_kernel(pieces, out):
    for w in range(pieces.shape[0]):
        held = snake("dom", w)
        for c in range(STRAIN):
            out[c, :, w * LANES : (w + 1) * LANES] = pieces[held, c * STEPS : (c + 1) * STEPS, :]


def shards(
    connect,
    interface_nodes,
    neighbours,
    point_rank,
    shape_grad,
    inverse_jacobian,
    lame_moduli,
    point_weights,
    mass_elem,
    source_pattern,
    wavelet,
):
    nodes = source_pattern.shape[1]
    f32 = jnp.float32
    field_t = jax.ShapeDtypeStruct((8, nodes), f32)
    lanes_t = jax.ShapeDtypeStruct((8, LANES), f32)
    index_t = jax.ShapeDtypeStruct((8, LANES), jnp.int32)
    strain_t = jax.ShapeDtypeStruct((STRAIN * POINTS, LANES), f32)

    face = lax.broadcasted_iota(jnp.int32, (8, LANES), 1) // (LANES // FACES)
    dom = lax.axis_index("dom")
    parity = jnp.where(face < 2, lax.axis_index("grp") % 2, (dom // DOM_ROW + dom) % 2)
    source = 2 * (face // 2) + jnp.bitwise_xor(parity, 1 - face % 2)

    def exchange(send):
        received = []
        for name in EXCHANGES:
            axis, offset = name[:3], int(name[3])
            count = lax.axis_size(axis)
            pairs = []
            for i in range(offset, count - 1, 2):
                first, second = snake(axis, i), snake(axis, i + 1)
                pairs += [(first, second), (second, first)]
            received.append(lax.ppermute(send, axis, pairs))
        return received

    i32, bf16 = jnp.int32, jnp.bfloat16
    rank_rows = point_rank.reshape(POINTS, LANES)
    arguments = (
        wavelet,
        neighbours,
        connect,
        interface_nodes,
        mass_elem,
        source_pattern,
        shape_grad.T,
        inverse_jacobian,
        lame_moduli,
        point_weights,
        rank_rows,
    )
    buffers = [pltpu.SMEM(x.shape, x.dtype) for x in arguments[:2]]
    buffers += [pltpu.VMEM(x.shape, x.dtype) for x in arguments[2:6] + arguments[7:]]
    packed, shape_t, wave = kernel_call(
        pack_kernel,
        [
            jax.ShapeDtypeStruct((PACKED_ROWS, LANES), f32),
            jax.ShapeDtypeStruct(shape_grad.T.shape, f32),
            jax.ShapeDtypeStruct((STEPS, LANES), f32),
        ],
        [HBM] * len(arguments),
        scratch=buffers + [pltpu.SemaphoreType.DMA((len(arguments),))],
    )(*(pltpu.with_memory_space_constraint(x, pltpu.MemorySpace.HBM) for x in arguments))
    writers = lax.axis_size("dom")
    packed = lax.ppermute(packed, "dom", [(i, snake("dom", i)) for i in range(writers)])
    outs = kernel_call(
        prepare_kernel,
        [
            jax.ShapeDtypeStruct((EL_NODES * LANES, LANES), bf16),
            field_t,
            lanes_t,
            index_t,
            jax.ShapeDtypeStruct((8, nodes), i32),
            jax.ShapeDtypeStruct((NODE_ROWS, LANES), i32),
            jax.ShapeDtypeStruct((9 * POINTS, 3 * GRADIENT_BLOCK), bf16),
            jax.ShapeDtypeStruct((3 * NODE_ROWS, 3 * FORCE_BLOCK), bf16),
            jax.ShapeDtypeStruct(inverse_jacobian.shape, f32),
            jax.ShapeDtypeStruct(lame_moduli.shape, f32),
            jax.ShapeDtypeStruct(point_weights.shape, f32),
            jax.ShapeDtypeStruct(rank_rows.shape, i32),
        ],
        [VMEM, VMEM],
    )(packed, shape_t)
    incidence, field, send, pick_index, inverse_index = outs[:5]
    rank = outs[11]
    element_data = (*outs[5:11], incidence)
    received = exchange(send)
    wave_t = jax.ShapeDtypeStruct((STEPS, LANES), f32)
    strain, displace, velocity, pattern, half_inverse_mass, force, send, wave = kernel_call(
        first_kernel,
        [strain_t, field_t, field_t, field_t, field_t, field_t, lanes_t, wave_t],
        [VMEM] * 16,
    )(wave, *received, source, inverse_index, pick_index, field, *element_data)
    strains = jnp.zeros((STEPS - 1, STRAIN * POINTS, LANES), f32)
    strains = lax.dynamic_update_index_in_dim(strains, strain, 0, 0)

    def advance(last, displace, velocity, force, send, wave):
        received = exchange(send)
        return kernel_call(
            step_kernel,
            [strain_t] + ([] if last else [field_t, field_t, field_t, lanes_t, wave_t]),
            [VMEM] * 20,
        )(
            wave,
            *received,
            source,
            inverse_index,
            pick_index,
            *element_data,
            pattern,
            half_inverse_mass,
            displace,
            velocity,
            force,
        )

    def body(step, carried):
        strains, *state = carried
        strain, *state = advance(False, *state)
        return (lax.dynamic_update_index_in_dim(strains, strain, step, 0), *state)

    carried = (strains, displace, velocity, force, send, wave)
    strains, *state = lax.fori_loop(1, STEPS - 1, body, carried)
    (strain,) = advance(True, *state)
    (ordered,) = kernel_call(
        order_kernel,
        [jax.ShapeDtypeStruct((writers, STEPS * STRAIN, LANES), jnp.bfloat16)],
        [VMEM] * 3,
        scratch=[pltpu.VMEM((STEPS * STRAIN * POINTS, LANES), f32)],
    )(rank, strains, strain)
    pieces = lax.all_to_all(ordered, "dom", split_axis=0, concat_axis=0, tiled=True)
    (placed,) = kernel_call(
        place_kernel, [jax.ShapeDtypeStruct((STRAIN, STEPS, writers * LANES), jnp.bfloat16)], [VMEM]
    )(pieces)
    return placed.transpose(1, 0, 2)


def solution(mesh):
    placed = (
        P(None, ("grp", "dom")),
        P(("grp", "dom"), None, None),
        P(("grp", "dom"), None),
        P(("grp", "dom"), None),
        P(),
        P(None, ("grp", "dom")),
        P(None, ("grp", "dom")),
        P(None, ("grp", "dom")),
        P(None, ("grp", "dom")),
        P(None, ("grp", "dom")),
        P(),
    )
    return jax.shard_map(
        shards, mesh=mesh, in_specs=placed, out_specs=P(None, None, ("grp", "dom")), check_vma=False
    )
```

```python
import jax
import jax.numpy as jnp
from jax import lax
from jax.experimental import pallas as pl
from jax.experimental.pallas import tpu as pltpu
from jax.sharding import PartitionSpec as P


EL_NODES = 20
NODE_ROWS = 24
POINTS = 16
STRAIN = 6
STEPS = 16
LANES = 128
FACES = 4
ORDER_WIDTH = 256

time_step = 0.5

DOM_ROW = 4

EXCHANGES = ("dom1", "grp1", "dom0", "grp0")

VMEM = pl.BlockSpec(memory_space=pltpu.VMEM)
HBM = pl.BlockSpec(memory_space=pltpu.MemorySpace.HBM)


def snake(axis, index):
    row, column = index // DOM_ROW, index % DOM_ROW
    return index if axis == "grp" or row % 2 == 0 else row * DOM_ROW + DOM_ROW - 1 - column


def kernel_call(body, outs, specs, scratch=()):
    return pl.pallas_call(
        body,
        out_shape=outs,
        in_specs=specs,
        out_specs=[VMEM] * len(outs),
        scratch_shapes=list(scratch),
        compiler_params=pltpu.CompilerParams(vmem_limit_bytes=24 * 1024 * 1024),
    )


def parts_of(x):
    high = x.astype(jnp.bfloat16).astype(jnp.float32)
    rest = x - high
    middle = rest.astype(jnp.bfloat16).astype(jnp.float32)
    low = (rest - middle).astype(jnp.bfloat16).astype(jnp.float32)
    return high, middle, low


def matmul(left, right):
    return jnp.dot(left, right, preferred_element_type=jnp.float32)


def lane_gather(row, index):
    return jnp.take_along_axis(row, index, axis=1)


def pick_lanes(field, index):
    low = jnp.bitwise_and(index, LANES - 1)
    chunk = jnp.right_shift(index, 7)
    out = lane_gather(field[:, 0:LANES], low)
    for j in range(1, field.shape[1] // LANES):
        out = jnp.where(
            chunk == j, lane_gather(field[:, j * LANES : (j + 1) * LANES], low), out
        )
    return out


def spread(received, inverse):
    out = []
    for j in range(inverse.shape[1] // LANES):
        index = inverse[:, j * LANES : (j + 1) * LANES]
        taken = lane_gather(received, jnp.maximum(index, 0))
        out.append(jnp.where(index >= 0, taken, 0.0))
    return jnp.concatenate(out, axis=1)


def merge_received(source, dom1, grp1, dom0, grp0):
    out = jnp.where(source == 0, grp0, grp1)
    out = jnp.where(source == 2, dom0, out)
    return jnp.where(source == 3, dom1, out)


def scatter_nodes(pieces, chunks, incidence):
    group = lax.broadcasted_iota(jnp.int32, (8, LANES), 0) // 4
    parts = [[], [], []]
    for piece, chunk in zip(pieces, chunks):
        both = [jnp.where(chunk == group + base, piece, 0.0) for base in (0, 2)]
        for i, part in enumerate(parts_of(jnp.concatenate(both, axis=0))):
            parts[i].append(part.astype(jnp.bfloat16))
    left = jnp.concatenate([jnp.concatenate(p, axis=1) for p in parts], axis=0)
    sums = matmul(left, incidence)
    total = (sums[32:48] + sums[16:32]) + sums[0:16]
    fields = []
    for base in (0, 8):
        rows = total[base : base + 8]
        fields += [rows, pltpu.roll(rows, 4, 0)]
    return jnp.concatenate(fields, axis=1)


CONNECT_ROW = 0
MASS_ROW = 24
LAME_ROW = 44
LISTED_ROW = 46
SWAPPED_ROW = 47
JACOBIAN_ROW = 48
WEIGHTS_ROW = 64
SOURCE_ROW = 80
RANK_ROW = 96
PACKED_ROWS = 112


def set_incidence(packed, incidence):
    element_nodes = packed[CONNECT_ROW : CONNECT_ROW + NODE_ROWS, :].astype(jnp.int32)
    low = jnp.bitwise_and(element_nodes, LANES - 1)
    own_lane = lax.broadcasted_iota(jnp.int32, (LANES, LANES), 1)
    for n in range(EL_NODES):
        column = jnp.broadcast_to(low[n : n + 1, :], (LANES, LANES)).T
        incidence[n * LANES : (n + 1) * LANES, :] = jnp.where(
            column == own_lane, 1.0, 0.0
        ).astype(jnp.bfloat16)


def set_field(packed, incidence, field):
    element_nodes = packed[CONNECT_ROW : CONNECT_ROW + NODE_ROWS, :].astype(jnp.int32)
    chunk = jnp.right_shift(element_nodes, 7)
    masses = [
        jnp.broadcast_to(packed[MASS_ROW + n : MASS_ROW + n + 1, :], (8, LANES))
        for n in range(EL_NODES)
    ]
    chunks = [chunk[n : n + 1, :] for n in range(EL_NODES)]
    field[...] = scatter_nodes(masses, chunks, incidence[...])
    for j in range(field.shape[1] // LANES):
        row = SOURCE_ROW + 3 * j
        field[0:3, j * LANES : (j + 1) * LANES] = packed[row : row + 3, :]


def pack_kernel(
    wavelet_in,
    neighbours_in,
    connect_in,
    lists_in,
    mass_in,
    source_in,
    shape_in,
    jacobian_in,
    lame_in,
    weights_in,
    rank_in,
    packed,
    shape_t,
    wave,
    send,
    wavelet,
    neighbours,
    connect,
    lists,
    mass_elem,
    source_pattern,
    jacobian,
    lame,
    weights,
    rank,
    sems,
    incidence,
    field,
):
    moves = [
        (wavelet_in, wavelet),
        (neighbours_in, neighbours),
        (connect_in, connect),
        (lists_in, lists),
        (mass_in, mass_elem),
        (source_in, source_pattern),
        (shape_in, shape_t),
        (jacobian_in, jacobian),
        (lame_in, lame),
        (weights_in, weights),
        (rank_in, rank),
    ]
    copies = [pltpu.make_async_copy(a, b, sems.at[i]) for i, (a, b) in enumerate(moves)]
    for copy in copies:
        copy.start()
    packed[...] = jnp.zeros(packed.shape, jnp.float32)
    for copy in copies:
        copy.wait()
    wave[...] = jnp.concatenate(
        [jnp.full((1, LANES), wavelet[t], jnp.float32) for t in range(STEPS)], axis=0
    )
    packed[CONNECT_ROW : CONNECT_ROW + EL_NODES, :] = connect[...].astype(jnp.float32)
    packed[MASS_ROW : MASS_ROW + EL_NODES, :] = mass_elem[...]
    packed[LAME_ROW : LAME_ROW + 2, :] = lame[...]
    packed[JACOBIAN_ROW : JACOBIAN_ROW + 9, :] = jacobian[...]
    packed[WEIGHTS_ROW : WEIGHTS_ROW + POINTS, :] = weights[...]
    packed[RANK_ROW : RANK_ROW + POINTS, :] = rank[...].astype(jnp.float32)
    for j in range(source_pattern.shape[1] // LANES):
        row = SOURCE_ROW + 3 * j
        packed[row : row + 3, :] = source_pattern[:, j * LANES : (j + 1) * LANES]
    face = [lists[0, k : k + 1, :] for k in range(FACES)]
    listed = jnp.concatenate(face, axis=1)
    swapped = jnp.concatenate([face[1], face[0], face[3], face[2]], axis=1)
    side = lax.broadcasted_iota(jnp.int32, (1, LANES), 1) // (LANES // FACES)
    open_side = jnp.where(
        side < 2,
        jnp.where(side == 0, neighbours[0, 0], neighbours[0, 1]),
        jnp.where(side == 2, neighbours[0, 2], neighbours[0, 3]),
    )
    listed = jnp.where(open_side != 0, listed, -1)
    packed[LISTED_ROW : LISTED_ROW + 1, :] = listed.astype(jnp.float32)
    packed[SWAPPED_ROW : SWAPPED_ROW + 1, :] = swapped.astype(jnp.float32)
    set_incidence(packed, incidence)
    set_field(packed, incidence, field)
    send[...] = pick_lanes(field[...], jnp.broadcast_to(swapped, (8, LANES)))


def prepare_kernel(
    packed,
    shape_t,
    incidence,
    field,
    pick_index,
    inverse_index,
    connect,
    wide_gradient,
    wide_force,
    inverse_jacobian,
    lame_moduli,
    point_weights,
    rank,
):
    nodes = field.shape[1]
    element_nodes = packed[CONNECT_ROW : CONNECT_ROW + NODE_ROWS, :].astype(jnp.int32)
    connect[...] = element_nodes
    inverse_jacobian[...] = packed[JACOBIAN_ROW : JACOBIAN_ROW + 9, :]
    lame_moduli[...] = packed[LAME_ROW : LAME_ROW + 2, :]
    point_weights[...] = packed[WEIGHTS_ROW : WEIGHTS_ROW + POINTS, :]
    rank[...] = packed[RANK_ROW : RANK_ROW + POINTS, :].astype(jnp.int32)
    set_incidence(packed, incidence)
    lane = lax.broadcasted_iota(jnp.int32, (LANES, nodes), 1)
    listed = packed[LISTED_ROW : LISTED_ROW + 1, :].astype(jnp.int32)
    column = jnp.broadcast_to(listed, (LANES, LANES)).T
    wide = jnp.concatenate([column] * (nodes // LANES), axis=1)
    slot = lax.broadcasted_iota(jnp.int32, (LANES, nodes), 0) + 1
    found = jnp.sum(jnp.where(wide == lane, slot, 0), axis=0, keepdims=True)
    inverse_index[...] = jnp.broadcast_to(found - 1, (8, nodes))
    swapped = packed[SWAPPED_ROW : SWAPPED_ROW + 1, :].astype(jnp.int32)
    index = jnp.broadcast_to(swapped, (8, LANES))
    pick_index[...] = index
    set_field(packed, incidence, field)

    reference_rows = 3 * POINTS
    shape_rows = jnp.concatenate(
        [shape_t[...], jnp.zeros((EL_NODES, LANES - reference_rows), jnp.float32)], axis=1
    )
    shape_rows = jnp.concatenate(
        [shape_rows, jnp.zeros((LANES - EL_NODES, LANES), jnp.float32)], axis=0
    )
    shape_columns = shape_rows.T
    for n in range(EL_NODES):
        wide_gradient[n] = jnp.broadcast_to(
            shape_columns[0:reference_rows, n : n + 1], (reference_rows, LANES)
        )
    for m in range(reference_rows):
        wide_force[m] = jnp.broadcast_to(shape_rows[0:NODE_ROWS, m : m + 1], (NODE_ROWS, LANES))


def contract(table, columns, count):
    sums = [[None, None] for _ in columns]
    for i in range(count):
        weights = table[i]
        for c, column in enumerate(columns):
            term = weights * column[i : i + 1, :]
            old = sums[c][i % 2]
            sums[c][i % 2] = term if old is None else old + term
    return [even + odd for even, odd in sums]


def wave_row(wave, width):
    return jnp.concatenate([wave[0:1, :]] * (width // LANES), axis=1)


def moved_up(wave):
    return pltpu.roll(wave[...], STEPS - 1, 0)


def strain_and_force(
    displace,
    strain,
    connect,
    wide_gradient,
    wide_force,
    inverse_jacobian,
    lame_moduli,
    point_weights,
    incidence,
    need_force,
):
    index = connect[...]
    low = jnp.bitwise_and(index, LANES - 1)
    chunk = jnp.right_shift(index, 7)
    is_chunk = [chunk == j for j in range(1, displace.shape[1] // LANES)]
    columns = []
    for c in range(3):
        pieces = []
        for b in range(NODE_ROWS // 8):
            rows = slice(8 * b, 8 * b + 8)
            out = None
            for j in range(displace.shape[1] // LANES):
                row = jnp.broadcast_to(displace[c : c + 1, j * LANES : (j + 1) * LANES], (8, LANES))
                taken = lane_gather(row, low[rows])
                out = taken if j == 0 else jnp.where(is_chunk[j - 1][rows], taken, out)
            pieces.append(out)
        columns.append(jnp.concatenate(pieces, axis=0))
    along = contract(wide_gradient, columns, EL_NODES)
    jac = [inverse_jacobian[i : i + 1, :] for i in range(9)]

    def ref_derivative(c, r):
        return along[c][r * POINTS : (r + 1) * POINTS, :]

    grad = [
        [
            (ref_derivative(c, 0) * jac[d] + ref_derivative(c, 1) * jac[3 + d])
            + ref_derivative(c, 2) * jac[6 + d]
            for d in range(3)
        ]
        for c in range(3)
    ]
    shear = {(c, d): grad[c][d] + grad[d][c] for c, d in ((1, 2), (0, 2), (0, 1))}
    rows = [grad[0][0], grad[1][1], grad[2][2]] + [0.5 * shear[k] for k in ((1, 2), (0, 2), (0, 1))]
    for s in range(STRAIN):
        strain[s * POINTS : (s + 1) * POINTS, :] = rows[s]
    if not need_force:
        return None
    volume = (grad[0][0] + grad[1][1]) + grad[2][2]
    weights = point_weights[...]
    shear_scale = lame_moduli[1:2, :] * weights
    pressure = (lame_moduli[0:1, :] * weights) * volume
    stress = [[None] * 3 for _ in range(3)]
    for c in range(3):
        for d in range(3):
            if c == d:
                stress[c][d] = shear_scale * (grad[c][c] + grad[c][c]) + pressure
            else:
                stress[c][d] = shear_scale * shear[(min(c, d), max(c, d))]
    columns = []
    for c in range(3):
        mapped = [
            (stress[c][0] * jac[3 * r] + stress[c][1] * jac[3 * r + 1])
            + stress[c][2] * jac[3 * r + 2]
            for r in range(3)
        ]
        columns.append(jnp.concatenate(mapped, axis=0))
    node_forces = contract(wide_force, columns, 3 * POINTS)
    row_id = lax.broadcasted_iota(jnp.int32, (8, LANES), 0) % 4
    pieces = []
    for n in range(EL_NODES):
        first, second, third = (
            jnp.broadcast_to(node_forces[c][n : n + 1, :], (8, LANES))
            for c in range(3)
        )
        pieces.append(jnp.where(row_id == 0, first, jnp.where(row_id == 1, second, third)))
    chunks = [chunk[n : n + 1, :] for n in range(EL_NODES)]
    return scatter_nodes(pieces, chunks, incidence[...])


def first_kernel(
    wave,
    dom1,
    grp1,
    dom0,
    grp0,
    source,
    inverse_index,
    pick_index,
    field,
    connect,
    wide_gradient,
    wide_force,
    inverse_jacobian,
    lame_moduli,
    point_weights,
    incidence,
    strain,
    displace,
    velocity,
    pattern,
    half_inverse_mass,
    force,
    send,
    next_wave,
):
    next_wave[...] = moved_up(wave)
    received = merge_received(source[...], dom1[...], grp1[...], dom0[...], grp0[...])
    total = field[...] + spread(received, inverse_index[...])
    scale = jnp.broadcast_to(time_step * (1.0 / total[3:4, :]), total.shape)
    pattern[...] = total
    half_inverse_mass[...] = scale
    new_velocity = scale * (wave_row(wave, total.shape[1]) * total)
    velocity[...] = new_velocity
    new_displace = time_step * new_velocity
    displace[...] = new_displace
    new_force = strain_and_force(
        new_displace,
        strain,
        connect,
        wide_gradient,
        wide_force,
        inverse_jacobian,
        lame_moduli,
        point_weights,
        incidence,
        True,
    )
    force[...] = new_force
    send[...] = pick_lanes(new_force, pick_index[...])


def step_kernel(
    wave,
    dom1,
    grp1,
    dom0,
    grp0,
    source,
    inverse_index,
    pick_index,
    connect,
    wide_gradient,
    wide_force,
    inverse_jacobian,
    lame_moduli,
    point_weights,
    incidence,
    pattern,
    half_inverse_mass,
    old_displace,
    old_velocity,
    old_force,
    strain,
    *rest,
):
    received = merge_received(source[...], dom1[...], grp1[...], dom0[...], grp0[...])
    stiff = old_force[...] + spread(received, inverse_index[...])
    total = wave_row(wave, stiff.shape[1]) * pattern[...] - stiff
    new_velocity = old_velocity[...] + half_inverse_mass[...] * total
    new_displace = old_displace[...] + time_step * new_velocity
    new_force = strain_and_force(
        new_displace,
        strain,
        connect,
        wide_gradient,
        wide_force,
        inverse_jacobian,
        lame_moduli,
        point_weights,
        incidence,
        bool(rest),
    )
    if rest:
        displace, velocity, force, send, next_wave = rest
        next_wave[...] = moved_up(wave)
        displace[...] = new_displace
        velocity[...] = new_velocity
        force[...] = new_force
        send[...] = pick_lanes(new_force, pick_index[...])


def order_kernel(rank, strains, last, out, store):
    for t in range(STEPS):
        for c in range(STRAIN):
            row = (c * STEPS + t) * POINTS
            rows = slice(c * POINTS, (c + 1) * POINTS)
            store[row : row + POINTS, :] = strains[t, rows, :] if t < STEPS - 1 else last[rows, :]
    lane = lax.broadcasted_iota(jnp.int32, (LANES, ORDER_WIDTH), 1)
    groups = rank.shape[0] * LANES // ORDER_WIDTH
    values, chosen = [], []
    for q in range(POINTS):
        block = store[pl.ds(q, STEPS * STRAIN, stride=POINTS), :]
        row = rank[q : q + 1, :]
        group = row // ORDER_WIDTH
        masked = [jnp.where(group == k, block, 0.0) for k in range(groups)]
        values.append(jnp.concatenate(masked, axis=0).astype(jnp.bfloat16))
        column = jnp.broadcast_to(row % ORDER_WIDTH, (LANES, LANES)).T
        wide = jnp.concatenate([column] * (ORDER_WIDTH // LANES), axis=1)
        chosen.append(jnp.where(wide == lane, 1.0, 0.0).astype(jnp.bfloat16))
    total = matmul(jnp.concatenate(values, axis=1), jnp.concatenate(chosen, axis=0))
    height = STEPS * STRAIN
    for w in range(rank.shape[0]):
        k, i = w * LANES // ORDER_WIDTH, w % (ORDER_WIDTH // LANES)
        block = total[k * height : (k + 1) * height, i * LANES : (i + 1) * LANES]
        out[w] = block.astype(jnp.bfloat16)


def place_kernel(pieces, out):
    for w in range(pieces.shape[0]):
        held = snake("dom", w)
        for c in range(STRAIN):
            out[c, :, w * LANES : (w + 1) * LANES] = pieces[held, c * STEPS : (c + 1) * STEPS, :]


def shards(
    connect,
    interface_nodes,
    neighbours,
    point_rank,
    shape_grad,
    inverse_jacobian,
    lame_moduli,
    point_weights,
    mass_elem,
    source_pattern,
    wavelet,
):
    nodes = source_pattern.shape[1]
    f32 = jnp.float32
    field_t = jax.ShapeDtypeStruct((8, nodes), f32)
    lanes_t = jax.ShapeDtypeStruct((8, LANES), f32)
    index_t = jax.ShapeDtypeStruct((8, LANES), jnp.int32)
    strain_t = jax.ShapeDtypeStruct((STRAIN * POINTS, LANES), f32)

    face = lax.broadcasted_iota(jnp.int32, (8, LANES), 1) // (LANES // FACES)
    dom = lax.axis_index("dom")
    parity = jnp.where(face < 2, lax.axis_index("grp") % 2, (dom // DOM_ROW + dom) % 2)
    source = 2 * (face // 2) + jnp.bitwise_xor(parity, 1 - face % 2)

    def exchange(send):
        received = []
        for name in EXCHANGES:
            axis, offset = name[:3], int(name[3])
            count = lax.axis_size(axis)
            pairs = []
            for i in range(offset, count - 1, 2):
                first, second = snake(axis, i), snake(axis, i + 1)
                pairs += [(first, second), (second, first)]
            received.append(lax.ppermute(send, axis, pairs))
        return received

    i32, bf16 = jnp.int32, jnp.bfloat16
    rank_rows = point_rank.reshape(POINTS, LANES)
    arguments = (
        wavelet,
        neighbours,
        connect,
        interface_nodes,
        mass_elem,
        source_pattern,
        shape_grad.T,
        inverse_jacobian,
        lame_moduli,
        point_weights,
        rank_rows,
    )
    buffers = [pltpu.SMEM(x.shape, x.dtype) for x in arguments[:2]]
    buffers += [pltpu.VMEM(x.shape, x.dtype) for x in arguments[2:6] + arguments[7:]]
    packed, shape_t, wave, send = kernel_call(
        pack_kernel,
        [
            jax.ShapeDtypeStruct((PACKED_ROWS, LANES), f32),
            jax.ShapeDtypeStruct(shape_grad.T.shape, f32),
            jax.ShapeDtypeStruct((STEPS, LANES), f32),
            lanes_t,
        ],
        [HBM] * len(arguments),
        scratch=buffers
        + [
            pltpu.SemaphoreType.DMA((len(arguments),)),
            pltpu.VMEM((EL_NODES * LANES, LANES), bf16),
            pltpu.VMEM(field_t.shape, f32),
        ],
    )(*(pltpu.with_memory_space_constraint(x, pltpu.MemorySpace.HBM) for x in arguments))
    writers = lax.axis_size("dom")
    packed = lax.ppermute(packed, "dom", [(i, snake("dom", i)) for i in range(writers)])
    received = []
    for name in EXCHANGES:
        axis, offset = name[:3], int(name[3])
        pairs = []
        for g in range(lax.axis_size("grp")):
            for w in range(writers):
                index, count = (g, lax.axis_size("grp")) if axis == "grp" else (w, writers)
                other = index + 1 if index % 2 == offset else index - 1
                if 0 <= other < count:
                    to_g, to_w = (other, w) if axis == "grp" else (g, other)
                    target = to_g * writers + snake("dom", to_w)
                    pairs.append((g * writers + w, target))
        received.append(lax.ppermute(send, ("grp", "dom"), pairs))

    prepare = kernel_call(
        prepare_kernel,
        [
            jax.ShapeDtypeStruct((EL_NODES * LANES, LANES), bf16),
            field_t,
            index_t,
            jax.ShapeDtypeStruct((8, nodes), i32),
            jax.ShapeDtypeStruct((NODE_ROWS, LANES), i32),
            jax.ShapeDtypeStruct((EL_NODES, 3 * POINTS, LANES), f32),
            jax.ShapeDtypeStruct((3 * POINTS, NODE_ROWS, LANES), f32),
            jax.ShapeDtypeStruct(inverse_jacobian.shape, f32),
            jax.ShapeDtypeStruct(lame_moduli.shape, f32),
            jax.ShapeDtypeStruct(point_weights.shape, f32),
            jax.ShapeDtypeStruct(rank_rows.shape, i32),
        ],
        [VMEM, VMEM],
    )
    outs = prepare(packed, shape_t)
    incidence, field, pick_index, inverse_index = outs[:4]
    rank = outs[10]
    element_data = (*outs[4:10], incidence)
    wave_t = jax.ShapeDtypeStruct((STEPS, LANES), f32)
    strain, displace, velocity, pattern, half_inverse_mass, force, send, wave = kernel_call(
        first_kernel,
        [strain_t, field_t, field_t, field_t, field_t, field_t, lanes_t, wave_t],
        [VMEM] * 16,
    )(wave, *received, source, inverse_index, pick_index, field, *element_data)
    strains = jnp.zeros((STEPS - 1, STRAIN * POINTS, LANES), f32)
    strains = lax.dynamic_update_index_in_dim(strains, strain, 0, 0)

    def advance(last, displace, velocity, force, send, wave):
        received = exchange(send)
        return kernel_call(
            step_kernel,
            [strain_t] + ([] if last else [field_t, field_t, field_t, lanes_t, wave_t]),
            [VMEM] * 20,
        )(
            wave,
            *received,
            source,
            inverse_index,
            pick_index,
            *element_data,
            pattern,
            half_inverse_mass,
            displace,
            velocity,
            force,
        )

    def body(step, carried):
        strains, *state = carried
        strain, *state = advance(False, *state)
        return (lax.dynamic_update_index_in_dim(strains, strain, step, 0), *state)

    carried = (strains, displace, velocity, force, send, wave)
    strains, *state = lax.fori_loop(1, STEPS - 1, body, carried)
    (strain,) = advance(True, *state)
    (ordered,) = kernel_call(
        order_kernel,
        [jax.ShapeDtypeStruct((writers, STEPS * STRAIN, LANES), jnp.bfloat16)],
        [VMEM] * 3,
        scratch=[pltpu.VMEM((STEPS * STRAIN * POINTS, LANES), f32)],
    )(rank, strains, strain)
    pieces = lax.all_to_all(ordered, "dom", split_axis=0, concat_axis=0, tiled=True)
    (placed,) = kernel_call(
        place_kernel, [jax.ShapeDtypeStruct((STRAIN, STEPS, writers * LANES), jnp.bfloat16)], [VMEM]
    )(pieces)
    return placed.transpose(1, 0, 2)


def solution(mesh):
    placed = (
        P(None, ("grp", "dom")),
        P(("grp", "dom"), None, None),
        P(("grp", "dom"), None),
        P(("grp", "dom"), None),
        P(),
        P(None, ("grp", "dom")),
        P(None, ("grp", "dom")),
        P(None, ("grp", "dom")),
        P(None, ("grp", "dom")),
        P(None, ("grp", "dom")),
        P(),
    )
    return jax.shard_map(
        shards, mesh=mesh, in_specs=placed, out_specs=P(None, None, ("grp", "dom")), check_vma=False
    )
```

```python
import jax
import jax.numpy as jnp
from jax import lax
from jax.experimental import pallas as pl
from jax.experimental.pallas import tpu as pltpu
from jax.sharding import PartitionSpec as P


EL_NODES = 20
NODE_ROWS = 24
POINTS = 16
STRAIN = 6
STEPS = 16
LANES = 128
FACES = 4
ORDER_WIDTH = 256

time_step = 0.5

DOM_ROW = 4

EXCHANGES = ("dom1", "grp1", "dom0", "grp0")

VMEM = pl.BlockSpec(memory_space=pltpu.VMEM)
HBM = pl.BlockSpec(memory_space=pltpu.MemorySpace.HBM)


def snake(axis, index):
    row, column = index // DOM_ROW, index % DOM_ROW
    return index if axis == "grp" or row % 2 == 0 else row * DOM_ROW + DOM_ROW - 1 - column


def kernel_call(body, outs, specs, scratch=()):
    return pl.pallas_call(
        body,
        out_shape=outs,
        in_specs=specs,
        out_specs=[VMEM] * len(outs),
        scratch_shapes=list(scratch),
        compiler_params=pltpu.CompilerParams(vmem_limit_bytes=24 * 1024 * 1024),
    )


def parts_of(x):
    high = x.astype(jnp.bfloat16).astype(jnp.float32)
    rest = x - high
    middle = rest.astype(jnp.bfloat16).astype(jnp.float32)
    low = (rest - middle).astype(jnp.bfloat16).astype(jnp.float32)
    return high, middle, low


def matmul(left, right):
    return jnp.dot(left, right, preferred_element_type=jnp.float32)


def lane_gather(row, index):
    return jnp.take_along_axis(row, index, axis=1)


def pick_lanes(field, index):
    low = jnp.bitwise_and(index, LANES - 1)
    chunk = jnp.right_shift(index, 7)
    out = lane_gather(field[:, 0:LANES], low)
    for j in range(1, field.shape[1] // LANES):
        out = jnp.where(
            chunk == j, lane_gather(field[:, j * LANES : (j + 1) * LANES], low), out
        )
    return out


def spread(received, inverse):
    out = []
    for j in range(inverse.shape[1] // LANES):
        index = inverse[:, j * LANES : (j + 1) * LANES]
        taken = lane_gather(received, jnp.maximum(index, 0))
        out.append(jnp.where(index >= 0, taken, 0.0))
    return jnp.concatenate(out, axis=1)


def merge_received(source, dom1, grp1, dom0, grp0):
    out = jnp.where(source == 0, grp0, grp1)
    out = jnp.where(source == 2, dom0, out)
    return jnp.where(source == 3, dom1, out)


def scatter_nodes(pieces, chunks, incidence):
    group = lax.broadcasted_iota(jnp.int32, (8, LANES), 0) // 4
    parts = [[], [], []]
    for piece, chunk in zip(pieces, chunks):
        both = [jnp.where(chunk == group + base, piece, 0.0) for base in (0, 2)]
        for i, part in enumerate(parts_of(jnp.concatenate(both, axis=0))):
            parts[i].append(part.astype(jnp.bfloat16))
    left = jnp.concatenate([jnp.concatenate(p, axis=1) for p in parts], axis=0)
    sums = matmul(left, incidence)
    total = (sums[32:48] + sums[16:32]) + sums[0:16]
    fields = []
    for base in (0, 8):
        rows = total[base : base + 8]
        fields += [rows, pltpu.roll(rows, 4, 0)]
    return jnp.concatenate(fields, axis=1)


CONNECT_ROW = 0
MASS_ROW = 24
LAME_ROW = 44
LISTED_ROW = 46
SWAPPED_ROW = 47
JACOBIAN_ROW = 48
WEIGHTS_ROW = 64
SOURCE_ROW = 80
RANK_ROW = 96
PACKED_ROWS = 112


def set_incidence(packed, incidence):
    element_nodes = packed[CONNECT_ROW : CONNECT_ROW + NODE_ROWS, :].astype(jnp.int32)
    low = jnp.bitwise_and(element_nodes, LANES - 1)
    own_lane = lax.broadcasted_iota(jnp.int32, (LANES, LANES), 1)
    for n in range(EL_NODES):
        column = jnp.broadcast_to(low[n : n + 1, :], (LANES, LANES)).T
        incidence[n * LANES : (n + 1) * LANES, :] = jnp.where(
            column == own_lane, 1.0, 0.0
        ).astype(jnp.bfloat16)


def set_faces(packed, faces):
    element_nodes = packed[CONNECT_ROW : CONNECT_ROW + NODE_ROWS, :].astype(jnp.int32)
    sent = packed[SWAPPED_ROW : SWAPPED_ROW + 1, :].astype(jnp.int32)
    for n in range(EL_NODES):
        column = jnp.broadcast_to(element_nodes[n : n + 1, :], (LANES, LANES)).T
        faces[n * LANES : (n + 1) * LANES, :] = jnp.where(column == sent, 1.0, 0.0).astype(
            jnp.bfloat16
        )


def set_field(packed, incidence, field):
    element_nodes = packed[CONNECT_ROW : CONNECT_ROW + NODE_ROWS, :].astype(jnp.int32)
    chunk = jnp.right_shift(element_nodes, 7)
    masses = [
        jnp.broadcast_to(packed[MASS_ROW + n : MASS_ROW + n + 1, :], (8, LANES))
        for n in range(EL_NODES)
    ]
    chunks = [chunk[n : n + 1, :] for n in range(EL_NODES)]
    field[...] = scatter_nodes(masses, chunks, incidence[...])
    for j in range(field.shape[1] // LANES):
        row = SOURCE_ROW + 3 * j
        field[0:3, j * LANES : (j + 1) * LANES] = packed[row : row + 3, :]


def pack_kernel(
    wavelet_in,
    neighbours_in,
    connect_in,
    lists_in,
    mass_in,
    source_in,
    shape_in,
    jacobian_in,
    lame_in,
    weights_in,
    rank_in,
    packed,
    shape_t,
    wave,
    send,
    wavelet,
    neighbours,
    connect,
    lists,
    mass_elem,
    source_pattern,
    jacobian,
    lame,
    weights,
    rank,
    sems,
    incidence,
    field,
):
    moves = [
        (wavelet_in, wavelet),
        (neighbours_in, neighbours),
        (connect_in, connect),
        (lists_in, lists),
        (mass_in, mass_elem),
        (source_in, source_pattern),
        (shape_in, shape_t),
        (jacobian_in, jacobian),
        (lame_in, lame),
        (weights_in, weights),
        (rank_in, rank),
    ]
    copies = [pltpu.make_async_copy(a, b, sems.at[i]) for i, (a, b) in enumerate(moves)]
    for copy in copies:
        copy.start()
    packed[...] = jnp.zeros(packed.shape, jnp.float32)
    for copy in copies:
        copy.wait()
    wave[...] = jnp.concatenate(
        [jnp.full((1, LANES), wavelet[t], jnp.float32) for t in range(STEPS)], axis=0
    )
    packed[CONNECT_ROW : CONNECT_ROW + EL_NODES, :] = connect[...].astype(jnp.float32)
    packed[MASS_ROW : MASS_ROW + EL_NODES, :] = mass_elem[...]
    packed[LAME_ROW : LAME_ROW + 2, :] = lame[...]
    packed[JACOBIAN_ROW : JACOBIAN_ROW + 9, :] = jacobian[...]
    packed[WEIGHTS_ROW : WEIGHTS_ROW + POINTS, :] = weights[...]
    packed[RANK_ROW : RANK_ROW + POINTS, :] = rank[...].astype(jnp.float32)
    for j in range(source_pattern.shape[1] // LANES):
        row = SOURCE_ROW + 3 * j
        packed[row : row + 3, :] = source_pattern[:, j * LANES : (j + 1) * LANES]
    face = [lists[0, k : k + 1, :] for k in range(FACES)]
    listed = jnp.concatenate(face, axis=1)
    swapped = jnp.concatenate([face[1], face[0], face[3], face[2]], axis=1)
    side = lax.broadcasted_iota(jnp.int32, (1, LANES), 1) // (LANES // FACES)
    open_side = jnp.where(
        side < 2,
        jnp.where(side == 0, neighbours[0, 0], neighbours[0, 1]),
        jnp.where(side == 2, neighbours[0, 2], neighbours[0, 3]),
    )
    listed = jnp.where(open_side != 0, listed, -1)
    packed[LISTED_ROW : LISTED_ROW + 1, :] = listed.astype(jnp.float32)
    packed[SWAPPED_ROW : SWAPPED_ROW + 1, :] = swapped.astype(jnp.float32)
    set_incidence(packed, incidence)
    set_field(packed, incidence, field)
    send[...] = pick_lanes(field[...], jnp.broadcast_to(swapped, (8, LANES)))


def prepare_kernel(
    packed,
    shape_t,
    incidence,
    field,
    faces,
    inverse_index,
    connect,
    wide_gradient,
    wide_force,
    inverse_jacobian,
    lame_moduli,
    point_weights,
    rank,
):
    nodes = field.shape[1]
    element_nodes = packed[CONNECT_ROW : CONNECT_ROW + NODE_ROWS, :].astype(jnp.int32)
    connect[...] = element_nodes
    inverse_jacobian[...] = packed[JACOBIAN_ROW : JACOBIAN_ROW + 9, :]
    lame_moduli[...] = packed[LAME_ROW : LAME_ROW + 2, :]
    point_weights[...] = packed[WEIGHTS_ROW : WEIGHTS_ROW + POINTS, :]
    rank[...] = packed[RANK_ROW : RANK_ROW + POINTS, :].astype(jnp.int32)
    set_incidence(packed, incidence)
    lane = lax.broadcasted_iota(jnp.int32, (LANES, nodes), 1)
    listed = packed[LISTED_ROW : LISTED_ROW + 1, :].astype(jnp.int32)
    column = jnp.broadcast_to(listed, (LANES, LANES)).T
    wide = jnp.concatenate([column] * (nodes // LANES), axis=1)
    slot = lax.broadcasted_iota(jnp.int32, (LANES, nodes), 0) + 1
    found = jnp.sum(jnp.where(wide == lane, slot, 0), axis=0, keepdims=True)
    inverse_index[...] = jnp.broadcast_to(found - 1, (8, nodes))
    set_faces(packed, faces)
    set_field(packed, incidence, field)

    reference_rows = 3 * POINTS
    shape_rows = jnp.concatenate(
        [shape_t[...], jnp.zeros((EL_NODES, LANES - reference_rows), jnp.float32)], axis=1
    )
    shape_rows = jnp.concatenate(
        [shape_rows, jnp.zeros((LANES - EL_NODES, LANES), jnp.float32)], axis=0
    )
    shape_columns = shape_rows.T
    for n in range(EL_NODES):
        wide_gradient[n] = jnp.broadcast_to(
            shape_columns[0:reference_rows, n : n + 1], (reference_rows, LANES)
        )
    for m in range(reference_rows):
        wide_force[m] = jnp.broadcast_to(shape_rows[0:NODE_ROWS, m : m + 1], (NODE_ROWS, LANES))


def contract(table, columns, count):
    sums = [[None, None] for _ in columns]
    for i in range(count):
        weights = table[i]
        for c, column in enumerate(columns):
            term = weights * column[i : i + 1, :]
            old = sums[c][i % 2]
            sums[c][i % 2] = term if old is None else old + term
    return [even + odd for even, odd in sums]


def wave_row(wave, width):
    return jnp.concatenate([wave[0:1, :]] * (width // LANES), axis=1)


def moved_up(wave):
    return pltpu.roll(wave[...], STEPS - 1, 0)


def strain_and_force(
    displace,
    strain,
    connect,
    wide_gradient,
    wide_force,
    inverse_jacobian,
    lame_moduli,
    point_weights,
    faces,
    need_force,
):
    index = connect[...]
    low = jnp.bitwise_and(index, LANES - 1)
    chunk = jnp.right_shift(index, 7)
    is_chunk = [chunk == j for j in range(1, displace.shape[1] // LANES)]
    columns = []
    for c in range(3):
        pieces = []
        for b in range(NODE_ROWS // 8):
            rows = slice(8 * b, 8 * b + 8)
            out = None
            for j in range(displace.shape[1] // LANES):
                row = jnp.broadcast_to(displace[c : c + 1, j * LANES : (j + 1) * LANES], (8, LANES))
                taken = lane_gather(row, low[rows])
                out = taken if j == 0 else jnp.where(is_chunk[j - 1][rows], taken, out)
            pieces.append(out)
        columns.append(jnp.concatenate(pieces, axis=0))
    along = contract(wide_gradient, columns, EL_NODES)
    jac = [inverse_jacobian[i : i + 1, :] for i in range(9)]

    def ref_derivative(c, r):
        return along[c][r * POINTS : (r + 1) * POINTS, :]

    grad = [
        [
            (ref_derivative(c, 0) * jac[d] + ref_derivative(c, 1) * jac[3 + d])
            + ref_derivative(c, 2) * jac[6 + d]
            for d in range(3)
        ]
        for c in range(3)
    ]
    shear = {(c, d): grad[c][d] + grad[d][c] for c, d in ((1, 2), (0, 2), (0, 1))}
    rows = [grad[0][0], grad[1][1], grad[2][2]] + [0.5 * shear[k] for k in ((1, 2), (0, 2), (0, 1))]
    for s in range(STRAIN):
        strain[s * POINTS : (s + 1) * POINTS, :] = rows[s]
    if not need_force:
        return None
    volume = (grad[0][0] + grad[1][1]) + grad[2][2]
    weights = point_weights[...]
    shear_scale = lame_moduli[1:2, :] * weights
    pressure = (lame_moduli[0:1, :] * weights) * volume
    stress = [[None] * 3 for _ in range(3)]
    for c in range(3):
        for d in range(3):
            if c == d:
                stress[c][d] = shear_scale * (grad[c][c] + grad[c][c]) + pressure
            else:
                stress[c][d] = shear_scale * shear[(min(c, d), max(c, d))]
    columns = []
    for c in range(3):
        mapped = [
            (stress[c][0] * jac[3 * r] + stress[c][1] * jac[3 * r + 1])
            + stress[c][2] * jac[3 * r + 2]
            for r in range(3)
        ]
        columns.append(jnp.concatenate(mapped, axis=0))
    node_forces = contract(wide_force, columns, 3 * POINTS)
    parts = parts_of(jnp.concatenate(node_rows(node_forces), axis=1))
    sums = matmul(jnp.concatenate(parts, axis=0).astype(jnp.bfloat16), faces[...])
    return node_forces, (sums[16:24] + sums[8:16]) + sums[0:8]


def node_rows(node_forces):
    row_id = lax.broadcasted_iota(jnp.int32, (8, LANES), 0) % 4
    pieces = []
    for n in range(EL_NODES):
        first, second, third = (
            jnp.broadcast_to(node_forces[c][n : n + 1, :], (8, LANES)) for c in range(3)
        )
        pieces.append(jnp.where(row_id == 0, first, jnp.where(row_id == 1, second, third)))
    return pieces


def scatter_kernel(node_forces, connect, incidence, force):
    parts = [node_forces[c] for c in range(3)]
    chunk = jnp.right_shift(connect[...], 7)
    chunks = [chunk[n : n + 1, :] for n in range(EL_NODES)]
    force[...] = scatter_nodes(node_rows(parts), chunks, incidence[...])


def keep_forces(result, node_forces, send):
    forces, faces = result
    for c in range(3):
        node_forces[c] = forces[c]
    send[...] = faces


def first_kernel(
    wave,
    dom1,
    grp1,
    dom0,
    grp0,
    source,
    inverse_index,
    field,
    connect,
    wide_gradient,
    wide_force,
    inverse_jacobian,
    lame_moduli,
    point_weights,
    faces,
    strain,
    displace,
    velocity,
    pattern,
    half_inverse_mass,
    node_forces,
    send,
    next_wave,
):
    next_wave[...] = moved_up(wave)
    received = merge_received(source[...], dom1[...], grp1[...], dom0[...], grp0[...])
    total = field[...] + spread(received, inverse_index[...])
    scale = jnp.broadcast_to(time_step * (1.0 / total[3:4, :]), total.shape)
    pattern[...] = total
    half_inverse_mass[...] = scale
    new_velocity = scale * (wave_row(wave, total.shape[1]) * total)
    velocity[...] = new_velocity
    new_displace = time_step * new_velocity
    displace[...] = new_displace
    result = strain_and_force(
        new_displace,
        strain,
        connect,
        wide_gradient,
        wide_force,
        inverse_jacobian,
        lame_moduli,
        point_weights,
        faces,
        True,
    )
    keep_forces(result, node_forces, send)


def step_kernel(
    wave,
    dom1,
    grp1,
    dom0,
    grp0,
    source,
    inverse_index,
    connect,
    wide_gradient,
    wide_force,
    inverse_jacobian,
    lame_moduli,
    point_weights,
    faces,
    pattern,
    half_inverse_mass,
    old_displace,
    old_velocity,
    old_force,
    strain,
    *rest,
):
    received = merge_received(source[...], dom1[...], grp1[...], dom0[...], grp0[...])
    stiff = old_force[...] + spread(received, inverse_index[...])
    total = wave_row(wave, stiff.shape[1]) * pattern[...] - stiff
    new_velocity = old_velocity[...] + half_inverse_mass[...] * total
    new_displace = old_displace[...] + time_step * new_velocity
    result = strain_and_force(
        new_displace,
        strain,
        connect,
        wide_gradient,
        wide_force,
        inverse_jacobian,
        lame_moduli,
        point_weights,
        faces,
        bool(rest),
    )
    if rest:
        displace, velocity, node_forces, send, next_wave = rest
        next_wave[...] = moved_up(wave)
        displace[...] = new_displace
        velocity[...] = new_velocity
        keep_forces(result, node_forces, send)


def order_kernel(rank, strains, last, out, store):
    for t in range(STEPS):
        for c in range(STRAIN):
            row = (c * STEPS + t) * POINTS
            rows = slice(c * POINTS, (c + 1) * POINTS)
            store[row : row + POINTS, :] = strains[t, rows, :] if t < STEPS - 1 else last[rows, :]
    lane = lax.broadcasted_iota(jnp.int32, (LANES, ORDER_WIDTH), 1)
    groups = rank.shape[0] * LANES // ORDER_WIDTH
    values, chosen = [], []
    for q in range(POINTS):
        block = store[pl.ds(q, STEPS * STRAIN, stride=POINTS), :]
        row = rank[q : q + 1, :]
        group = row // ORDER_WIDTH
        masked = [jnp.where(group == k, block, 0.0) for k in range(groups)]
        values.append(jnp.concatenate(masked, axis=0).astype(jnp.bfloat16))
        column = jnp.broadcast_to(row % ORDER_WIDTH, (LANES, LANES)).T
        wide = jnp.concatenate([column] * (ORDER_WIDTH // LANES), axis=1)
        chosen.append(jnp.where(wide == lane, 1.0, 0.0).astype(jnp.bfloat16))
    total = matmul(jnp.concatenate(values, axis=1), jnp.concatenate(chosen, axis=0))
    height = STEPS * STRAIN
    for w in range(rank.shape[0]):
        k, i = w * LANES // ORDER_WIDTH, w % (ORDER_WIDTH // LANES)
        block = total[k * height : (k + 1) * height, i * LANES : (i + 1) * LANES]
        out[w] = block.astype(jnp.bfloat16)


def place_kernel(pieces, out):
    for w in range(pieces.shape[0]):
        held = snake("dom", w)
        for c in range(STRAIN):
            out[c, :, w * LANES : (w + 1) * LANES] = pieces[held, c * STEPS : (c + 1) * STEPS, :]


def shards(
    connect,
    interface_nodes,
    neighbours,
    point_rank,
    shape_grad,
    inverse_jacobian,
    lame_moduli,
    point_weights,
    mass_elem,
    source_pattern,
    wavelet,
):
    nodes = source_pattern.shape[1]
    f32 = jnp.float32
    field_t = jax.ShapeDtypeStruct((8, nodes), f32)
    lanes_t = jax.ShapeDtypeStruct((8, LANES), f32)
    strain_t = jax.ShapeDtypeStruct((STRAIN * POINTS, LANES), f32)

    face = lax.broadcasted_iota(jnp.int32, (8, LANES), 1) // (LANES // FACES)
    dom = lax.axis_index("dom")
    parity = jnp.where(face < 2, lax.axis_index("grp") % 2, (dom // DOM_ROW + dom) % 2)
    source = 2 * (face // 2) + jnp.bitwise_xor(parity, 1 - face % 2)

    def exchange(send):
        received = []
        for name in EXCHANGES:
            axis, offset = name[:3], int(name[3])
            count = lax.axis_size(axis)
            pairs = []
            for i in range(offset, count - 1, 2):
                first, second = snake(axis, i), snake(axis, i + 1)
                pairs += [(first, second), (second, first)]
            received.append(lax.ppermute(send, axis, pairs))
        return received

    i32, bf16 = jnp.int32, jnp.bfloat16
    rank_rows = point_rank.reshape(POINTS, LANES)
    arguments = (
        wavelet,
        neighbours,
        connect,
        interface_nodes,
        mass_elem,
        source_pattern,
        shape_grad.T,
        inverse_jacobian,
        lame_moduli,
        point_weights,
        rank_rows,
    )
    buffers = [pltpu.SMEM(x.shape, x.dtype) for x in arguments[:2]]
    buffers += [pltpu.VMEM(x.shape, x.dtype) for x in arguments[2:6] + arguments[7:]]
    packed, shape_t, wave, send = kernel_call(
        pack_kernel,
        [
            jax.ShapeDtypeStruct((PACKED_ROWS, LANES), f32),
            jax.ShapeDtypeStruct(shape_grad.T.shape, f32),
            jax.ShapeDtypeStruct((STEPS, LANES), f32),
            lanes_t,
        ],
        [HBM] * len(arguments),
        scratch=buffers
        + [
            pltpu.SemaphoreType.DMA((len(arguments),)),
            pltpu.VMEM((EL_NODES * LANES, LANES), bf16),
            pltpu.VMEM(field_t.shape, f32),
        ],
    )(*(pltpu.with_memory_space_constraint(x, pltpu.MemorySpace.HBM) for x in arguments))
    writers = lax.axis_size("dom")
    packed = lax.ppermute(packed, "dom", [(i, snake("dom", i)) for i in range(writers)])
    received = []
    for name in EXCHANGES:
        axis, offset = name[:3], int(name[3])
        pairs = []
        for g in range(lax.axis_size("grp")):
            for w in range(writers):
                index, count = (g, lax.axis_size("grp")) if axis == "grp" else (w, writers)
                other = index + 1 if index % 2 == offset else index - 1
                if 0 <= other < count:
                    to_g, to_w = (other, w) if axis == "grp" else (g, other)
                    target = to_g * writers + snake("dom", to_w)
                    pairs.append((g * writers + w, target))
        received.append(lax.ppermute(send, ("grp", "dom"), pairs))

    prepare = kernel_call(
        prepare_kernel,
        [
            jax.ShapeDtypeStruct((EL_NODES * LANES, LANES), bf16),
            field_t,
            jax.ShapeDtypeStruct((EL_NODES * LANES, LANES), bf16),
            jax.ShapeDtypeStruct((8, nodes), i32),
            jax.ShapeDtypeStruct((NODE_ROWS, LANES), i32),
            jax.ShapeDtypeStruct((EL_NODES, 3 * POINTS, LANES), f32),
            jax.ShapeDtypeStruct((3 * POINTS, NODE_ROWS, LANES), f32),
            jax.ShapeDtypeStruct(inverse_jacobian.shape, f32),
            jax.ShapeDtypeStruct(lame_moduli.shape, f32),
            jax.ShapeDtypeStruct(point_weights.shape, f32),
            jax.ShapeDtypeStruct(rank_rows.shape, i32),
        ],
        [VMEM, VMEM],
    )
    outs = prepare(packed, shape_t)
    incidence, field, faces, inverse_index = outs[:4]
    rank = outs[10]
    connect_rows = outs[4]
    element_data = (*outs[4:10], faces)
    wave_t = jax.ShapeDtypeStruct((STEPS, LANES), f32)
    forces_t = jax.ShapeDtypeStruct((3, NODE_ROWS, LANES), f32)
    strain, displace, velocity, pattern, half_inverse_mass, node_forces, send, wave = kernel_call(
        first_kernel,
        [strain_t, field_t, field_t, field_t, field_t, forces_t, lanes_t, wave_t],
        [VMEM] * 15,
    )(wave, *received, source, inverse_index, field, *element_data)
    strains = jnp.zeros((STEPS - 1, STRAIN * POINTS, LANES), f32)
    strains = lax.dynamic_update_index_in_dim(strains, strain, 0, 0)

    def advance(last, displace, velocity, node_forces, send, wave):
        received = exchange(send)
        scatter = kernel_call(scatter_kernel, [field_t], [VMEM] * 3)
        (force,) = scatter(node_forces, connect_rows, incidence)
        return kernel_call(
            step_kernel,
            [strain_t] + ([] if last else [field_t, field_t, forces_t, lanes_t, wave_t]),
            [VMEM] * 19,
        )(
            wave,
            *received,
            source,
            inverse_index,
            *element_data,
            pattern,
            half_inverse_mass,
            displace,
            velocity,
            force,
        )

    def body(step, carried):
        strains, *state = carried
        strain, *state = advance(False, *state)
        return (lax.dynamic_update_index_in_dim(strains, strain, step, 0), *state)

    carried = (strains, displace, velocity, node_forces, send, wave)
    strains, *state = lax.fori_loop(1, STEPS - 1, body, carried)
    (strain,) = advance(True, *state)
    (ordered,) = kernel_call(
        order_kernel,
        [jax.ShapeDtypeStruct((writers, STEPS * STRAIN, LANES), jnp.bfloat16)],
        [VMEM] * 3,
        scratch=[pltpu.VMEM((STEPS * STRAIN * POINTS, LANES), f32)],
    )(rank, strains, strain)
    pieces = lax.all_to_all(ordered, "dom", split_axis=0, concat_axis=0, tiled=True)
    (placed,) = kernel_call(
        place_kernel, [jax.ShapeDtypeStruct((STRAIN, STEPS, writers * LANES), jnp.bfloat16)], [VMEM]
    )(pieces)
    return placed.transpose(1, 0, 2)


def solution(mesh):
    placed = (
        P(None, ("grp", "dom")),
        P(("grp", "dom"), None, None),
        P(("grp", "dom"), None),
        P(("grp", "dom"), None),
        P(),
        P(None, ("grp", "dom")),
        P(None, ("grp", "dom")),
        P(None, ("grp", "dom")),
        P(None, ("grp", "dom")),
        P(None, ("grp", "dom")),
        P(),
    )
    return jax.shard_map(
        shards, mesh=mesh, in_specs=placed, out_specs=P(None, None, ("grp", "dom")), check_vma=False
    )
```

```python
import jax
import jax.numpy as jnp
from jax import lax
from jax.experimental import pallas as pl
from jax.experimental.pallas import tpu as pltpu
from jax.sharding import PartitionSpec as P


EL_NODES = 20
NODE_ROWS = 24
POINTS = 16
STRAIN = 6
STEPS = 16
LANES = 128
FACES = 4
ORDER_WIDTH = 256

time_step = 0.5

DOM_ROW = 4

EXCHANGES = ("dom1", "grp1", "dom0", "grp0")

VMEM = pl.BlockSpec(memory_space=pltpu.VMEM)
HBM = pl.BlockSpec(memory_space=pltpu.MemorySpace.HBM)


def snake(axis, index):
    row, column = index // DOM_ROW, index % DOM_ROW
    return index if axis == "grp" or row % 2 == 0 else row * DOM_ROW + DOM_ROW - 1 - column


def kernel_call(body, outs, specs, scratch=()):
    return pl.pallas_call(
        body,
        out_shape=outs,
        in_specs=specs,
        out_specs=[VMEM] * len(outs),
        scratch_shapes=list(scratch),
        compiler_params=pltpu.CompilerParams(vmem_limit_bytes=24 * 1024 * 1024),
    )


def parts_of(x):
    high = x.astype(jnp.bfloat16).astype(jnp.float32)
    rest = x - high
    middle = rest.astype(jnp.bfloat16).astype(jnp.float32)
    low = (rest - middle).astype(jnp.bfloat16).astype(jnp.float32)
    return high, middle, low


def matmul(left, right):
    return jnp.dot(left, right, preferred_element_type=jnp.float32)


def lane_gather(row, index):
    return jnp.take_along_axis(row, index, axis=1)


def pick_lanes(field, index):
    low = jnp.bitwise_and(index, LANES - 1)
    chunk = jnp.right_shift(index, 7)
    out = lane_gather(field[:, 0:LANES], low)
    for j in range(1, field.shape[1] // LANES):
        out = jnp.where(
            chunk == j, lane_gather(field[:, j * LANES : (j + 1) * LANES], low), out
        )
    return out


def spread(received, inverse):
    out = []
    for j in range(inverse.shape[1] // LANES):
        index = inverse[:, j * LANES : (j + 1) * LANES]
        taken = lane_gather(received, jnp.maximum(index, 0))
        out.append(jnp.where(index >= 0, taken, 0.0))
    return jnp.concatenate(out, axis=1)


def early_received(source, dom1, grp1):
    return jnp.where(source == 3, dom1, jnp.where(source == 1, grp1, 0.0))


def late_received(source, dom0, grp0):
    return jnp.where(source == 2, dom0, jnp.where(source == 0, grp0, 0.0))


def scatter_nodes(pieces, chunks, incidence):
    group = lax.broadcasted_iota(jnp.int32, (8, LANES), 0) // 4
    parts = [[], [], []]
    for piece, chunk in zip(pieces, chunks):
        both = [jnp.where(chunk == group + base, piece, 0.0) for base in (0, 2)]
        for i, part in enumerate(parts_of(jnp.concatenate(both, axis=0))):
            parts[i].append(part.astype(jnp.bfloat16))
    left = jnp.concatenate([jnp.concatenate(p, axis=1) for p in parts], axis=0)
    sums = matmul(left, incidence)
    total = (sums[32:48] + sums[16:32]) + sums[0:16]
    fields = []
    for base in (0, 8):
        rows = total[base : base + 8]
        fields += [rows, pltpu.roll(rows, 4, 0)]
    return jnp.concatenate(fields, axis=1)


CONNECT_ROW = 0
MASS_ROW = 24
LAME_ROW = 44
LISTED_ROW = 46
SWAPPED_ROW = 47
JACOBIAN_ROW = 48
WEIGHTS_ROW = 64
SOURCE_ROW = 80
RANK_ROW = 96
PACKED_ROWS = 112


def set_incidence(packed, incidence):
    element_nodes = packed[CONNECT_ROW : CONNECT_ROW + NODE_ROWS, :].astype(jnp.int32)
    low = jnp.bitwise_and(element_nodes, LANES - 1)
    own_lane = lax.broadcasted_iota(jnp.int32, (LANES, LANES), 1)
    for n in range(EL_NODES):
        column = jnp.broadcast_to(low[n : n + 1, :], (LANES, LANES)).T
        incidence[n * LANES : (n + 1) * LANES, :] = jnp.where(
            column == own_lane, 1.0, 0.0
        ).astype(jnp.bfloat16)


def set_faces(packed, faces):
    element_nodes = packed[CONNECT_ROW : CONNECT_ROW + NODE_ROWS, :].astype(jnp.int32)
    sent = packed[SWAPPED_ROW : SWAPPED_ROW + 1, :].astype(jnp.int32)
    for n in range(EL_NODES):
        column = jnp.broadcast_to(element_nodes[n : n + 1, :], (LANES, LANES)).T
        faces[n * LANES : (n + 1) * LANES, :] = jnp.where(column == sent, 1.0, 0.0).astype(
            jnp.bfloat16
        )


def set_field(packed, incidence, field):
    element_nodes = packed[CONNECT_ROW : CONNECT_ROW + NODE_ROWS, :].astype(jnp.int32)
    chunk = jnp.right_shift(element_nodes, 7)
    masses = [
        jnp.broadcast_to(packed[MASS_ROW + n : MASS_ROW + n + 1, :], (8, LANES))
        for n in range(EL_NODES)
    ]
    chunks = [chunk[n : n + 1, :] for n in range(EL_NODES)]
    field[...] = scatter_nodes(masses, chunks, incidence[...])
    for j in range(field.shape[1] // LANES):
        row = SOURCE_ROW + 3 * j
        field[0:3, j * LANES : (j + 1) * LANES] = packed[row : row + 3, :]


def pack_kernel(
    wavelet_in,
    neighbours_in,
    connect_in,
    lists_in,
    mass_in,
    source_in,
    shape_in,
    jacobian_in,
    lame_in,
    weights_in,
    rank_in,
    packed,
    shape_t,
    wave,
    send,
    wavelet,
    neighbours,
    connect,
    lists,
    mass_elem,
    source_pattern,
    jacobian,
    lame,
    weights,
    rank,
    sems,
    incidence,
    field,
):
    moves = [
        (wavelet_in, wavelet),
        (neighbours_in, neighbours),
        (connect_in, connect),
        (lists_in, lists),
        (mass_in, mass_elem),
        (source_in, source_pattern),
        (shape_in, shape_t),
        (jacobian_in, jacobian),
        (lame_in, lame),
        (weights_in, weights),
        (rank_in, rank),
    ]
    copies = [pltpu.make_async_copy(a, b, sems.at[i]) for i, (a, b) in enumerate(moves)]
    for copy in copies:
        copy.start()
    packed[...] = jnp.zeros(packed.shape, jnp.float32)
    for copy in copies:
        copy.wait()
    wave[...] = jnp.concatenate(
        [jnp.full((1, LANES), wavelet[t], jnp.float32) for t in range(STEPS)], axis=0
    )
    packed[CONNECT_ROW : CONNECT_ROW + EL_NODES, :] = connect[...].astype(jnp.float32)
    packed[MASS_ROW : MASS_ROW + EL_NODES, :] = mass_elem[...]
    packed[LAME_ROW : LAME_ROW + 2, :] = lame[...]
    packed[JACOBIAN_ROW : JACOBIAN_ROW + 9, :] = jacobian[...]
    packed[WEIGHTS_ROW : WEIGHTS_ROW + POINTS, :] = weights[...]
    packed[RANK_ROW : RANK_ROW + POINTS, :] = rank[...].astype(jnp.float32)
    for j in range(source_pattern.shape[1] // LANES):
        row = SOURCE_ROW + 3 * j
        packed[row : row + 3, :] = source_pattern[:, j * LANES : (j + 1) * LANES]
    face = [lists[0, k : k + 1, :] for k in range(FACES)]
    listed = jnp.concatenate(face, axis=1)
    swapped = jnp.concatenate([face[1], face[0], face[3], face[2]], axis=1)
    side = lax.broadcasted_iota(jnp.int32, (1, LANES), 1) // (LANES // FACES)
    open_side = jnp.where(
        side < 2,
        jnp.where(side == 0, neighbours[0, 0], neighbours[0, 1]),
        jnp.where(side == 2, neighbours[0, 2], neighbours[0, 3]),
    )
    listed = jnp.where(open_side != 0, listed, -1)
    packed[LISTED_ROW : LISTED_ROW + 1, :] = listed.astype(jnp.float32)
    packed[SWAPPED_ROW : SWAPPED_ROW + 1, :] = swapped.astype(jnp.float32)
    set_incidence(packed, incidence)
    set_field(packed, incidence, field)
    send[...] = pick_lanes(field[...], jnp.broadcast_to(swapped, (8, LANES)))


def prepare_kernel(
    packed,
    shape_t,
    source,
    incidence,
    field,
    faces,
    inverse_index,
    connect,
    wide_gradient,
    wide_force,
    inverse_jacobian,
    lame_moduli,
    point_weights,
    rank,
    late_index,
    listed_index,
):
    nodes = field.shape[1]
    element_nodes = packed[CONNECT_ROW : CONNECT_ROW + NODE_ROWS, :].astype(jnp.int32)
    connect[...] = element_nodes
    inverse_jacobian[...] = packed[JACOBIAN_ROW : JACOBIAN_ROW + 9, :]
    lame_moduli[...] = packed[LAME_ROW : LAME_ROW + 2, :]
    point_weights[...] = packed[WEIGHTS_ROW : WEIGHTS_ROW + POINTS, :]
    rank[...] = packed[RANK_ROW : RANK_ROW + POINTS, :].astype(jnp.int32)
    set_incidence(packed, incidence)
    lane = lax.broadcasted_iota(jnp.int32, (LANES, nodes), 1)
    listed = packed[LISTED_ROW : LISTED_ROW + 1, :].astype(jnp.int32)
    column = jnp.broadcast_to(listed, (LANES, LANES)).T
    wide = jnp.concatenate([column] * (nodes // LANES), axis=1)
    late = jnp.broadcast_to(256 * (1 - source[0:1, :] % 2), (LANES, LANES)).T
    late = jnp.concatenate([late] * (nodes // LANES), axis=1)
    slot = lax.broadcasted_iota(jnp.int32, (LANES, nodes), 0) + 1 + late
    found = jnp.sum(jnp.where(wide == lane, slot, 0), axis=0, keepdims=True)
    placed = jnp.bitwise_and(found, 255) - 1
    inverse_index[...] = jnp.broadcast_to(placed, (8, nodes))
    late_row = jnp.where(found >= 256, placed, -1).astype(jnp.float32)
    late_row = jnp.broadcast_to(late_row, (8, nodes))
    for b in range(NODE_ROWS // 8):
        rows = slice(8 * b, 8 * b + 8)
        late_index[rows, :] = pick_lanes(late_row, element_nodes[rows]).astype(jnp.int32)
    listed_index[...] = jnp.broadcast_to(jnp.maximum(listed, 0), (8, LANES))
    set_faces(packed, faces)
    set_field(packed, incidence, field)

    reference_rows = 3 * POINTS
    shape_rows = jnp.concatenate(
        [shape_t[...], jnp.zeros((EL_NODES, LANES - reference_rows), jnp.float32)], axis=1
    )
    shape_rows = jnp.concatenate(
        [shape_rows, jnp.zeros((LANES - EL_NODES, LANES), jnp.float32)], axis=0
    )
    shape_columns = shape_rows.T
    for n in range(EL_NODES):
        wide_gradient[n] = jnp.broadcast_to(
            shape_columns[0:reference_rows, n : n + 1], (reference_rows, LANES)
        )
    for m in range(reference_rows):
        wide_force[m] = jnp.broadcast_to(shape_rows[0:NODE_ROWS, m : m + 1], (NODE_ROWS, LANES))


def contract(table, columns, count):
    sums = [[None, None] for _ in columns]
    for i in range(count):
        weights = table[i]
        for c, column in enumerate(columns):
            term = weights * column[i : i + 1, :]
            old = sums[c][i % 2]
            sums[c][i % 2] = term if old is None else old + term
    return [even + odd for even, odd in sums]


def wave_row(wave, width):
    return jnp.concatenate([wave[0:1, :]] * (width // LANES), axis=1)


def moved_up(wave):
    return pltpu.roll(wave[...], STEPS - 1, 0)


def at_elements(displace, connect):
    index = connect[...]
    columns = []
    for c in range(3):
        pieces = []
        for b in range(NODE_ROWS // 8):
            row = jnp.broadcast_to(displace[c : c + 1, :], (8, displace.shape[1]))
            pieces.append(pick_lanes(row, index[8 * b : 8 * b + 8]))
        columns.append(jnp.concatenate(pieces, axis=0))
    return columns


def strain_and_force(
    columns,
    strain,
    wide_gradient,
    wide_force,
    inverse_jacobian,
    lame_moduli,
    point_weights,
    faces,
    need_force,
):
    along = contract(wide_gradient, columns, EL_NODES)
    jac = [inverse_jacobian[i : i + 1, :] for i in range(9)]

    def ref_derivative(c, r):
        return along[c][r * POINTS : (r + 1) * POINTS, :]

    grad = [
        [
            (ref_derivative(c, 0) * jac[d] + ref_derivative(c, 1) * jac[3 + d])
            + ref_derivative(c, 2) * jac[6 + d]
            for d in range(3)
        ]
        for c in range(3)
    ]
    shear = {(c, d): grad[c][d] + grad[d][c] for c, d in ((1, 2), (0, 2), (0, 1))}
    rows = [grad[0][0], grad[1][1], grad[2][2]] + [0.5 * shear[k] for k in ((1, 2), (0, 2), (0, 1))]
    for s in range(STRAIN):
        strain[s * POINTS : (s + 1) * POINTS, :] = rows[s]
    if not need_force:
        return None
    volume = (grad[0][0] + grad[1][1]) + grad[2][2]
    weights = point_weights[...]
    shear_scale = lame_moduli[1:2, :] * weights
    pressure = (lame_moduli[0:1, :] * weights) * volume
    stress = [[None] * 3 for _ in range(3)]
    for c in range(3):
        for d in range(3):
            if c == d:
                stress[c][d] = shear_scale * (grad[c][c] + grad[c][c]) + pressure
            else:
                stress[c][d] = shear_scale * shear[(min(c, d), max(c, d))]
    columns = []
    for c in range(3):
        mapped = [
            (stress[c][0] * jac[3 * r] + stress[c][1] * jac[3 * r + 1])
            + stress[c][2] * jac[3 * r + 2]
            for r in range(3)
        ]
        columns.append(jnp.concatenate(mapped, axis=0))
    node_forces = contract(wide_force, columns, 3 * POINTS)
    parts = parts_of(jnp.concatenate(node_rows(node_forces), axis=1))
    sums = matmul(jnp.concatenate(parts, axis=0).astype(jnp.bfloat16), faces[...])
    return node_forces, (sums[16:24] + sums[8:16]) + sums[0:8]


def node_rows(node_forces):
    row_id = lax.broadcasted_iota(jnp.int32, (8, LANES), 0) % 4
    pieces = []
    for n in range(EL_NODES):
        first, second, third = (
            jnp.broadcast_to(node_forces[c][n : n + 1, :], (8, LANES)) for c in range(3)
        )
        pieces.append(jnp.where(row_id == 0, first, jnp.where(row_id == 1, second, third)))
    return pieces


def keep_forces(result, node_forces, send):
    forces, faces = result
    for c in range(3):
        node_forces[c] = forces[c]
    send[...] = faces


def first_kernel(
    wave,
    dom1,
    grp1,
    dom0,
    grp0,
    source,
    inverse_index,
    listed_index,
    field,
    connect,
    wide_gradient,
    wide_force,
    inverse_jacobian,
    lame_moduli,
    point_weights,
    faces,
    strain,
    displace,
    velocity,
    pattern,
    half_inverse_mass,
    late_scale,
    node_forces,
    send,
    next_wave,
):
    next_wave[...] = moved_up(wave)
    received = early_received(source[...], dom1[...], grp1[...])
    received = received + late_received(source[...], dom0[...], grp0[...])
    total = field[...] + spread(received, inverse_index[...])
    scale = jnp.broadcast_to(time_step * (1.0 / total[3:4, :]), total.shape)
    pattern[...] = total
    half_inverse_mass[...] = scale
    late_scale[...] = time_step * pick_lanes(scale, listed_index[...])
    new_velocity = scale * (wave_row(wave, total.shape[1]) * total)
    velocity[...] = new_velocity
    new_displace = time_step * new_velocity
    displace[...] = new_displace
    result = strain_and_force(
        at_elements(new_displace, connect),
        strain,
        wide_gradient,
        wide_force,
        inverse_jacobian,
        lame_moduli,
        point_weights,
        faces,
        True,
    )
    keep_forces(result, node_forces, send)


def side_kernel(
    wave,
    dom1,
    grp1,
    last_dom0,
    last_grp0,
    source,
    inverse_index,
    connect,
    incidence,
    pattern,
    half_inverse_mass,
    old_displace,
    old_velocity,
    node_forces,
    displace,
    velocity,
    columns,
    next_wave,
):
    next_wave[...] = moved_up(wave)
    index, scale = inverse_index[...], half_inverse_mass[...]
    missing = spread(late_received(source[...], last_dom0[...], last_grp0[...]), index) * scale
    parts = [node_forces[c] for c in range(3)]
    chunk = jnp.right_shift(connect[...], 7)
    chunks = [chunk[n : n + 1, :] for n in range(EL_NODES)]
    force = scatter_nodes(node_rows(parts), chunks, incidence[...])
    stiff = force + spread(early_received(source[...], dom1[...], grp1[...]), index)
    total = wave_row(wave, stiff.shape[1]) * pattern[...] - stiff
    new_velocity = (old_velocity[...] - missing) + scale * total
    velocity[...] = new_velocity
    new_displace = (old_displace[...] - time_step * missing) + time_step * new_velocity
    displace[...] = new_displace
    for c, column in enumerate(at_elements(new_displace, connect)):
        columns[c] = column


def step_kernel(
    dom0,
    grp0,
    source,
    late_index,
    late_scale,
    base_columns,
    wide_gradient,
    wide_force,
    inverse_jacobian,
    lame_moduli,
    point_weights,
    faces,
    strain,
    *rest,
):
    late = late_scale[...] * late_received(source[...], dom0[...], grp0[...])
    columns = []
    for c in range(3):
        row = jnp.broadcast_to(late[c : c + 1, :], (8, LANES))
        pieces = []
        for b in range(NODE_ROWS // 8):
            index = late_index[8 * b : 8 * b + 8, :]
            taken = jnp.where(index >= 0, lane_gather(row, jnp.maximum(index, 0)), 0.0)
            pieces.append(base_columns[c, 8 * b : 8 * b + 8, :] - taken)
        columns.append(jnp.concatenate(pieces, axis=0))
    result = strain_and_force(
        columns,
        strain,
        wide_gradient,
        wide_force,
        inverse_jacobian,
        lame_moduli,
        point_weights,
        faces,
        bool(rest),
    )
    if rest:
        keep_forces(result, *rest)


def order_kernel(rank, strains, last, out, store):
    for t in range(STEPS):
        for c in range(STRAIN):
            row = (c * STEPS + t) * POINTS
            rows = slice(c * POINTS, (c + 1) * POINTS)
            store[row : row + POINTS, :] = strains[t, rows, :] if t < STEPS - 1 else last[rows, :]
    lane = lax.broadcasted_iota(jnp.int32, (LANES, ORDER_WIDTH), 1)
    groups = rank.shape[0] * LANES // ORDER_WIDTH
    values, chosen = [], []
    for q in range(POINTS):
        block = store[pl.ds(q, STEPS * STRAIN, stride=POINTS), :]
        row = rank[q : q + 1, :]
        group = row // ORDER_WIDTH
        masked = [jnp.where(group == k, block, 0.0) for k in range(groups)]
        values.append(jnp.concatenate(masked, axis=0).astype(jnp.bfloat16))
        column = jnp.broadcast_to(row % ORDER_WIDTH, (LANES, LANES)).T
        wide = jnp.concatenate([column] * (ORDER_WIDTH // LANES), axis=1)
        chosen.append(jnp.where(wide == lane, 1.0, 0.0).astype(jnp.bfloat16))
    total = matmul(jnp.concatenate(values, axis=1), jnp.concatenate(chosen, axis=0))
    height = STEPS * STRAIN
    for w in range(rank.shape[0]):
        k, i = w * LANES // ORDER_WIDTH, w % (ORDER_WIDTH // LANES)
        block = total[k * height : (k + 1) * height, i * LANES : (i + 1) * LANES]
        out[w] = block.astype(jnp.bfloat16)


def place_kernel(pieces, out):
    for w in range(pieces.shape[0]):
        held = snake("dom", w)
        for c in range(STRAIN):
            out[c, :, w * LANES : (w + 1) * LANES] = pieces[held, c * STEPS : (c + 1) * STEPS, :]


def shards(
    connect,
    interface_nodes,
    neighbours,
    point_rank,
    shape_grad,
    inverse_jacobian,
    lame_moduli,
    point_weights,
    mass_elem,
    source_pattern,
    wavelet,
):
    nodes = source_pattern.shape[1]
    f32 = jnp.float32
    field_t = jax.ShapeDtypeStruct((8, nodes), f32)
    lanes_t = jax.ShapeDtypeStruct((8, LANES), f32)
    index_t = jax.ShapeDtypeStruct((8, LANES), jnp.int32)
    strain_t = jax.ShapeDtypeStruct((STRAIN * POINTS, LANES), f32)

    face = lax.broadcasted_iota(jnp.int32, (8, LANES), 1) // (LANES // FACES)
    dom = lax.axis_index("dom")
    parity = jnp.where(face < 2, lax.axis_index("grp") % 2, (dom // DOM_ROW + dom) % 2)
    source = 2 * (face // 2) + jnp.bitwise_xor(parity, 1 - face % 2)

    def exchange(send):
        received = []
        for name in EXCHANGES:
            axis, offset = name[:3], int(name[3])
            count = lax.axis_size(axis)
            pairs = []
            for i in range(offset, count - 1, 2):
                first, second = snake(axis, i), snake(axis, i + 1)
                pairs += [(first, second), (second, first)]
            received.append(lax.ppermute(send, axis, pairs))
        return received

    i32, bf16 = jnp.int32, jnp.bfloat16
    rank_rows = point_rank.reshape(POINTS, LANES)
    arguments = (
        wavelet,
        neighbours,
        connect,
        interface_nodes,
        mass_elem,
        source_pattern,
        shape_grad.T,
        inverse_jacobian,
        lame_moduli,
        point_weights,
        rank_rows,
    )
    buffers = [pltpu.SMEM(x.shape, x.dtype) for x in arguments[:2]]
    buffers += [pltpu.VMEM(x.shape, x.dtype) for x in arguments[2:6] + arguments[7:]]
    packed, shape_t, wave, send = kernel_call(
        pack_kernel,
        [
            jax.ShapeDtypeStruct((PACKED_ROWS, LANES), f32),
            jax.ShapeDtypeStruct(shape_grad.T.shape, f32),
            jax.ShapeDtypeStruct((STEPS, LANES), f32),
            lanes_t,
        ],
        [HBM] * len(arguments),
        scratch=buffers
        + [
            pltpu.SemaphoreType.DMA((len(arguments),)),
            pltpu.VMEM((EL_NODES * LANES, LANES), bf16),
            pltpu.VMEM(field_t.shape, f32),
        ],
    )(*(pltpu.with_memory_space_constraint(x, pltpu.MemorySpace.HBM) for x in arguments))
    writers = lax.axis_size("dom")
    packed = lax.ppermute(packed, "dom", [(i, snake("dom", i)) for i in range(writers)])
    received = []
    for name in EXCHANGES:
        axis, offset = name[:3], int(name[3])
        pairs = []
        for g in range(lax.axis_size("grp")):
            for w in range(writers):
                index, count = (g, lax.axis_size("grp")) if axis == "grp" else (w, writers)
                other = index + 1 if index % 2 == offset else index - 1
                if 0 <= other < count:
                    to_g, to_w = (other, w) if axis == "grp" else (g, other)
                    target = to_g * writers + snake("dom", to_w)
                    pairs.append((g * writers + w, target))
        received.append(lax.ppermute(send, ("grp", "dom"), pairs))

    prepare = kernel_call(
        prepare_kernel,
        [
            jax.ShapeDtypeStruct((EL_NODES * LANES, LANES), bf16),
            field_t,
            jax.ShapeDtypeStruct((EL_NODES * LANES, LANES), bf16),
            jax.ShapeDtypeStruct((8, nodes), i32),
            jax.ShapeDtypeStruct((NODE_ROWS, LANES), i32),
            jax.ShapeDtypeStruct((EL_NODES, 3 * POINTS, LANES), f32),
            jax.ShapeDtypeStruct((3 * POINTS, NODE_ROWS, LANES), f32),
            jax.ShapeDtypeStruct(inverse_jacobian.shape, f32),
            jax.ShapeDtypeStruct(lame_moduli.shape, f32),
            jax.ShapeDtypeStruct(point_weights.shape, f32),
            jax.ShapeDtypeStruct(rank_rows.shape, i32),
            jax.ShapeDtypeStruct((NODE_ROWS, LANES), i32),
            index_t,
        ],
        [VMEM] * 3,
    )
    outs = prepare(packed, shape_t, source)
    incidence, field, faces, inverse_index = outs[:4]
    rank = outs[10]
    connect_rows = outs[4]
    late_index, listed_index = outs[11:]
    element_data = (*outs[5:10], faces)
    wave_t = jax.ShapeDtypeStruct((STEPS, LANES), f32)
    forces_t = jax.ShapeDtypeStruct((3, NODE_ROWS, LANES), f32)
    (
        strain,
        displace,
        velocity,
        pattern,
        half_inverse_mass,
        late_scale,
        node_forces,
        send,
        wave,
    ) = kernel_call(
        first_kernel,
        [strain_t, field_t, field_t, field_t, field_t, lanes_t, forces_t, lanes_t, wave_t],
        [VMEM] * 16,
    )(wave, *received, source, inverse_index, listed_index, field, connect_rows, *element_data)
    strains = jnp.zeros((STEPS - 1, STRAIN * POINTS, LANES), f32)
    strains = lax.dynamic_update_index_in_dim(strains, strain, 0, 0)

    def advance(last, displace, velocity, late, node_forces, send, wave):
        dom1, grp1, *new_late = exchange(send)
        side = kernel_call(side_kernel, [field_t, field_t, forces_t, wave_t], [VMEM] * 14)
        displace, velocity, columns, wave = side(
            wave,
            dom1,
            grp1,
            *late,
            source,
            inverse_index,
            connect_rows,
            incidence,
            pattern,
            half_inverse_mass,
            displace,
            velocity,
            node_forces,
        )
        outs = kernel_call(
            step_kernel, [strain_t] + ([] if last else [forces_t, lanes_t]), [VMEM] * 12
        )(*new_late, source, late_index, late_scale, columns, *element_data)
        return outs[0], displace, velocity, new_late, *outs[1:], wave

    def body(step, carried):
        strains, *state = carried
        strain, *state = advance(False, *state)
        return (lax.dynamic_update_index_in_dim(strains, strain, step, 0), *state)

    none = [jnp.zeros((8, LANES), f32)] * 2
    carried = (strains, displace, velocity, none, node_forces, send, wave)
    strains, *state = lax.fori_loop(1, STEPS - 1, body, carried)
    strain = advance(True, *state)[0]
    (ordered,) = kernel_call(
        order_kernel,
        [jax.ShapeDtypeStruct((writers, STEPS * STRAIN, LANES), jnp.bfloat16)],
        [VMEM] * 3,
        scratch=[pltpu.VMEM((STEPS * STRAIN * POINTS, LANES), f32)],
    )(rank, strains, strain)
    pieces = lax.all_to_all(ordered, "dom", split_axis=0, concat_axis=0, tiled=True)
    (placed,) = kernel_call(
        place_kernel, [jax.ShapeDtypeStruct((STRAIN, STEPS, writers * LANES), jnp.bfloat16)], [VMEM]
    )(pieces)
    return placed.transpose(1, 0, 2)


def solution(mesh):
    placed = (
        P(None, ("grp", "dom")),
        P(("grp", "dom"), None, None),
        P(("grp", "dom"), None),
        P(("grp", "dom"), None),
        P(),
        P(None, ("grp", "dom")),
        P(None, ("grp", "dom")),
        P(None, ("grp", "dom")),
        P(None, ("grp", "dom")),
        P(None, ("grp", "dom")),
        P(),
    )
    return jax.shard_map(
        shards, mesh=mesh, in_specs=placed, out_specs=P(None, None, ("grp", "dom")), check_vma=False
    )
```

```python
import jax
import jax.numpy as jnp
from jax import lax
from jax.experimental import pallas as pl
from jax.experimental.pallas import tpu as pltpu
from jax.sharding import PartitionSpec as P


EL_NODES = 20
NODE_ROWS = 24
POINTS = 16
STRAIN = 6
STEPS = 16
LANES = 128
FACES = 4
ORDER_WIDTH = 256

time_step = 0.5

DOM_ROW = 4

EXCHANGES = ("dom1", "grp1", "dom0", "grp0")

VMEM = pl.BlockSpec(memory_space=pltpu.VMEM)
HBM = pl.BlockSpec(memory_space=pltpu.MemorySpace.HBM)


def snake(axis, index):
    row, column = index // DOM_ROW, index % DOM_ROW
    return index if axis == "grp" or row % 2 == 0 else row * DOM_ROW + DOM_ROW - 1 - column


def kernel_call(body, outs, specs, scratch=()):
    return pl.pallas_call(
        body,
        out_shape=outs,
        in_specs=specs,
        out_specs=[VMEM] * len(outs),
        scratch_shapes=list(scratch),
        compiler_params=pltpu.CompilerParams(vmem_limit_bytes=24 * 1024 * 1024),
    )


def parts_of(x):
    high = x.astype(jnp.bfloat16).astype(jnp.float32)
    rest = x - high
    middle = rest.astype(jnp.bfloat16).astype(jnp.float32)
    low = (rest - middle).astype(jnp.bfloat16).astype(jnp.float32)
    return high, middle, low


def matmul(left, right):
    return jnp.dot(left, right, preferred_element_type=jnp.float32)


def lane_gather(row, index):
    return jnp.take_along_axis(row, index, axis=1, mode="promise_in_bounds")


def pick_lanes(field, index):
    low = jnp.bitwise_and(index, LANES - 1)
    chunk = jnp.right_shift(index, 7)
    out = lane_gather(field[:, 0:LANES], low)
    for j in range(1, field.shape[1] // LANES):
        out = jnp.where(
            chunk == j, lane_gather(field[:, j * LANES : (j + 1) * LANES], low), out
        )
    return out


def spread(received, inverse):
    out = []
    for j in range(inverse.shape[1] // LANES):
        index = inverse[:, j * LANES : (j + 1) * LANES]
        taken = lane_gather(received, jnp.maximum(index, 0))
        out.append(jnp.where(index >= 0, taken, 0.0))
    return jnp.concatenate(out, axis=1)


def early_received(source, dom1, grp1):
    return jnp.where(source == 3, dom1, jnp.where(source == 1, grp1, 0.0))


def late_received(source, dom0, grp0):
    return jnp.where(source == 2, dom0, jnp.where(source == 0, grp0, 0.0))


def scatter_nodes(pieces, chunks, incidence):
    group = lax.broadcasted_iota(jnp.int32, (8, LANES), 0) // 4
    parts = [[], [], []]
    for piece, chunk in zip(pieces, chunks):
        both = [jnp.where(chunk == group + base, piece, 0.0) for base in (0, 2)]
        for i, part in enumerate(parts_of(jnp.concatenate(both, axis=0))):
            parts[i].append(part.astype(jnp.bfloat16))
    left = jnp.concatenate([jnp.concatenate(p, axis=1) for p in parts], axis=0)
    sums = matmul(left, incidence)
    total = (sums[32:48] + sums[16:32]) + sums[0:16]
    fields = []
    for base in (0, 8):
        rows = total[base : base + 8]
        fields += [rows, pltpu.roll(rows, 4, 0)]
    return jnp.concatenate(fields, axis=1)


CONNECT_ROW = 0
MASS_ROW = 24
LAME_ROW = 44
LISTED_ROW = 46
SWAPPED_ROW = 47
JACOBIAN_ROW = 48
WEIGHTS_ROW = 64
SOURCE_ROW = 80
RANK_ROW = 96
PACKED_ROWS = 112


def set_incidence(packed, incidence):
    element_nodes = packed[CONNECT_ROW : CONNECT_ROW + NODE_ROWS, :].astype(jnp.int32)
    low = jnp.bitwise_and(element_nodes, LANES - 1)
    own_lane = lax.broadcasted_iota(jnp.int32, (LANES, LANES), 1)
    for n in range(EL_NODES):
        column = jnp.broadcast_to(low[n : n + 1, :], (LANES, LANES)).T
        incidence[n * LANES : (n + 1) * LANES, :] = jnp.where(
            column == own_lane, 1.0, 0.0
        ).astype(jnp.bfloat16)


def set_faces(packed, faces):
    element_nodes = packed[CONNECT_ROW : CONNECT_ROW + NODE_ROWS, :].astype(jnp.int32)
    sent = packed[SWAPPED_ROW : SWAPPED_ROW + 1, :].astype(jnp.int32)
    for n in range(EL_NODES):
        column = jnp.broadcast_to(element_nodes[n : n + 1, :], (LANES, LANES)).T
        faces[n * LANES : (n + 1) * LANES, :] = jnp.where(column == sent, 1.0, 0.0).astype(
            jnp.bfloat16
        )


def set_field(packed, incidence, field):
    element_nodes = packed[CONNECT_ROW : CONNECT_ROW + NODE_ROWS, :].astype(jnp.int32)
    chunk = jnp.right_shift(element_nodes, 7)
    masses = [
        jnp.broadcast_to(packed[MASS_ROW + n : MASS_ROW + n + 1, :], (8, LANES))
        for n in range(EL_NODES)
    ]
    chunks = [chunk[n : n + 1, :] for n in range(EL_NODES)]
    field[...] = scatter_nodes(masses, chunks, incidence[...])
    for j in range(field.shape[1] // LANES):
        row = SOURCE_ROW + 3 * j
        field[0:3, j * LANES : (j + 1) * LANES] = packed[row : row + 3, :]


def pack_kernel(
    wavelet_in,
    neighbours_in,
    connect_in,
    lists_in,
    mass_in,
    source_in,
    shape_in,
    jacobian_in,
    lame_in,
    weights_in,
    rank_in,
    packed,
    shape_t,
    wave,
    send,
    wavelet,
    neighbours,
    connect,
    lists,
    mass_elem,
    source_pattern,
    jacobian,
    lame,
    weights,
    rank,
    sems,
    incidence,
    field,
):
    moves = [
        (wavelet_in, wavelet),
        (neighbours_in, neighbours),
        (connect_in, connect),
        (lists_in, lists),
        (mass_in, mass_elem),
        (source_in, source_pattern),
        (shape_in, shape_t),
        (jacobian_in, jacobian),
        (lame_in, lame),
        (weights_in, weights),
        (rank_in, rank),
    ]
    copies = [pltpu.make_async_copy(a, b, sems.at[i]) for i, (a, b) in enumerate(moves)]
    for copy in copies:
        copy.start()
    packed[...] = jnp.zeros(packed.shape, jnp.float32)
    for copy in copies:
        copy.wait()
    wave[...] = jnp.concatenate(
        [jnp.full((1, LANES), wavelet[t], jnp.float32) for t in range(STEPS)], axis=0
    )
    packed[CONNECT_ROW : CONNECT_ROW + EL_NODES, :] = connect[...].astype(jnp.float32)
    packed[MASS_ROW : MASS_ROW + EL_NODES, :] = mass_elem[...]
    packed[LAME_ROW : LAME_ROW + 2, :] = lame[...]
    packed[JACOBIAN_ROW : JACOBIAN_ROW + 9, :] = jacobian[...]
    packed[WEIGHTS_ROW : WEIGHTS_ROW + POINTS, :] = weights[...]
    packed[RANK_ROW : RANK_ROW + POINTS, :] = rank[...].astype(jnp.float32)
    for j in range(source_pattern.shape[1] // LANES):
        row = SOURCE_ROW + 3 * j
        packed[row : row + 3, :] = source_pattern[:, j * LANES : (j + 1) * LANES]
    face = [lists[0, k : k + 1, :] for k in range(FACES)]
    listed = jnp.concatenate(face, axis=1)
    swapped = jnp.concatenate([face[1], face[0], face[3], face[2]], axis=1)
    side = lax.broadcasted_iota(jnp.int32, (1, LANES), 1) // (LANES // FACES)
    open_side = jnp.where(
        side < 2,
        jnp.where(side == 0, neighbours[0, 0], neighbours[0, 1]),
        jnp.where(side == 2, neighbours[0, 2], neighbours[0, 3]),
    )
    listed = jnp.where(open_side != 0, listed, -1)
    packed[LISTED_ROW : LISTED_ROW + 1, :] = listed.astype(jnp.float32)
    packed[SWAPPED_ROW : SWAPPED_ROW + 1, :] = swapped.astype(jnp.float32)
    set_incidence(packed, incidence)
    set_field(packed, incidence, field)
    send[...] = pick_lanes(field[...], jnp.broadcast_to(swapped, (8, LANES)))


def prepare_kernel(
    packed,
    shape_t,
    source,
    incidence,
    field,
    faces,
    inverse_index,
    connect,
    wide_gradient,
    wide_force,
    inverse_jacobian,
    lame_moduli,
    point_weights,
    rank,
    late_index,
    listed_index,
):
    nodes = field.shape[1]
    element_nodes = packed[CONNECT_ROW : CONNECT_ROW + NODE_ROWS, :].astype(jnp.int32)
    connect[...] = element_nodes
    inverse_jacobian[...] = packed[JACOBIAN_ROW : JACOBIAN_ROW + 9, :]
    lame_moduli[...] = packed[LAME_ROW : LAME_ROW + 2, :]
    point_weights[...] = packed[WEIGHTS_ROW : WEIGHTS_ROW + POINTS, :]
    rank[...] = packed[RANK_ROW : RANK_ROW + POINTS, :].astype(jnp.int32)
    set_incidence(packed, incidence)
    lane = lax.broadcasted_iota(jnp.int32, (LANES, nodes), 1)
    listed = packed[LISTED_ROW : LISTED_ROW + 1, :].astype(jnp.int32)
    column = jnp.broadcast_to(listed, (LANES, LANES)).T
    wide = jnp.concatenate([column] * (nodes // LANES), axis=1)
    late = jnp.broadcast_to(256 * (1 - source[0:1, :] % 2), (LANES, LANES)).T
    late = jnp.concatenate([late] * (nodes // LANES), axis=1)
    slot = lax.broadcasted_iota(jnp.int32, (LANES, nodes), 0) + 1 + late
    found = jnp.sum(jnp.where(wide == lane, slot, 0), axis=0, keepdims=True)
    placed = jnp.bitwise_and(found, 255) - 1
    inverse_index[...] = jnp.broadcast_to(placed, (8, nodes))
    late_row = jnp.where(found >= 256, placed, -1).astype(jnp.float32)
    late_row = jnp.broadcast_to(late_row, (8, nodes))
    for b in range(NODE_ROWS // 8):
        rows = slice(8 * b, 8 * b + 8)
        late_index[rows, :] = pick_lanes(late_row, element_nodes[rows]).astype(jnp.int32)
    listed_index[...] = jnp.broadcast_to(jnp.maximum(listed, 0), (8, LANES))
    set_faces(packed, faces)
    set_field(packed, incidence, field)

    reference_rows = 3 * POINTS
    shape_rows = jnp.concatenate(
        [shape_t[...], jnp.zeros((EL_NODES, LANES - reference_rows), jnp.float32)], axis=1
    )
    shape_rows = jnp.concatenate(
        [shape_rows, jnp.zeros((LANES - EL_NODES, LANES), jnp.float32)], axis=0
    )
    shape_columns = shape_rows.T
    for n in range(EL_NODES):
        wide_gradient[n] = jnp.broadcast_to(
            shape_columns[0:reference_rows, n : n + 1], (reference_rows, LANES)
        )
    for m in range(reference_rows):
        wide_force[m] = jnp.broadcast_to(shape_rows[0:NODE_ROWS, m : m + 1], (NODE_ROWS, LANES))


def contract(table, columns, count):
    sums = [[None, None] for _ in columns]
    for i in range(count):
        weights = table[i]
        for c, column in enumerate(columns):
            term = weights * column[i : i + 1, :]
            old = sums[c][i % 2]
            sums[c][i % 2] = term if old is None else old + term
    return [even + odd for even, odd in sums]


def wave_row(wave, width):
    return jnp.concatenate([wave[0:1, :]] * (width // LANES), axis=1)


def moved_up(wave):
    return pltpu.roll(wave[...], STEPS - 1, 0)


def at_elements(displace, connect):
    index = connect[...]
    columns = []
    for c in range(3):
        pieces = []
        for b in range(NODE_ROWS // 8):
            row = jnp.broadcast_to(displace[c : c + 1, :], (8, displace.shape[1]))
            pieces.append(pick_lanes(row, index[8 * b : 8 * b + 8]))
        columns.append(jnp.concatenate(pieces, axis=0))
    return columns


def strain_and_force(
    columns,
    strain,
    wide_gradient,
    wide_force,
    inverse_jacobian,
    lame_moduli,
    point_weights,
    faces,
    need_force,
):
    along = contract(wide_gradient, columns, EL_NODES)
    jac = [inverse_jacobian[i : i + 1, :] for i in range(9)]

    def ref_derivative(c, r):
        return along[c][r * POINTS : (r + 1) * POINTS, :]

    grad = [
        [
            (ref_derivative(c, 0) * jac[d] + ref_derivative(c, 1) * jac[3 + d])
            + ref_derivative(c, 2) * jac[6 + d]
            for d in range(3)
        ]
        for c in range(3)
    ]
    shear = {(c, d): grad[c][d] + grad[d][c] for c, d in ((1, 2), (0, 2), (0, 1))}
    rows = [grad[0][0], grad[1][1], grad[2][2]] + [0.5 * shear[k] for k in ((1, 2), (0, 2), (0, 1))]
    for s in range(STRAIN):
        strain[s * POINTS : (s + 1) * POINTS, :] = rows[s]
    if not need_force:
        return None
    volume = (grad[0][0] + grad[1][1]) + grad[2][2]
    weights = point_weights[...]
    shear_scale = lame_moduli[1:2, :] * weights
    pressure = (lame_moduli[0:1, :] * weights) * volume
    stress = [[None] * 3 for _ in range(3)]
    for c in range(3):
        for d in range(3):
            if c == d:
                stress[c][d] = shear_scale * (grad[c][c] + grad[c][c]) + pressure
            else:
                stress[c][d] = shear_scale * shear[(min(c, d), max(c, d))]
    columns = []
    for c in range(3):
        mapped = [
            (stress[c][0] * jac[3 * r] + stress[c][1] * jac[3 * r + 1])
            + stress[c][2] * jac[3 * r + 2]
            for r in range(3)
        ]
        columns.append(jnp.concatenate(mapped, axis=0))
    node_forces = contract(wide_force, columns, 3 * POINTS)
    parts = parts_of(jnp.concatenate(node_rows(node_forces), axis=1))
    sums = matmul(jnp.concatenate(parts, axis=0).astype(jnp.bfloat16), faces[...])
    return node_forces, (sums[16:24] + sums[8:16]) + sums[0:8]


def node_rows(node_forces):
    row_id = lax.broadcasted_iota(jnp.int32, (8, LANES), 0) % 4
    pieces = []
    for n in range(EL_NODES):
        first, second, third = (
            jnp.broadcast_to(node_forces[c][n : n + 1, :], (8, LANES)) for c in range(3)
        )
        pieces.append(jnp.where(row_id == 0, first, jnp.where(row_id == 1, second, third)))
    return pieces


def keep_forces(result, node_forces, send):
    forces, faces = result
    for c in range(3):
        node_forces[c] = forces[c]
    send[...] = faces


def first_kernel(
    wave,
    dom1,
    grp1,
    dom0,
    grp0,
    source,
    inverse_index,
    listed_index,
    field,
    connect,
    wide_gradient,
    wide_force,
    inverse_jacobian,
    lame_moduli,
    point_weights,
    faces,
    strain,
    displace,
    velocity,
    pattern,
    half_inverse_mass,
    late_scale,
    node_forces,
    send,
    next_wave,
):
    next_wave[...] = moved_up(wave)
    received = early_received(source[...], dom1[...], grp1[...])
    received = received + late_received(source[...], dom0[...], grp0[...])
    total = field[...] + spread(received, inverse_index[...])
    scale = jnp.broadcast_to(time_step * (1.0 / total[3:4, :]), total.shape)
    pattern[...] = total
    half_inverse_mass[...] = scale
    late_scale[...] = time_step * pick_lanes(scale, listed_index[...])
    new_velocity = scale * (wave_row(wave, total.shape[1]) * total)
    velocity[...] = new_velocity
    new_displace = time_step * new_velocity
    displace[...] = new_displace
    result = strain_and_force(
        at_elements(new_displace, connect),
        strain,
        wide_gradient,
        wide_force,
        inverse_jacobian,
        lame_moduli,
        point_weights,
        faces,
        True,
    )
    keep_forces(result, node_forces, send)


def side_kernel(
    wave,
    dom1,
    grp1,
    last_dom0,
    last_grp0,
    source,
    inverse_index,
    connect,
    incidence,
    pattern,
    half_inverse_mass,
    old_displace,
    old_velocity,
    node_forces,
    displace,
    velocity,
    columns,
    next_wave,
):
    next_wave[...] = moved_up(wave)
    index, scale = inverse_index[...], half_inverse_mass[...]
    missing = spread(late_received(source[...], last_dom0[...], last_grp0[...]), index) * scale
    parts = [node_forces[c] for c in range(3)]
    chunk = jnp.right_shift(connect[...], 7)
    chunks = [chunk[n : n + 1, :] for n in range(EL_NODES)]
    force = scatter_nodes(node_rows(parts), chunks, incidence[...])
    stiff = force + spread(early_received(source[...], dom1[...], grp1[...]), index)
    total = wave_row(wave, stiff.shape[1]) * pattern[...] - stiff
    new_velocity = (old_velocity[...] - missing) + scale * total
    velocity[...] = new_velocity
    new_displace = (old_displace[...] - time_step * missing) + time_step * new_velocity
    displace[...] = new_displace
    for c, column in enumerate(at_elements(new_displace, connect)):
        columns[c] = column


def step_kernel(
    dom0,
    grp0,
    source,
    late_index,
    late_scale,
    base_columns,
    wide_gradient,
    wide_force,
    inverse_jacobian,
    lame_moduli,
    point_weights,
    faces,
    strain,
    *rest,
):
    late = late_scale[...] * late_received(source[...], dom0[...], grp0[...])
    columns = []
    for c in range(3):
        row = jnp.broadcast_to(late[c : c + 1, :], (8, LANES))
        pieces = []
        for b in range(NODE_ROWS // 8):
            index = late_index[8 * b : 8 * b + 8, :]
            taken = jnp.where(index >= 0, lane_gather(row, jnp.maximum(index, 0)), 0.0)
            pieces.append(base_columns[c, 8 * b : 8 * b + 8, :] - taken)
        columns.append(jnp.concatenate(pieces, axis=0))
    result = strain_and_force(
        columns,
        strain,
        wide_gradient,
        wide_force,
        inverse_jacobian,
        lame_moduli,
        point_weights,
        faces,
        bool(rest),
    )
    if rest:
        keep_forces(result, *rest)


def order_kernel(rank, strains, before_last, last, out, store):
    for t in range(STEPS):
        for c in range(STRAIN):
            row = (c * STEPS + t) * POINTS
            rows = slice(c * POINTS, (c + 1) * POINTS)
            if t < STEPS - 2:
                store[row : row + POINTS, :] = strains[t, rows, :]
            else:
                end = before_last if t == STEPS - 2 else last
                store[row : row + POINTS, :] = end[rows, :]
    lane = lax.broadcasted_iota(jnp.int32, (LANES, ORDER_WIDTH), 1)
    groups = rank.shape[0] * LANES // ORDER_WIDTH
    values, chosen = [], []
    for q in range(POINTS):
        block = store[pl.ds(q, STEPS * STRAIN, stride=POINTS), :]
        row = rank[q : q + 1, :]
        group = row // ORDER_WIDTH
        masked = [jnp.where(group == k, block, 0.0) for k in range(groups)]
        values.append(jnp.concatenate(masked, axis=0).astype(jnp.bfloat16))
        column = jnp.broadcast_to(row % ORDER_WIDTH, (LANES, LANES)).T
        wide = jnp.concatenate([column] * (ORDER_WIDTH // LANES), axis=1)
        chosen.append(jnp.where(wide == lane, 1.0, 0.0).astype(jnp.bfloat16))
    total = matmul(jnp.concatenate(values, axis=1), jnp.concatenate(chosen, axis=0))
    height = STEPS * STRAIN
    for w in range(rank.shape[0]):
        k, i = w * LANES // ORDER_WIDTH, w % (ORDER_WIDTH // LANES)
        block = total[k * height : (k + 1) * height, i * LANES : (i + 1) * LANES]
        out[w] = block.astype(jnp.bfloat16)


def place_kernel(pieces, out):
    for w in range(pieces.shape[0]):
        held = snake("dom", w)
        for c in range(STRAIN):
            out[c, :, w * LANES : (w + 1) * LANES] = pieces[held, c * STEPS : (c + 1) * STEPS, :]


def shards(
    connect,
    interface_nodes,
    neighbours,
    point_rank,
    shape_grad,
    inverse_jacobian,
    lame_moduli,
    point_weights,
    mass_elem,
    source_pattern,
    wavelet,
):
    nodes = source_pattern.shape[1]
    f32 = jnp.float32
    field_t = jax.ShapeDtypeStruct((8, nodes), f32)
    lanes_t = jax.ShapeDtypeStruct((8, LANES), f32)
    index_t = jax.ShapeDtypeStruct((8, LANES), jnp.int32)
    strain_t = jax.ShapeDtypeStruct((STRAIN * POINTS, LANES), f32)

    face = lax.broadcasted_iota(jnp.int32, (8, LANES), 1) // (LANES // FACES)
    dom = lax.axis_index("dom")
    parity = jnp.where(face < 2, lax.axis_index("grp") % 2, (dom // DOM_ROW + dom) % 2)
    source = 2 * (face // 2) + jnp.bitwise_xor(parity, 1 - face % 2)

    def exchange(send):
        received = []
        for name in EXCHANGES:
            axis, offset = name[:3], int(name[3])
            count = lax.axis_size(axis)
            pairs = []
            for i in range(offset, count - 1, 2):
                first, second = snake(axis, i), snake(axis, i + 1)
                pairs += [(first, second), (second, first)]
            received.append(lax.ppermute(send, axis, pairs))
        return received

    i32, bf16 = jnp.int32, jnp.bfloat16
    rank_rows = point_rank.reshape(POINTS, LANES)
    arguments = (
        wavelet,
        neighbours,
        connect,
        interface_nodes,
        mass_elem,
        source_pattern,
        shape_grad.T,
        inverse_jacobian,
        lame_moduli,
        point_weights,
        rank_rows,
    )
    buffers = [pltpu.SMEM(x.shape, x.dtype) for x in arguments[:2]]
    buffers += [pltpu.VMEM(x.shape, x.dtype) for x in arguments[2:6] + arguments[7:]]
    packed, shape_t, wave, send = kernel_call(
        pack_kernel,
        [
            jax.ShapeDtypeStruct((PACKED_ROWS, LANES), f32),
            jax.ShapeDtypeStruct(shape_grad.T.shape, f32),
            jax.ShapeDtypeStruct((STEPS, LANES), f32),
            lanes_t,
        ],
        [HBM] * len(arguments),
        scratch=buffers
        + [
            pltpu.SemaphoreType.DMA((len(arguments),)),
            pltpu.VMEM((EL_NODES * LANES, LANES), bf16),
            pltpu.VMEM(field_t.shape, f32),
        ],
    )(*(pltpu.with_memory_space_constraint(x, pltpu.MemorySpace.HBM) for x in arguments))
    writers = lax.axis_size("dom")
    packed = lax.ppermute(packed, "dom", [(i, snake("dom", i)) for i in range(writers)])
    received = []
    for name in EXCHANGES:
        axis, offset = name[:3], int(name[3])
        pairs = []
        for g in range(lax.axis_size("grp")):
            for w in range(writers):
                index, count = (g, lax.axis_size("grp")) if axis == "grp" else (w, writers)
                other = index + 1 if index % 2 == offset else index - 1
                if 0 <= other < count:
                    to_g, to_w = (other, w) if axis == "grp" else (g, other)
                    target = to_g * writers + snake("dom", to_w)
                    pairs.append((g * writers + w, target))
        received.append(lax.ppermute(send, ("grp", "dom"), pairs))

    prepare = kernel_call(
        prepare_kernel,
        [
            jax.ShapeDtypeStruct((EL_NODES * LANES, LANES), bf16),
            field_t,
            jax.ShapeDtypeStruct((EL_NODES * LANES, LANES), bf16),
            jax.ShapeDtypeStruct((8, nodes), i32),
            jax.ShapeDtypeStruct((NODE_ROWS, LANES), i32),
            jax.ShapeDtypeStruct((EL_NODES, 3 * POINTS, LANES), f32),
            jax.ShapeDtypeStruct((3 * POINTS, NODE_ROWS, LANES), f32),
            jax.ShapeDtypeStruct(inverse_jacobian.shape, f32),
            jax.ShapeDtypeStruct(lame_moduli.shape, f32),
            jax.ShapeDtypeStruct(point_weights.shape, f32),
            jax.ShapeDtypeStruct(rank_rows.shape, i32),
            jax.ShapeDtypeStruct((NODE_ROWS, LANES), i32),
            index_t,
        ],
        [VMEM] * 3,
    )
    outs = prepare(packed, shape_t, source)
    incidence, field, faces, inverse_index = outs[:4]
    rank = outs[10]
    connect_rows = outs[4]
    late_index, listed_index = outs[11:]
    element_data = (*outs[5:10], faces)
    wave_t = jax.ShapeDtypeStruct((STEPS, LANES), f32)
    forces_t = jax.ShapeDtypeStruct((3, NODE_ROWS, LANES), f32)
    (
        strain,
        displace,
        velocity,
        pattern,
        half_inverse_mass,
        late_scale,
        node_forces,
        send,
        wave,
    ) = kernel_call(
        first_kernel,
        [strain_t, field_t, field_t, field_t, field_t, lanes_t, forces_t, lanes_t, wave_t],
        [VMEM] * 16,
    )(wave, *received, source, inverse_index, listed_index, field, connect_rows, *element_data)
    strains = jnp.zeros((STEPS - 2, STRAIN * POINTS, LANES), f32)

    def advance(last, displace, velocity, late, node_forces, send, wave):
        dom1, grp1, *new_late = exchange(send)
        side = kernel_call(side_kernel, [field_t, field_t, forces_t, wave_t], [VMEM] * 14)
        displace, velocity, columns, wave = side(
            wave,
            dom1,
            grp1,
            *late,
            source,
            inverse_index,
            connect_rows,
            incidence,
            pattern,
            half_inverse_mass,
            displace,
            velocity,
            node_forces,
        )
        outs = kernel_call(
            step_kernel, [strain_t] + ([] if last else [forces_t, lanes_t]), [VMEM] * 12
        )(*new_late, source, late_index, late_scale, columns, *element_data)
        return outs[0], displace, velocity, new_late, *outs[1:], wave

    def body(step, carried):
        strains, strain, *state = carried
        strains = lax.dynamic_update_index_in_dim(strains, strain, step - 1, 0)
        return (strains, *advance(False, *state))

    none = [jnp.zeros((8, LANES), f32)] * 2
    carried = (strains, strain, displace, velocity, none, node_forces, send, wave)
    strains, strain, *state = lax.fori_loop(1, STEPS - 1, body, carried)
    strain = (strain, advance(True, *state)[0])
    (ordered,) = kernel_call(
        order_kernel,
        [jax.ShapeDtypeStruct((writers, STEPS * STRAIN, LANES), jnp.bfloat16)],
        [VMEM] * 4,
        scratch=[pltpu.VMEM(((STEPS * STRAIN + 1) * POINTS, LANES), f32)],
    )(rank, strains, *strain)
    pieces = lax.all_to_all(ordered, "dom", split_axis=0, concat_axis=0, tiled=True)
    (placed,) = kernel_call(
        place_kernel, [jax.ShapeDtypeStruct((STRAIN, STEPS, writers * LANES), jnp.bfloat16)], [VMEM]
    )(pieces)
    return placed.transpose(1, 0, 2)


def solution(mesh):
    placed = (
        P(None, ("grp", "dom")),
        P(("grp", "dom"), None, None),
        P(("grp", "dom"), None),
        P(("grp", "dom"), None),
        P(),
        P(None, ("grp", "dom")),
        P(None, ("grp", "dom")),
        P(None, ("grp", "dom")),
        P(None, ("grp", "dom")),
        P(None, ("grp", "dom")),
        P(),
    )
    return jax.shard_map(
        shards, mesh=mesh, in_specs=placed, out_specs=P(None, None, ("grp", "dom")), check_vma=False
    )
```

```python
import jax
import jax.numpy as jnp
from jax import lax
from jax.experimental import pallas as pl
from jax.experimental.pallas import tpu as pltpu
from jax.sharding import PartitionSpec as P


EL_NODES = 20
NODE_ROWS = 24
POINTS = 16
STRAIN = 6
STEPS = 16
LANES = 128
FACES = 4
ORDER_WIDTH = 256

time_step = 0.5

DOM_ROW = 4

EXCHANGES = ("dom1", "grp1", "dom0", "grp0")

VMEM = pl.BlockSpec(memory_space=pltpu.VMEM)
HBM = pl.BlockSpec(memory_space=pltpu.MemorySpace.HBM)


def snake(axis, index):
    row, column = index // DOM_ROW, index % DOM_ROW
    return index if axis == "grp" or row % 2 == 0 else row * DOM_ROW + DOM_ROW - 1 - column


def kernel_call(body, outs, specs, scratch=()):
    return pl.pallas_call(
        body,
        out_shape=outs,
        in_specs=specs,
        out_specs=[VMEM] * len(outs),
        scratch_shapes=list(scratch),
        compiler_params=pltpu.CompilerParams(vmem_limit_bytes=24 * 1024 * 1024),
    )


def parts_of(x):
    high = x.astype(jnp.bfloat16).astype(jnp.float32)
    rest = x - high
    middle = rest.astype(jnp.bfloat16).astype(jnp.float32)
    low = (rest - middle).astype(jnp.bfloat16).astype(jnp.float32)
    return high, middle, low


def matmul(left, right):
    return jnp.dot(left, right, preferred_element_type=jnp.float32)


def lane_gather(row, index):
    return jnp.take_along_axis(row, index, axis=1, mode="promise_in_bounds")


def pick_lanes(field, index):
    low = jnp.bitwise_and(index, LANES - 1)
    chunk = jnp.right_shift(index, 7)
    out = lane_gather(field[:, 0:LANES], low)
    for j in range(1, field.shape[1] // LANES):
        out = jnp.where(
            chunk == j, lane_gather(field[:, j * LANES : (j + 1) * LANES], low), out
        )
    return out


def spread(received, inverse):
    out = []
    for j in range(inverse.shape[1] // LANES):
        index = inverse[:, j * LANES : (j + 1) * LANES]
        taken = lane_gather(received, jnp.maximum(index, 0))
        out.append(jnp.where(index >= 0, taken, 0.0))
    return jnp.concatenate(out, axis=1)


def early_received(source, dom1, grp1):
    return jnp.where(source == 3, dom1, jnp.where(source == 1, grp1, 0.0))


def late_received(source, dom0, grp0):
    return jnp.where(source == 2, dom0, jnp.where(source == 0, grp0, 0.0))


def scatter_nodes(pieces, chunks, incidence):
    group = lax.broadcasted_iota(jnp.int32, (8, LANES), 0) // 4
    parts = [[], [], []]
    for piece, chunk in zip(pieces, chunks):
        both = [jnp.where(chunk == group + base, piece, 0.0) for base in (0, 2)]
        for i, part in enumerate(parts_of(jnp.concatenate(both, axis=0))):
            parts[i].append(part.astype(jnp.bfloat16))
    left = jnp.concatenate([jnp.concatenate(p, axis=1) for p in parts], axis=0)
    sums = matmul(left, incidence)
    total = (sums[32:48] + sums[16:32]) + sums[0:16]
    fields = []
    for base in (0, 8):
        rows = total[base : base + 8]
        fields += [rows, pltpu.roll(rows, 4, 0)]
    return jnp.concatenate(fields, axis=1)


CONNECT_ROW = 0
MASS_ROW = 24
LAME_ROW = 44
LISTED_ROW = 46
SWAPPED_ROW = 47
JACOBIAN_ROW = 48
WEIGHTS_ROW = 64
SOURCE_ROW = 80
RANK_ROW = 96
PACKED_ROWS = 112


def set_incidence(packed, incidence):
    element_nodes = packed[CONNECT_ROW : CONNECT_ROW + NODE_ROWS, :].astype(jnp.int32)
    low = jnp.bitwise_and(element_nodes, LANES - 1)
    own_lane = lax.broadcasted_iota(jnp.int32, (LANES, LANES), 1)
    for n in range(EL_NODES):
        column = jnp.broadcast_to(low[n : n + 1, :], (LANES, LANES)).T
        incidence[n * LANES : (n + 1) * LANES, :] = jnp.where(
            column == own_lane, 1.0, 0.0
        ).astype(jnp.bfloat16)


def set_faces(packed, faces):
    element_nodes = packed[CONNECT_ROW : CONNECT_ROW + NODE_ROWS, :].astype(jnp.int32)
    sent = packed[SWAPPED_ROW : SWAPPED_ROW + 1, :].astype(jnp.int32)
    for n in range(EL_NODES):
        column = jnp.broadcast_to(element_nodes[n : n + 1, :], (LANES, LANES)).T
        faces[n * LANES : (n + 1) * LANES, :] = jnp.where(column == sent, 1.0, 0.0).astype(
            jnp.bfloat16
        )


def set_field(packed, incidence, field):
    element_nodes = packed[CONNECT_ROW : CONNECT_ROW + NODE_ROWS, :].astype(jnp.int32)
    chunk = jnp.right_shift(element_nodes, 7)
    masses = [
        jnp.broadcast_to(packed[MASS_ROW + n : MASS_ROW + n + 1, :], (8, LANES))
        for n in range(EL_NODES)
    ]
    chunks = [chunk[n : n + 1, :] for n in range(EL_NODES)]
    field[...] = scatter_nodes(masses, chunks, incidence[...])
    for j in range(field.shape[1] // LANES):
        row = SOURCE_ROW + 3 * j
        field[0:3, j * LANES : (j + 1) * LANES] = packed[row : row + 3, :]


def pack_kernel(
    wavelet_in,
    neighbours_in,
    connect_in,
    lists_in,
    mass_in,
    source_in,
    shape_in,
    jacobian_in,
    lame_in,
    weights_in,
    rank_in,
    packed,
    shape_t,
    wave,
    send,
    wavelet,
    neighbours,
    connect,
    lists,
    mass_elem,
    source_pattern,
    jacobian,
    lame,
    weights,
    rank,
    sems,
    incidence,
    field,
):
    moves = [
        (wavelet_in, wavelet),
        (neighbours_in, neighbours),
        (connect_in, connect),
        (lists_in, lists),
        (mass_in, mass_elem),
        (source_in, source_pattern),
        (shape_in, shape_t),
        (jacobian_in, jacobian),
        (lame_in, lame),
        (weights_in, weights),
        (rank_in, rank),
    ]
    copies = [pltpu.make_async_copy(a, b, sems.at[i]) for i, (a, b) in enumerate(moves)]
    for copy in copies:
        copy.start()
    packed[...] = jnp.zeros(packed.shape, jnp.float32)
    for copy in copies:
        copy.wait()
    wave[...] = jnp.concatenate(
        [jnp.full((1, LANES), wavelet[t], jnp.float32) for t in range(STEPS)], axis=0
    )
    packed[CONNECT_ROW : CONNECT_ROW + EL_NODES, :] = connect[...].astype(jnp.float32)
    packed[MASS_ROW : MASS_ROW + EL_NODES, :] = mass_elem[...]
    packed[LAME_ROW : LAME_ROW + 2, :] = lame[...]
    packed[JACOBIAN_ROW : JACOBIAN_ROW + 9, :] = jacobian[...]
    packed[WEIGHTS_ROW : WEIGHTS_ROW + POINTS, :] = weights[...]
    packed[RANK_ROW : RANK_ROW + POINTS, :] = rank[...].astype(jnp.float32)
    for j in range(source_pattern.shape[1] // LANES):
        row = SOURCE_ROW + 3 * j
        packed[row : row + 3, :] = source_pattern[:, j * LANES : (j + 1) * LANES]
    face = [lists[0, k : k + 1, :] for k in range(FACES)]
    listed = jnp.concatenate(face, axis=1)
    swapped = jnp.concatenate([face[1], face[0], face[3], face[2]], axis=1)
    side = lax.broadcasted_iota(jnp.int32, (1, LANES), 1) // (LANES // FACES)
    open_side = jnp.where(
        side < 2,
        jnp.where(side == 0, neighbours[0, 0], neighbours[0, 1]),
        jnp.where(side == 2, neighbours[0, 2], neighbours[0, 3]),
    )
    listed = jnp.where(open_side != 0, listed, -1)
    packed[LISTED_ROW : LISTED_ROW + 1, :] = listed.astype(jnp.float32)
    packed[SWAPPED_ROW : SWAPPED_ROW + 1, :] = swapped.astype(jnp.float32)
    set_incidence(packed, incidence)
    set_field(packed, incidence, field)
    send[...] = pick_lanes(field[...], jnp.broadcast_to(swapped, (8, LANES)))


def prepare_kernel(
    packed,
    shape_t,
    source,
    incidence,
    field,
    faces,
    inverse_index,
    connect,
    wide_gradient,
    wide_force,
    inverse_jacobian,
    lame_moduli,
    point_weights,
    rank,
    late_index,
    listed_index,
):
    nodes = field.shape[1]
    element_nodes = packed[CONNECT_ROW : CONNECT_ROW + NODE_ROWS, :].astype(jnp.int32)
    connect[...] = element_nodes
    inverse_jacobian[...] = packed[JACOBIAN_ROW : JACOBIAN_ROW + 9, :]
    lame_moduli[...] = packed[LAME_ROW : LAME_ROW + 2, :]
    point_weights[...] = packed[WEIGHTS_ROW : WEIGHTS_ROW + POINTS, :]
    rank[...] = packed[RANK_ROW : RANK_ROW + POINTS, :].astype(jnp.int32)
    set_incidence(packed, incidence)
    lane = lax.broadcasted_iota(jnp.int32, (LANES, nodes), 1)
    listed = packed[LISTED_ROW : LISTED_ROW + 1, :].astype(jnp.int32)
    column = jnp.broadcast_to(listed, (LANES, LANES)).T
    wide = jnp.concatenate([column] * (nodes // LANES), axis=1)
    late = jnp.broadcast_to(256 * (1 - source[0:1, :] % 2), (LANES, LANES)).T
    late = jnp.concatenate([late] * (nodes // LANES), axis=1)
    slot = lax.broadcasted_iota(jnp.int32, (LANES, nodes), 0) + 1 + late
    found = jnp.sum(jnp.where(wide == lane, slot, 0), axis=0, keepdims=True)
    placed = jnp.bitwise_and(found, 255) - 1
    inverse_index[...] = jnp.broadcast_to(placed, (8, nodes))
    late_row = jnp.where(found >= 256, placed, -1).astype(jnp.float32)
    late_row = jnp.broadcast_to(late_row, (8, nodes))
    for b in range(NODE_ROWS // 8):
        rows = slice(8 * b, 8 * b + 8)
        late_index[rows, :] = pick_lanes(late_row, element_nodes[rows]).astype(jnp.int32)
    listed_index[...] = jnp.broadcast_to(jnp.maximum(listed, 0), (8, LANES))
    set_faces(packed, faces)
    set_field(packed, incidence, field)

    reference_rows = 3 * POINTS
    shape_rows = jnp.concatenate(
        [shape_t[...], jnp.zeros((EL_NODES, LANES - reference_rows), jnp.float32)], axis=1
    )
    shape_rows = jnp.concatenate(
        [shape_rows, jnp.zeros((LANES - EL_NODES, LANES), jnp.float32)], axis=0
    )
    shape_columns = shape_rows.T
    for n in range(EL_NODES):
        wide_gradient[n] = jnp.broadcast_to(
            shape_columns[0:reference_rows, n : n + 1], (reference_rows, LANES)
        )
    for m in range(reference_rows):
        wide_force[m] = jnp.broadcast_to(shape_rows[0:NODE_ROWS, m : m + 1], (NODE_ROWS, LANES))


def contract(table, columns, count):
    sums = [[None, None] for _ in columns]
    for i in range(count):
        weights = table[i]
        for c, column in enumerate(columns):
            term = weights * column[i : i + 1, :]
            old = sums[c][i % 2]
            sums[c][i % 2] = term if old is None else old + term
    return [even + odd for even, odd in sums]


def wave_row(wave, width):
    return jnp.concatenate([wave[0:1, :]] * (width // LANES), axis=1)


def moved_up(wave):
    return pltpu.roll(wave[...], STEPS - 1, 0)


def at_elements(displace, connect):
    index = connect[...]
    columns = []
    for c in range(3):
        pieces = []
        for b in range(NODE_ROWS // 8):
            row = jnp.broadcast_to(displace[c : c + 1, :], (8, displace.shape[1]))
            pieces.append(pick_lanes(row, index[8 * b : 8 * b + 8]))
        columns.append(jnp.concatenate(pieces, axis=0))
    return columns


def strain_and_force(
    columns,
    strain,
    wide_gradient,
    wide_force,
    inverse_jacobian,
    lame_moduli,
    point_weights,
    faces,
    need_force,
):
    along = contract(wide_gradient, columns, EL_NODES)
    jac = [inverse_jacobian[i : i + 1, :] for i in range(9)]

    def ref_derivative(c, r):
        return along[c][r * POINTS : (r + 1) * POINTS, :]

    grad = [
        [
            (ref_derivative(c, 0) * jac[d] + ref_derivative(c, 1) * jac[3 + d])
            + ref_derivative(c, 2) * jac[6 + d]
            for d in range(3)
        ]
        for c in range(3)
    ]
    shear = {(c, d): grad[c][d] + grad[d][c] for c, d in ((1, 2), (0, 2), (0, 1))}
    rows = [grad[0][0], grad[1][1], grad[2][2]] + [0.5 * shear[k] for k in ((1, 2), (0, 2), (0, 1))]
    for s in range(STRAIN):
        strain[s * POINTS : (s + 1) * POINTS, :] = rows[s]
    if not need_force:
        return None
    volume = (grad[0][0] + grad[1][1]) + grad[2][2]
    weights = point_weights[...]
    shear_scale = lame_moduli[1:2, :] * weights
    pressure = (lame_moduli[0:1, :] * weights) * volume
    stress = [[None] * 3 for _ in range(3)]
    for c in range(3):
        for d in range(3):
            if c == d:
                stress[c][d] = shear_scale * (grad[c][c] + grad[c][c]) + pressure
            else:
                stress[c][d] = shear_scale * shear[(min(c, d), max(c, d))]
    columns = []
    for c in range(3):
        mapped = [
            (stress[c][0] * jac[3 * r] + stress[c][1] * jac[3 * r + 1])
            + stress[c][2] * jac[3 * r + 2]
            for r in range(3)
        ]
        columns.append(jnp.concatenate(mapped, axis=0))
    node_forces = contract(wide_force, columns, 3 * POINTS)
    parts = parts_of(jnp.concatenate(node_rows(node_forces), axis=1))
    sums = matmul(jnp.concatenate(parts, axis=0).astype(jnp.bfloat16), faces[...])
    return node_forces, (sums[16:24] + sums[8:16]) + sums[0:8]


def node_rows(node_forces):
    row_id = lax.broadcasted_iota(jnp.int32, (8, LANES), 0) % 4
    pieces = []
    for n in range(EL_NODES):
        first, second, third = (
            jnp.broadcast_to(node_forces[c][n : n + 1, :], (8, LANES)) for c in range(3)
        )
        pieces.append(jnp.where(row_id == 0, first, jnp.where(row_id == 1, second, third)))
    return pieces


def keep_forces(result, node_forces, send):
    forces, faces = result
    for c in range(3):
        node_forces[c] = forces[c]
    send[...] = faces


def first_kernel(
    wave,
    dom1,
    grp1,
    dom0,
    grp0,
    source,
    inverse_index,
    listed_index,
    field,
    connect,
    wide_gradient,
    wide_force,
    inverse_jacobian,
    lame_moduli,
    point_weights,
    faces,
    strain,
    displace,
    velocity,
    pattern,
    half_inverse_mass,
    late_scale,
    node_forces,
    send,
    next_wave,
):
    next_wave[...] = moved_up(wave)
    received = early_received(source[...], dom1[...], grp1[...])
    received = received + late_received(source[...], dom0[...], grp0[...])
    total = field[...] + spread(received, inverse_index[...])
    scale = jnp.broadcast_to(time_step * (1.0 / total[3:4, :]), total.shape)
    pattern[...] = total
    half_inverse_mass[...] = scale
    late_scale[...] = time_step * pick_lanes(scale, listed_index[...])
    new_velocity = scale * (wave_row(wave, total.shape[1]) * total)
    velocity[...] = new_velocity
    new_displace = time_step * new_velocity
    displace[...] = new_displace
    result = strain_and_force(
        at_elements(new_displace, connect),
        strain,
        wide_gradient,
        wide_force,
        inverse_jacobian,
        lame_moduli,
        point_weights,
        faces,
        True,
    )
    keep_forces(result, node_forces, send)


def side_kernel(
    wave,
    dom1,
    grp1,
    last_dom0,
    last_grp0,
    source,
    inverse_index,
    connect,
    incidence,
    pattern,
    half_inverse_mass,
    old_displace,
    old_velocity,
    node_forces,
    displace,
    velocity,
    columns,
    next_wave,
):
    next_wave[...] = moved_up(wave)
    index, scale = inverse_index[...], half_inverse_mass[...]
    missing = spread(late_received(source[...], last_dom0[...], last_grp0[...]), index) * scale
    parts = [node_forces[c] for c in range(3)]
    chunk = jnp.right_shift(connect[...], 7)
    chunks = [chunk[n : n + 1, :] for n in range(EL_NODES)]
    force = scatter_nodes(node_rows(parts), chunks, incidence[...])
    stiff = force + spread(early_received(source[...], dom1[...], grp1[...]), index)
    total = wave_row(wave, stiff.shape[1]) * pattern[...] - stiff
    new_velocity = (old_velocity[...] - missing) + scale * total
    velocity[...] = new_velocity
    new_displace = (old_displace[...] - time_step * missing) + time_step * new_velocity
    displace[...] = new_displace
    for c, column in enumerate(at_elements(new_displace, connect)):
        columns[c] = column


def step_kernel(
    dom0,
    grp0,
    source,
    late_index,
    late_scale,
    base_columns,
    wide_gradient,
    wide_force,
    inverse_jacobian,
    lame_moduli,
    point_weights,
    faces,
    strain,
    *rest,
):
    late = late_scale[...] * late_received(source[...], dom0[...], grp0[...])
    columns = []
    for c in range(3):
        row = jnp.broadcast_to(late[c : c + 1, :], (8, LANES))
        pieces = []
        for b in range(NODE_ROWS // 8):
            index = late_index[8 * b : 8 * b + 8, :]
            taken = jnp.where(index >= 0, lane_gather(row, jnp.maximum(index, 0)), 0.0)
            pieces.append(base_columns[c, 8 * b : 8 * b + 8, :] - taken)
        columns.append(jnp.concatenate(pieces, axis=0))
    result = strain_and_force(
        columns,
        strain,
        wide_gradient,
        wide_force,
        inverse_jacobian,
        lame_moduli,
        point_weights,
        faces,
        bool(rest),
    )
    if rest:
        keep_forces(result, *rest)


def order_kernel(rank, strains, before_last, total, chosen, store):
    for t in range(STEPS):
        for c in range(STRAIN):
            row = (c * STEPS + t) * POINTS
            rows = slice(c * POINTS, (c + 1) * POINTS)
            if t < STEPS - 2:
                block = strains[t, rows, :]
            elif t == STEPS - 2:
                block = before_last[rows, :]
            else:
                block = jnp.zeros((POINTS, LANES), jnp.float32)
            store[row : row + POINTS, :] = block
    lane = lax.broadcasted_iota(jnp.int32, (LANES, ORDER_WIDTH), 1)
    for q in range(POINTS):
        column = jnp.broadcast_to(rank[q : q + 1, :] % ORDER_WIDTH, (LANES, LANES)).T
        wide = jnp.concatenate([column] * (ORDER_WIDTH // LANES), axis=1)
        chosen[q * LANES : (q + 1) * LANES, :] = jnp.where(wide == lane, 1.0, 0.0).astype(
            jnp.bfloat16
        )
    total[...] = matmul(grouped_values(rank, store, STEPS * STRAIN), chosen[...])


def grouped_values(rank, store, height):
    values = []
    for q in range(POINTS):
        block = store[pl.ds(q, height, stride=POINTS), :]
        group = rank[q : q + 1, :] // ORDER_WIDTH
        masked = [
            jnp.where(group == k, block, 0.0) for k in range(POINTS * LANES // ORDER_WIDTH)
        ]
        values.append(jnp.concatenate(masked, axis=0).astype(jnp.bfloat16))
    return jnp.concatenate(values, axis=1)


def finish_kernel(rank, total, chosen, last, out, store):
    store[...] = jnp.zeros(store.shape, jnp.float32)
    store[0 : STRAIN * POINTS, :] = last[...]
    ends = matmul(grouped_values(rank, store, 8), chosen[...])
    height = STEPS * STRAIN
    row_id = lax.broadcasted_iota(jnp.int32, (STEPS, LANES), 0)
    for w in range(rank.shape[0]):
        k, i = w * LANES // ORDER_WIDTH, w % (ORDER_WIDTH // LANES)
        lanes = slice(i * LANES, (i + 1) * LANES)
        for c in range(STRAIN):
            row = k * height + c * STEPS
            end = jnp.broadcast_to(ends[8 * k + c : 8 * k + c + 1, lanes], (STEPS, LANES))
            block = jnp.where(row_id == STEPS - 1, end, total[row : row + STEPS, lanes])
            out[w, c * STEPS : (c + 1) * STEPS, :] = block.astype(jnp.bfloat16)


def place_kernel(pieces, out):
    for w in range(pieces.shape[0]):
        held = snake("dom", w)
        for c in range(STRAIN):
            out[c, :, w * LANES : (w + 1) * LANES] = pieces[held, c * STEPS : (c + 1) * STEPS, :]


def shards(
    connect,
    interface_nodes,
    neighbours,
    point_rank,
    shape_grad,
    inverse_jacobian,
    lame_moduli,
    point_weights,
    mass_elem,
    source_pattern,
    wavelet,
):
    nodes = source_pattern.shape[1]
    f32 = jnp.float32
    field_t = jax.ShapeDtypeStruct((8, nodes), f32)
    lanes_t = jax.ShapeDtypeStruct((8, LANES), f32)
    index_t = jax.ShapeDtypeStruct((8, LANES), jnp.int32)
    strain_t = jax.ShapeDtypeStruct((STRAIN * POINTS, LANES), f32)

    face = lax.broadcasted_iota(jnp.int32, (8, LANES), 1) // (LANES // FACES)
    dom = lax.axis_index("dom")
    parity = jnp.where(face < 2, lax.axis_index("grp") % 2, (dom // DOM_ROW + dom) % 2)
    source = 2 * (face // 2) + jnp.bitwise_xor(parity, 1 - face % 2)

    def exchange(send):
        received = []
        for name in EXCHANGES:
            axis, offset = name[:3], int(name[3])
            count = lax.axis_size(axis)
            pairs = []
            for i in range(offset, count - 1, 2):
                first, second = snake(axis, i), snake(axis, i + 1)
                pairs += [(first, second), (second, first)]
            received.append(lax.ppermute(send, axis, pairs))
        return received

    i32, bf16 = jnp.int32, jnp.bfloat16
    rank_rows = point_rank.reshape(POINTS, LANES)
    arguments = (
        wavelet,
        neighbours,
        connect,
        interface_nodes,
        mass_elem,
        source_pattern,
        shape_grad.T,
        inverse_jacobian,
        lame_moduli,
        point_weights,
        rank_rows,
    )
    buffers = [pltpu.SMEM(x.shape, x.dtype) for x in arguments[:2]]
    buffers += [pltpu.VMEM(x.shape, x.dtype) for x in arguments[2:6] + arguments[7:]]
    packed, shape_t, wave, send = kernel_call(
        pack_kernel,
        [
            jax.ShapeDtypeStruct((PACKED_ROWS, LANES), f32),
            jax.ShapeDtypeStruct(shape_grad.T.shape, f32),
            jax.ShapeDtypeStruct((STEPS, LANES), f32),
            lanes_t,
        ],
        [HBM] * len(arguments),
        scratch=buffers
        + [
            pltpu.SemaphoreType.DMA((len(arguments),)),
            pltpu.VMEM((EL_NODES * LANES, LANES), bf16),
            pltpu.VMEM(field_t.shape, f32),
        ],
    )(*(pltpu.with_memory_space_constraint(x, pltpu.MemorySpace.HBM) for x in arguments))
    writers = lax.axis_size("dom")
    packed = lax.ppermute(packed, "dom", [(i, snake("dom", i)) for i in range(writers)])
    received = []
    for name in EXCHANGES:
        axis, offset = name[:3], int(name[3])
        pairs = []
        for g in range(lax.axis_size("grp")):
            for w in range(writers):
                index, count = (g, lax.axis_size("grp")) if axis == "grp" else (w, writers)
                other = index + 1 if index % 2 == offset else index - 1
                if 0 <= other < count:
                    to_g, to_w = (other, w) if axis == "grp" else (g, other)
                    target = to_g * writers + snake("dom", to_w)
                    pairs.append((g * writers + w, target))
        received.append(lax.ppermute(send, ("grp", "dom"), pairs))

    prepare = kernel_call(
        prepare_kernel,
        [
            jax.ShapeDtypeStruct((EL_NODES * LANES, LANES), bf16),
            field_t,
            jax.ShapeDtypeStruct((EL_NODES * LANES, LANES), bf16),
            jax.ShapeDtypeStruct((8, nodes), i32),
            jax.ShapeDtypeStruct((NODE_ROWS, LANES), i32),
            jax.ShapeDtypeStruct((EL_NODES, 3 * POINTS, LANES), f32),
            jax.ShapeDtypeStruct((3 * POINTS, NODE_ROWS, LANES), f32),
            jax.ShapeDtypeStruct(inverse_jacobian.shape, f32),
            jax.ShapeDtypeStruct(lame_moduli.shape, f32),
            jax.ShapeDtypeStruct(point_weights.shape, f32),
            jax.ShapeDtypeStruct(rank_rows.shape, i32),
            jax.ShapeDtypeStruct((NODE_ROWS, LANES), i32),
            index_t,
        ],
        [VMEM] * 3,
    )
    outs = prepare(packed, shape_t, source)
    incidence, field, faces, inverse_index = outs[:4]
    rank = outs[10]
    connect_rows = outs[4]
    late_index, listed_index = outs[11:]
    element_data = (*outs[5:10], faces)
    wave_t = jax.ShapeDtypeStruct((STEPS, LANES), f32)
    forces_t = jax.ShapeDtypeStruct((3, NODE_ROWS, LANES), f32)
    (
        strain,
        displace,
        velocity,
        pattern,
        half_inverse_mass,
        late_scale,
        node_forces,
        send,
        wave,
    ) = kernel_call(
        first_kernel,
        [strain_t, field_t, field_t, field_t, field_t, lanes_t, forces_t, lanes_t, wave_t],
        [VMEM] * 16,
    )(wave, *received, source, inverse_index, listed_index, field, connect_rows, *element_data)
    strains = jnp.zeros((STEPS - 2, STRAIN * POINTS, LANES), f32)

    def advance(last, displace, velocity, late, node_forces, send, wave):
        dom1, grp1, *new_late = exchange(send)
        side = kernel_call(side_kernel, [field_t, field_t, forces_t, wave_t], [VMEM] * 14)
        displace, velocity, columns, wave = side(
            wave,
            dom1,
            grp1,
            *late,
            source,
            inverse_index,
            connect_rows,
            incidence,
            pattern,
            half_inverse_mass,
            displace,
            velocity,
            node_forces,
        )
        outs = kernel_call(
            step_kernel, [strain_t] + ([] if last else [forces_t, lanes_t]), [VMEM] * 12
        )(*new_late, source, late_index, late_scale, columns, *element_data)
        return outs[0], displace, velocity, new_late, *outs[1:], wave

    def body(step, carried):
        strains, strain, *state = carried
        strains = lax.dynamic_update_index_in_dim(strains, strain, step - 1, 0)
        return (strains, *advance(False, *state))

    none = [jnp.zeros((8, LANES), f32)] * 2
    carried = (strains, strain, displace, velocity, none, node_forces, send, wave)
    strains, strain, *state = lax.fori_loop(1, STEPS - 1, body, carried)
    order = kernel_call(
        order_kernel,
        [
            jax.ShapeDtypeStruct((POINTS * LANES // ORDER_WIDTH * STEPS * STRAIN, ORDER_WIDTH), f32),
            jax.ShapeDtypeStruct((POINTS * LANES, ORDER_WIDTH), bf16),
        ],
        [VMEM] * 3,
        scratch=[pltpu.VMEM(((STEPS * STRAIN + 1) * POINTS, LANES), f32)],
    )
    total, chosen = order(rank, strains, strain)
    strain = advance(True, *state)[0]
    (ordered,) = kernel_call(
        finish_kernel,
        [jax.ShapeDtypeStruct((writers, STEPS * STRAIN, LANES), bf16)],
        [VMEM] * 4,
        scratch=[pltpu.VMEM((9 * POINTS, LANES), f32)],
    )(rank, total, chosen, strain)
    pieces = lax.all_to_all(ordered, "dom", split_axis=0, concat_axis=0, tiled=True)
    (placed,) = kernel_call(
        place_kernel, [jax.ShapeDtypeStruct((STRAIN, STEPS, writers * LANES), jnp.bfloat16)], [VMEM]
    )(pieces)
    return placed.transpose(1, 0, 2)


def solution(mesh):
    placed = (
        P(None, ("grp", "dom")),
        P(("grp", "dom"), None, None),
        P(("grp", "dom"), None),
        P(("grp", "dom"), None),
        P(),
        P(None, ("grp", "dom")),
        P(None, ("grp", "dom")),
        P(None, ("grp", "dom")),
        P(None, ("grp", "dom")),
        P(None, ("grp", "dom")),
        P(),
    )
    return jax.shard_map(
        shards, mesh=mesh, in_specs=placed, out_specs=P(None, None, ("grp", "dom")), check_vma=False
    )
```

```python
import jax
import jax.numpy as jnp
from jax import lax
from jax.experimental import pallas as pl
from jax.experimental.pallas import tpu as pltpu
from jax.sharding import PartitionSpec as P


EL_NODES = 20
NODE_ROWS = 24
POINTS = 16
STRAIN = 6
STEPS = 16
LANES = 128
FACES = 4
ORDER_WIDTH = 256

time_step = 0.5

DOM_ROW = 4

EXCHANGES = ("grp1", "dom1", "dom0", "grp0")
HANDED = ("dom1", "grp1", "dom0", "grp0")

VMEM = pl.BlockSpec(memory_space=pltpu.VMEM)
HBM = pl.BlockSpec(memory_space=pltpu.MemorySpace.HBM)


def snake(axis, index):
    row, column = index // DOM_ROW, index % DOM_ROW
    return index if axis == "grp" or row % 2 == 0 else row * DOM_ROW + DOM_ROW - 1 - column


def kernel_call(body, outs, specs, scratch=()):
    return pl.pallas_call(
        body,
        out_shape=outs,
        in_specs=specs,
        out_specs=[VMEM] * len(outs),
        scratch_shapes=list(scratch),
        compiler_params=pltpu.CompilerParams(vmem_limit_bytes=24 * 1024 * 1024),
    )


def parts_of(x):
    high = x.astype(jnp.bfloat16).astype(jnp.float32)
    rest = x - high
    middle = rest.astype(jnp.bfloat16).astype(jnp.float32)
    low = (rest - middle).astype(jnp.bfloat16).astype(jnp.float32)
    return high, middle, low


def matmul(left, right):
    return jnp.dot(left, right, preferred_element_type=jnp.float32)


def lane_gather(row, index):
    return jnp.take_along_axis(row, index, axis=1, mode="promise_in_bounds")


def pick_lanes(field, index):
    low = jnp.bitwise_and(index, LANES - 1)
    chunk = jnp.right_shift(index, 7)
    out = lane_gather(field[:, 0:LANES], low)
    for j in range(1, field.shape[1] // LANES):
        out = jnp.where(
            chunk == j, lane_gather(field[:, j * LANES : (j + 1) * LANES], low), out
        )
    return out


def spread(received, inverse):
    out = []
    for j in range(inverse.shape[1] // LANES):
        index = inverse[:, j * LANES : (j + 1) * LANES]
        taken = lane_gather(received, jnp.maximum(index, 0))
        out.append(jnp.where(index >= 0, taken, 0.0))
    return jnp.concatenate(out, axis=1)


def early_received(source, dom1, grp1):
    return jnp.where(source == 3, dom1, jnp.where(source == 1, grp1, 0.0))


def late_received(source, dom0, grp0):
    return jnp.where(source == 2, dom0, jnp.where(source == 0, grp0, 0.0))


def scatter_nodes(pieces, chunks, incidence):
    group = lax.broadcasted_iota(jnp.int32, (8, LANES), 0) // 4
    parts = [[], [], []]
    for piece, chunk in zip(pieces, chunks):
        both = [jnp.where(chunk == group + base, piece, 0.0) for base in (0, 2)]
        for i, part in enumerate(parts_of(jnp.concatenate(both, axis=0))):
            parts[i].append(part.astype(jnp.bfloat16))
    left = jnp.concatenate([jnp.concatenate(p, axis=1) for p in parts], axis=0)
    sums = matmul(left, incidence)
    total = (sums[32:48] + sums[16:32]) + sums[0:16]
    fields = []
    for base in (0, 8):
        rows = total[base : base + 8]
        fields += [rows, pltpu.roll(rows, 4, 0)]
    return jnp.concatenate(fields, axis=1)


CONNECT_ROW = 0
MASS_ROW = 24
LAME_ROW = 44
LISTED_ROW = 46
SWAPPED_ROW = 47
JACOBIAN_ROW = 48
WEIGHTS_ROW = 64
SOURCE_ROW = 80
RANK_ROW = 96
PACKED_ROWS = 112


def set_incidence(packed, incidence):
    element_nodes = packed[CONNECT_ROW : CONNECT_ROW + NODE_ROWS, :].astype(jnp.int32)
    low = jnp.bitwise_and(element_nodes, LANES - 1)
    own_lane = lax.broadcasted_iota(jnp.int32, (LANES, LANES), 1)
    for n in range(EL_NODES):
        column = jnp.broadcast_to(low[n : n + 1, :], (LANES, LANES)).T
        incidence[n * LANES : (n + 1) * LANES, :] = jnp.where(
            column == own_lane, 1.0, 0.0
        ).astype(jnp.bfloat16)


def set_faces(packed, faces):
    element_nodes = packed[CONNECT_ROW : CONNECT_ROW + NODE_ROWS, :].astype(jnp.int32)
    sent = packed[SWAPPED_ROW : SWAPPED_ROW + 1, :].astype(jnp.int32)
    for n in range(EL_NODES):
        column = jnp.broadcast_to(element_nodes[n : n + 1, :], (LANES, LANES)).T
        faces[n * LANES : (n + 1) * LANES, :] = jnp.where(column == sent, 1.0, 0.0).astype(
            jnp.bfloat16
        )


def set_field(packed, incidence, field):
    element_nodes = packed[CONNECT_ROW : CONNECT_ROW + NODE_ROWS, :].astype(jnp.int32)
    chunk = jnp.right_shift(element_nodes, 7)
    masses = [
        jnp.broadcast_to(packed[MASS_ROW + n : MASS_ROW + n + 1, :], (8, LANES))
        for n in range(EL_NODES)
    ]
    chunks = [chunk[n : n + 1, :] for n in range(EL_NODES)]
    field[...] = scatter_nodes(masses, chunks, incidence[...])
    for j in range(field.shape[1] // LANES):
        row = SOURCE_ROW + 3 * j
        field[0:3, j * LANES : (j + 1) * LANES] = packed[row : row + 3, :]


def pack_kernel(
    wavelet_in,
    neighbours_in,
    connect_in,
    lists_in,
    mass_in,
    source_in,
    shape_in,
    jacobian_in,
    lame_in,
    weights_in,
    rank_in,
    packed,
    shape_t,
    wave,
    send,
    wavelet,
    neighbours,
    connect,
    lists,
    mass_elem,
    source_pattern,
    jacobian,
    lame,
    weights,
    rank,
    sems,
    incidence,
    field,
):
    moves = [
        (wavelet_in, wavelet),
        (neighbours_in, neighbours),
        (connect_in, connect),
        (lists_in, lists),
        (mass_in, mass_elem),
        (source_in, source_pattern),
        (shape_in, shape_t),
        (jacobian_in, jacobian),
        (lame_in, lame),
        (weights_in, weights),
        (rank_in, rank),
    ]
    copies = [pltpu.make_async_copy(a, b, sems.at[i]) for i, (a, b) in enumerate(moves)]
    for copy in copies:
        copy.start()
    packed[...] = jnp.zeros(packed.shape, jnp.float32)
    for copy in copies:
        copy.wait()
    wave[...] = jnp.concatenate(
        [jnp.full((1, LANES), wavelet[t], jnp.float32) for t in range(STEPS)], axis=0
    )
    packed[CONNECT_ROW : CONNECT_ROW + EL_NODES, :] = connect[...].astype(jnp.float32)
    packed[MASS_ROW : MASS_ROW + EL_NODES, :] = mass_elem[...]
    packed[LAME_ROW : LAME_ROW + 2, :] = lame[...]
    packed[JACOBIAN_ROW : JACOBIAN_ROW + 9, :] = jacobian[...]
    packed[WEIGHTS_ROW : WEIGHTS_ROW + POINTS, :] = weights[...]
    packed[RANK_ROW : RANK_ROW + POINTS, :] = rank[...].astype(jnp.float32)
    for j in range(source_pattern.shape[1] // LANES):
        row = SOURCE_ROW + 3 * j
        packed[row : row + 3, :] = source_pattern[:, j * LANES : (j + 1) * LANES]
    face = [lists[0, k : k + 1, :] for k in range(FACES)]
    listed = jnp.concatenate(face, axis=1)
    swapped = jnp.concatenate([face[1], face[0], face[3], face[2]], axis=1)
    side = lax.broadcasted_iota(jnp.int32, (1, LANES), 1) // (LANES // FACES)
    open_side = jnp.where(
        side < 2,
        jnp.where(side == 0, neighbours[0, 0], neighbours[0, 1]),
        jnp.where(side == 2, neighbours[0, 2], neighbours[0, 3]),
    )
    listed = jnp.where(open_side != 0, listed, -1)
    packed[LISTED_ROW : LISTED_ROW + 1, :] = listed.astype(jnp.float32)
    packed[SWAPPED_ROW : SWAPPED_ROW + 1, :] = swapped.astype(jnp.float32)
    set_incidence(packed, incidence)
    set_field(packed, incidence, field)
    send[...] = pick_lanes(field[...], jnp.broadcast_to(swapped, (8, LANES)))


def prepare_kernel(
    packed,
    shape_t,
    source,
    incidence,
    field,
    faces,
    inverse_index,
    connect,
    wide_gradient,
    wide_force,
    inverse_jacobian,
    lame_moduli,
    point_weights,
    rank,
    late_index,
    listed_index,
):
    nodes = field.shape[1]
    element_nodes = packed[CONNECT_ROW : CONNECT_ROW + NODE_ROWS, :].astype(jnp.int32)
    connect[...] = element_nodes
    inverse_jacobian[...] = packed[JACOBIAN_ROW : JACOBIAN_ROW + 9, :]
    lame_moduli[...] = packed[LAME_ROW : LAME_ROW + 2, :]
    point_weights[...] = packed[WEIGHTS_ROW : WEIGHTS_ROW + POINTS, :]
    rank[...] = packed[RANK_ROW : RANK_ROW + POINTS, :].astype(jnp.int32)
    set_incidence(packed, incidence)
    lane = lax.broadcasted_iota(jnp.int32, (LANES, nodes), 1)
    listed = packed[LISTED_ROW : LISTED_ROW + 1, :].astype(jnp.int32)
    column = jnp.broadcast_to(listed, (LANES, LANES)).T
    wide = jnp.concatenate([column] * (nodes // LANES), axis=1)
    late = jnp.broadcast_to(256 * (1 - source[0:1, :] % 2), (LANES, LANES)).T
    late = jnp.concatenate([late] * (nodes // LANES), axis=1)
    slot = lax.broadcasted_iota(jnp.int32, (LANES, nodes), 0) + 1 + late
    found = jnp.sum(jnp.where(wide == lane, slot, 0), axis=0, keepdims=True)
    placed = jnp.bitwise_and(found, 255) - 1
    inverse_index[...] = jnp.broadcast_to(placed, (8, nodes))
    late_row = jnp.where(found >= 256, placed, -1).astype(jnp.float32)
    late_row = jnp.broadcast_to(late_row, (8, nodes))
    for b in range(NODE_ROWS // 8):
        rows = slice(8 * b, 8 * b + 8)
        late_index[rows, :] = pick_lanes(late_row, element_nodes[rows]).astype(jnp.int32)
    listed_index[...] = jnp.broadcast_to(jnp.maximum(listed, 0), (8, LANES))
    set_faces(packed, faces)
    set_field(packed, incidence, field)

    reference_rows = 3 * POINTS
    shape_rows = jnp.concatenate(
        [shape_t[...], jnp.zeros((EL_NODES, LANES - reference_rows), jnp.float32)], axis=1
    )
    shape_rows = jnp.concatenate(
        [shape_rows, jnp.zeros((LANES - EL_NODES, LANES), jnp.float32)], axis=0
    )
    shape_columns = shape_rows.T
    for n in range(EL_NODES):
        wide_gradient[n] = jnp.broadcast_to(
            shape_columns[0:reference_rows, n : n + 1], (reference_rows, LANES)
        )
    for m in range(reference_rows):
        wide_force[m] = jnp.broadcast_to(shape_rows[0:NODE_ROWS, m : m + 1], (NODE_ROWS, LANES))


def contract(table, columns, count):
    sums = [[None, None] for _ in columns]
    for i in range(count):
        weights = table[i]
        for c, column in enumerate(columns):
            term = weights * column[i : i + 1, :]
            old = sums[c][i % 2]
            sums[c][i % 2] = term if old is None else old + term
    return [even + odd for even, odd in sums]


def wave_row(wave, width):
    return jnp.concatenate([wave[0:1, :]] * (width // LANES), axis=1)


def moved_up(wave):
    return pltpu.roll(wave[...], STEPS - 1, 0)


def at_elements(displace, connect):
    index = connect[...]
    columns = []
    for c in range(3):
        pieces = []
        for b in range(NODE_ROWS // 8):
            row = jnp.broadcast_to(displace[c : c + 1, :], (8, displace.shape[1]))
            pieces.append(pick_lanes(row, index[8 * b : 8 * b + 8]))
        columns.append(jnp.concatenate(pieces, axis=0))
    return columns


def strain_and_force(
    columns,
    strain,
    wide_gradient,
    wide_force,
    inverse_jacobian,
    lame_moduli,
    point_weights,
    faces,
    need_force,
):
    along = contract(wide_gradient, columns, EL_NODES)
    jac = [inverse_jacobian[i : i + 1, :] for i in range(9)]

    def ref_derivative(c, r):
        return along[c][r * POINTS : (r + 1) * POINTS, :]

    grad = [
        [
            (ref_derivative(c, 0) * jac[d] + ref_derivative(c, 1) * jac[3 + d])
            + ref_derivative(c, 2) * jac[6 + d]
            for d in range(3)
        ]
        for c in range(3)
    ]
    shear = {(c, d): grad[c][d] + grad[d][c] for c, d in ((1, 2), (0, 2), (0, 1))}
    rows = [grad[0][0], grad[1][1], grad[2][2]] + [0.5 * shear[k] for k in ((1, 2), (0, 2), (0, 1))]
    for s in range(STRAIN):
        strain[s * POINTS : (s + 1) * POINTS, :] = rows[s]
    if not need_force:
        return None
    volume = (grad[0][0] + grad[1][1]) + grad[2][2]
    weights = point_weights[...]
    shear_scale = lame_moduli[1:2, :] * weights
    pressure = (lame_moduli[0:1, :] * weights) * volume
    stress = [[None] * 3 for _ in range(3)]
    for c in range(3):
        for d in range(3):
            if c == d:
                stress[c][d] = shear_scale * (grad[c][c] + grad[c][c]) + pressure
            else:
                stress[c][d] = shear_scale * shear[(min(c, d), max(c, d))]
    columns = []
    for c in range(3):
        mapped = [
            (stress[c][0] * jac[3 * r] + stress[c][1] * jac[3 * r + 1])
            + stress[c][2] * jac[3 * r + 2]
            for r in range(3)
        ]
        columns.append(jnp.concatenate(mapped, axis=0))
    node_forces = contract(wide_force, columns, 3 * POINTS)
    parts = parts_of(jnp.concatenate(node_rows(node_forces), axis=1))[:2]
    sums = matmul(jnp.concatenate(parts, axis=0).astype(jnp.bfloat16), faces[...])
    return node_forces, sums[8:16] + sums[0:8]


def node_rows(node_forces):
    row_id = lax.broadcasted_iota(jnp.int32, (8, LANES), 0) % 4
    pieces = []
    for n in range(EL_NODES):
        first, second, third = (
            jnp.broadcast_to(node_forces[c][n : n + 1, :], (8, LANES)) for c in range(3)
        )
        pieces.append(jnp.where(row_id == 0, first, jnp.where(row_id == 1, second, third)))
    return pieces


def keep_forces(result, node_forces, send):
    forces, faces = result
    for c in range(3):
        node_forces[c] = forces[c]
    send[...] = faces


def first_kernel(
    wave,
    dom1,
    grp1,
    dom0,
    grp0,
    source,
    inverse_index,
    listed_index,
    field,
    connect,
    wide_gradient,
    wide_force,
    inverse_jacobian,
    lame_moduli,
    point_weights,
    faces,
    strain,
    displace,
    velocity,
    pattern,
    half_inverse_mass,
    late_scale,
    node_forces,
    send,
    next_wave,
):
    next_wave[...] = moved_up(wave)
    received = early_received(source[...], dom1[...], grp1[...])
    received = received + late_received(source[...], dom0[...], grp0[...])
    total = field[...] + spread(received, inverse_index[...])
    scale = jnp.broadcast_to(time_step * (1.0 / total[3:4, :]), total.shape)
    pattern[...] = total
    half_inverse_mass[...] = scale
    late_scale[...] = time_step * pick_lanes(scale, listed_index[...])
    new_velocity = scale * (wave_row(wave, total.shape[1]) * total)
    velocity[...] = new_velocity
    new_displace = time_step * new_velocity
    displace[...] = new_displace
    result = strain_and_force(
        at_elements(new_displace, connect),
        strain,
        wide_gradient,
        wide_force,
        inverse_jacobian,
        lame_moduli,
        point_weights,
        faces,
        True,
    )
    keep_forces(result, node_forces, send)


def side_kernel(
    wave,
    dom1,
    grp1,
    last_dom0,
    last_grp0,
    source,
    inverse_index,
    connect,
    incidence,
    pattern,
    half_inverse_mass,
    old_displace,
    old_velocity,
    node_forces,
    displace,
    velocity,
    columns,
    next_wave,
):
    next_wave[...] = moved_up(wave)
    index, scale = inverse_index[...], half_inverse_mass[...]
    missing = spread(late_received(source[...], last_dom0[...], last_grp0[...]), index) * scale
    parts = [node_forces[c] for c in range(3)]
    chunk = jnp.right_shift(connect[...], 7)
    chunks = [chunk[n : n + 1, :] for n in range(EL_NODES)]
    force = scatter_nodes(node_rows(parts), chunks, incidence[...])
    stiff = force + spread(early_received(source[...], dom1[...], grp1[...]), index)
    total = wave_row(wave, stiff.shape[1]) * pattern[...] - stiff
    new_velocity = (old_velocity[...] - missing) + scale * total
    velocity[...] = new_velocity
    new_displace = (old_displace[...] - time_step * missing) + time_step * new_velocity
    displace[...] = new_displace
    for c, column in enumerate(at_elements(new_displace, connect)):
        columns[c] = column


def step_kernel(
    dom0,
    grp0,
    source,
    late_index,
    late_scale,
    base_columns,
    wide_gradient,
    wide_force,
    inverse_jacobian,
    lame_moduli,
    point_weights,
    faces,
    strain,
    *rest,
):
    late = late_scale[...] * late_received(source[...], dom0[...], grp0[...])
    columns = []
    for c in range(3):
        row = jnp.broadcast_to(late[c : c + 1, :], (8, LANES))
        pieces = []
        for b in range(NODE_ROWS // 8):
            index = late_index[8 * b : 8 * b + 8, :]
            taken = jnp.where(index >= 0, lane_gather(row, jnp.maximum(index, 0)), 0.0)
            pieces.append(base_columns[c, 8 * b : 8 * b + 8, :] - taken)
        columns.append(jnp.concatenate(pieces, axis=0))
    result = strain_and_force(
        columns,
        strain,
        wide_gradient,
        wide_force,
        inverse_jacobian,
        lame_moduli,
        point_weights,
        faces,
        bool(rest),
    )
    if rest:
        keep_forces(result, *rest)


def order_kernel(rank, strains, before_last, total, chosen, store):
    for t in range(STEPS):
        for c in range(STRAIN):
            row = (c * STEPS + t) * POINTS
            rows = slice(c * POINTS, (c + 1) * POINTS)
            if t < STEPS - 2:
                block = strains[t, rows, :]
            elif t == STEPS - 2:
                block = before_last[rows, :]
            else:
                block = jnp.zeros((POINTS, LANES), jnp.float32)
            store[row : row + POINTS, :] = block
    lane = lax.broadcasted_iota(jnp.int32, (LANES, ORDER_WIDTH), 1)
    for q in range(POINTS):
        column = jnp.broadcast_to(rank[q : q + 1, :] % ORDER_WIDTH, (LANES, LANES)).T
        wide = jnp.concatenate([column] * (ORDER_WIDTH // LANES), axis=1)
        chosen[q * LANES : (q + 1) * LANES, :] = jnp.where(wide == lane, 1.0, 0.0).astype(
            jnp.bfloat16
        )
    total[...] = matmul(grouped_values(rank, store, STEPS * STRAIN), chosen[...])


def grouped_values(rank, store, height):
    values = []
    for q in range(POINTS):
        block = store[pl.ds(q, height, stride=POINTS), :]
        group = rank[q : q + 1, :] // ORDER_WIDTH
        masked = [
            jnp.where(group == k, block, 0.0) for k in range(POINTS * LANES // ORDER_WIDTH)
        ]
        values.append(jnp.concatenate(masked, axis=0).astype(jnp.bfloat16))
    return jnp.concatenate(values, axis=1)


def finish_kernel(rank, total, chosen, last, out, store):
    store[...] = jnp.zeros(store.shape, jnp.float32)
    store[0 : STRAIN * POINTS, :] = last[...]
    ends = matmul(grouped_values(rank, store, 8), chosen[...])
    height = STEPS * STRAIN
    row_id = lax.broadcasted_iota(jnp.int32, (STEPS, LANES), 0)
    for w in range(rank.shape[0]):
        k, i = w * LANES // ORDER_WIDTH, w % (ORDER_WIDTH // LANES)
        lanes = slice(i * LANES, (i + 1) * LANES)
        for c in range(STRAIN):
            row = k * height + c * STEPS
            end = jnp.broadcast_to(ends[8 * k + c : 8 * k + c + 1, lanes], (STEPS, LANES))
            block = jnp.where(row_id == STEPS - 1, end, total[row : row + STEPS, lanes])
            out[w, c * STEPS : (c + 1) * STEPS, :] = block.astype(jnp.bfloat16)


def place_kernel(pieces, out):
    for w in range(pieces.shape[0]):
        held = snake("dom", w)
        for c in range(STRAIN):
            out[c, :, w * LANES : (w + 1) * LANES] = pieces[held, c * STEPS : (c + 1) * STEPS, :]


def shards(
    connect,
    interface_nodes,
    neighbours,
    point_rank,
    shape_grad,
    inverse_jacobian,
    lame_moduli,
    point_weights,
    mass_elem,
    source_pattern,
    wavelet,
):
    nodes = source_pattern.shape[1]
    f32 = jnp.float32
    field_t = jax.ShapeDtypeStruct((8, nodes), f32)
    lanes_t = jax.ShapeDtypeStruct((8, LANES), f32)
    index_t = jax.ShapeDtypeStruct((8, LANES), jnp.int32)
    strain_t = jax.ShapeDtypeStruct((STRAIN * POINTS, LANES), f32)

    face = lax.broadcasted_iota(jnp.int32, (8, LANES), 1) // (LANES // FACES)
    dom = lax.axis_index("dom")
    parity = jnp.where(face < 2, lax.axis_index("grp") % 2, (dom // DOM_ROW + dom) % 2)
    source = 2 * (face // 2) + jnp.bitwise_xor(parity, 1 - face % 2)

    def exchange(send):
        received = {}
        for name in EXCHANGES:
            axis, offset = name[:3], int(name[3])
            count = lax.axis_size(axis)
            pairs = []
            for i in range(offset, count - 1, 2):
                first, second = snake(axis, i), snake(axis, i + 1)
                pairs += [(first, second), (second, first)]
            received[name] = lax.ppermute(send, axis, pairs)
        return [received[name] for name in HANDED]

    i32, bf16 = jnp.int32, jnp.bfloat16
    rank_rows = point_rank.reshape(POINTS, LANES)
    arguments = (
        wavelet,
        neighbours,
        connect,
        interface_nodes,
        mass_elem,
        source_pattern,
        shape_grad.T,
        inverse_jacobian,
        lame_moduli,
        point_weights,
        rank_rows,
    )
    buffers = [pltpu.SMEM(x.shape, x.dtype) for x in arguments[:2]]
    buffers += [pltpu.VMEM(x.shape, x.dtype) for x in arguments[2:6] + arguments[7:]]
    packed, shape_t, wave, send = kernel_call(
        pack_kernel,
        [
            jax.ShapeDtypeStruct((PACKED_ROWS, LANES), f32),
            jax.ShapeDtypeStruct(shape_grad.T.shape, f32),
            jax.ShapeDtypeStruct((STEPS, LANES), f32),
            lanes_t,
        ],
        [HBM] * len(arguments),
        scratch=buffers
        + [
            pltpu.SemaphoreType.DMA((len(arguments),)),
            pltpu.VMEM((EL_NODES * LANES, LANES), bf16),
            pltpu.VMEM(field_t.shape, f32),
        ],
    )(*(pltpu.with_memory_space_constraint(x, pltpu.MemorySpace.HBM) for x in arguments))
    writers = lax.axis_size("dom")
    packed = lax.ppermute(packed, "dom", [(i, snake("dom", i)) for i in range(writers)])
    received = {}
    for name in EXCHANGES:
        axis, offset = name[:3], int(name[3])
        pairs = []
        for g in range(lax.axis_size("grp")):
            for w in range(writers):
                index, count = (g, lax.axis_size("grp")) if axis == "grp" else (w, writers)
                other = index + 1 if index % 2 == offset else index - 1
                if 0 <= other < count:
                    to_g, to_w = (other, w) if axis == "grp" else (g, other)
                    target = to_g * writers + snake("dom", to_w)
                    pairs.append((g * writers + w, target))
        received[name] = lax.ppermute(send, ("grp", "dom"), pairs)

    received = [received[name] for name in HANDED]
    prepare = kernel_call(
        prepare_kernel,
        [
            jax.ShapeDtypeStruct((EL_NODES * LANES, LANES), bf16),
            field_t,
            jax.ShapeDtypeStruct((EL_NODES * LANES, LANES), bf16),
            jax.ShapeDtypeStruct((8, nodes), i32),
            jax.ShapeDtypeStruct((NODE_ROWS, LANES), i32),
            jax.ShapeDtypeStruct((EL_NODES, 3 * POINTS, LANES), f32),
            jax.ShapeDtypeStruct((3 * POINTS, NODE_ROWS, LANES), f32),
            jax.ShapeDtypeStruct(inverse_jacobian.shape, f32),
            jax.ShapeDtypeStruct(lame_moduli.shape, f32),
            jax.ShapeDtypeStruct(point_weights.shape, f32),
            jax.ShapeDtypeStruct(rank_rows.shape, i32),
            jax.ShapeDtypeStruct((NODE_ROWS, LANES), i32),
            index_t,
        ],
        [VMEM] * 3,
    )
    outs = prepare(packed, shape_t, source)
    incidence, field, faces, inverse_index = outs[:4]
    rank = outs[10]
    connect_rows = outs[4]
    late_index, listed_index = outs[11:]
    element_data = (*outs[5:10], faces)
    wave_t = jax.ShapeDtypeStruct((STEPS, LANES), f32)
    forces_t = jax.ShapeDtypeStruct((3, NODE_ROWS, LANES), f32)
    (
        strain,
        displace,
        velocity,
        pattern,
        half_inverse_mass,
        late_scale,
        node_forces,
        send,
        wave,
    ) = kernel_call(
        first_kernel,
        [strain_t, field_t, field_t, field_t, field_t, lanes_t, forces_t, lanes_t, wave_t],
        [VMEM] * 16,
    )(wave, *received, source, inverse_index, listed_index, field, connect_rows, *element_data)
    strains = jnp.zeros((STEPS - 2, STRAIN * POINTS, LANES), f32)

    def advance(last, displace, velocity, late, node_forces, send, wave):
        dom1, grp1, *new_late = exchange(send)
        side = kernel_call(side_kernel, [field_t, field_t, forces_t, wave_t], [VMEM] * 14)
        displace, velocity, columns, wave = side(
            wave,
            dom1,
            grp1,
            *late,
            source,
            inverse_index,
            connect_rows,
            incidence,
            pattern,
            half_inverse_mass,
            displace,
            velocity,
            node_forces,
        )
        outs = kernel_call(
            step_kernel, [strain_t] + ([] if last else [forces_t, lanes_t]), [VMEM] * 12
        )(*new_late, source, late_index, late_scale, columns, *element_data)
        return outs[0], displace, velocity, new_late, *outs[1:], wave

    def body(step, carried):
        strains, strain, *state = carried
        strains = lax.dynamic_update_index_in_dim(strains, strain, step - 1, 0)
        return (strains, *advance(False, *state))

    none = [jnp.zeros((8, LANES), f32)] * 2
    carried = (strains, strain, displace, velocity, none, node_forces, send, wave)
    strains, strain, *state = lax.fori_loop(1, STEPS - 1, body, carried)
    order = kernel_call(
        order_kernel,
        [
            jax.ShapeDtypeStruct((POINTS * LANES // ORDER_WIDTH * STEPS * STRAIN, ORDER_WIDTH), f32),
            jax.ShapeDtypeStruct((POINTS * LANES, ORDER_WIDTH), bf16),
        ],
        [VMEM] * 3,
        scratch=[pltpu.VMEM(((STEPS * STRAIN + 1) * POINTS, LANES), f32)],
    )
    total, chosen = order(rank, strains, strain)
    strain = advance(True, *state)[0]
    (ordered,) = kernel_call(
        finish_kernel,
        [jax.ShapeDtypeStruct((writers, STEPS * STRAIN, LANES), bf16)],
        [VMEM] * 4,
        scratch=[pltpu.VMEM((9 * POINTS, LANES), f32)],
    )(rank, total, chosen, strain)
    pieces = lax.all_to_all(ordered, "dom", split_axis=0, concat_axis=0, tiled=True)
    (placed,) = kernel_call(
        place_kernel, [jax.ShapeDtypeStruct((STRAIN, STEPS, writers * LANES), jnp.bfloat16)], [VMEM]
    )(pieces)
    return placed.transpose(1, 0, 2)


def solution(mesh):
    placed = (
        P(None, ("grp", "dom")),
        P(("grp", "dom"), None, None),
        P(("grp", "dom"), None),
        P(("grp", "dom"), None),
        P(),
        P(None, ("grp", "dom")),
        P(None, ("grp", "dom")),
        P(None, ("grp", "dom")),
        P(None, ("grp", "dom")),
        P(None, ("grp", "dom")),
        P(),
    )
    return jax.shard_map(
        shards, mesh=mesh, in_specs=placed, out_specs=P(None, None, ("grp", "dom")), check_vma=False
    )
```
